32 devices in a mesh: wide: 16 (over z, x, core), narrow: 2 (over y).
Axes of the slice: x: 2, y: 2, z: 4, core: 2. Of those that a mesh axis runs over, the one named last changes fastest.
Arguments:
- tokens: bfloat16 [2, 32768, 768], P(None, ('wide', 'narrow')), may hold values from -6 to 6
- grad_out: bfloat16 [2, 32768, 768], P(None, ('wide', 'narrow')), may hold values from -6 to 6
- route_ids: int32 [2, 32768], P(None, ('wide', 'narrow')), may hold values from 0 to 15, as said below
- slot_ids: int32 [2, 32768], P(None, ('wide', 'narrow')), may hold values from 0 to 63, as said below
- keep_ids: int32 [2, 32768], P(None, ('wide', 'narrow')), may hold values from 0 to 1, as said below
- gain_one: float32 [768], replicated, may hold values from 0.5 to 1.5
- w_query: bfloat16 [768, 768], replicated, may hold values from -0.21875 to 0.21875
- w_key: bfloat16 [768, 768], replicated, may hold values from -0.21875 to 0.21875
- w_value: bfloat16 [768, 768], replicated, may hold values from -0.21875 to 0.21875
- w_out: bfloat16 [768, 768], replicated, may hold values from -4 to 4
- gain_two: float32 [768], replicated, may hold values from 0.5 to 1.5
- w_route: bfloat16 [768, 16], replicated, may hold values from -0.21875 to 0.21875
- embed: float32 [16, 16], replicated, may hold values from -6 to 6
- w_in: bfloat16 [16, 768, 3072], P('wide', None, 'narrow'), may hold values from -0.21875 to 0.21875
- w_outer: bfloat16 [16, 3072, 768], P('wide', 'narrow'), may hold values from -1.75 to 1.75
Outputs:
- block_out: bfloat16 [2, 32768, 768], P(None, ('wide', 'narrow'))
- grad_tokens: bfloat16 [2, 32768, 768], P(None, ('wide', 'narrow'))
- grad_gain_one: float32 [768], replicated
- grad_w_query: float32 [768, 768], replicated
- grad_w_key: float32 [768, 768], replicated
- grad_w_value: float32 [768, 768], replicated
- grad_w_out: float32 [768, 768], replicated
- grad_gain_two: float32 [768], replicated
- grad_w_route: float32 [768, 16], replicated
- grad_embed: float32 [16, 16], replicated
- grad_w_in: float32 [16, 768, 3072], P('wide', None, 'narrow')
- grad_w_outer: float32 [16, 3072, 768], P('wide', 'narrow')
The draws below stay inside these ranges and needn't reach their ends.
Inputs may be any that keep to these rules, and one draw needn't show every extreme that they name: `route_ids`: an expert's number for every token. `slot_ids`: within one aligned block of 1024 tokens of a micro-batch, the kept tokens bound for one expert carry slots 0, 1, 2, ... in token order; a token that would need slot 64 or more is dropped and carries 0. In every block some expert has all 64 slots filled and more tokens than that. `keep_ids`: 1 exactly for the tokens that got a slot; tokens are dropped in token order once an expert's 64 slots of the block are taken.
All inputs are finite; a program needn't handle non-finite values.
Results may differ from the reference program's by a relative error of at most 0.015.
Values may be sent and summed in bfloat16 or wider, within the bound.
A program may use at most 384 MiB of HBM per device.

```python
import jax
import jax.numpy as jnp
from jax import lax

D = 768
HEADS = 12
HEAD_DIM = 64
FF = 3072
RDIM = 16
LENGTH = 1024
MICRO = 2
EXPERTS = 16
TOK_MB = 1024
TOKENS = 32768
CAP = 64


def routing_tables(key):
    base_key, hot_key, order_key = jax.random.split(jax.random.fold_in(key, 11), 3)
    blocks = MICRO * TOKENS // TOK_MB
    base_ids = jax.random.randint(base_key, (blocks, TOK_MB), 0, EXPERTS, dtype=jnp.int32)
    hot_ids = jax.random.randint(hot_key, (blocks, 1), 0, EXPERTS, dtype=jnp.int32)
    orders = jax.vmap(lambda block_key: jax.random.permutation(block_key, TOK_MB))(jax.random.split(order_key, blocks))
    routes = jnp.where(orders <= CAP, hot_ids, base_ids).astype(jnp.int32)
    onehot = (routes[:, :, None] == jnp.arange(EXPERTS, dtype=jnp.int32)[None, None, :]).astype(jnp.int32)
    before = jnp.cumsum(onehot, axis=1) - onehot
    slots = jnp.sum(before * onehot, axis=-1).astype(jnp.int32)
    keeps = (slots < CAP).astype(jnp.int32)
    slots = jnp.where(keeps > 0, slots, 0).astype(jnp.int32)
    return (routes.reshape(MICRO, TOKENS), slots.reshape(MICRO, TOKENS), keeps.reshape(MICRO, TOKENS))


def draw_route_ids(key, part):
    return routing_tables(key)[0]


def draw_slot_ids(key, part):
    return routing_tables(key)[1]


def draw_keep_ids(key, part):
    return routing_tables(key)[2]


def block_levels(rng, extent, cuts, smallest, top_value):
    def one(axis_at, parts):
        draws = jax.random.uniform(jax.random.fold_in(jax.random.fold_in(rng, 6), axis_at), (parts,), jnp.float32, smallest / len(cuts), top_value / len(cuts))
        return jnp.repeat(jnp.exp(draws), extent[axis_at] // parts).reshape((-1,) + (1,) * (len(extent) - axis_at - 1))

    loudness = one(*cuts[0])
    for cut in cuts[1:]:
        loudness = loudness * one(*cut)
    return loudness


def bell_draw(stream_key, dims, deviation, bound, cuts=(), held_as=jnp.bfloat16):
    loudness = block_levels(stream_key, dims, cuts, -0.22, 0.18) if cuts else 1.0
    array = jax.random.normal(stream_key, dims, jnp.float32) * deviation * loudness
    return jnp.minimum(jnp.maximum(array, -bound), bound).astype(held_as)


def setup_inputs(seed: int = 0) -> dict:
    key_of = jax.random.split(jax.random.key(seed), 16)
    return {
        "tokens": bell_draw(key_of[0], (MICRO, TOKENS, D), 1.0, 6.0, ((1, 32),)),
        "grad_out": bell_draw(key_of[1], (MICRO, TOKENS, D), 1.0, 6.0, ((1, 32),)),
        "route_ids": draw_route_ids(jax.random.fold_in(key_of[15], 71), 0),
        "slot_ids": draw_slot_ids(jax.random.fold_in(key_of[15], 71), 0),
        "keep_ids": draw_keep_ids(jax.random.fold_in(key_of[15], 71), 0),
        "gain_one": jnp.clip(1.0 + 0.1 * jax.random.normal(key_of[5], (D,), jnp.float32), 0.5, 1.5),
        "w_query": bell_draw(key_of[6], (D, D), D ** -0.5, 0.21875),
        "w_key": bell_draw(key_of[7], (D, D), D ** -0.5, 0.21875),
        "w_value": bell_draw(key_of[8], (D, D), D ** -0.5, 0.21875),
        "w_out": bell_draw(key_of[9], (D, D), (max(1, 3 * D // LENGTH)) ** -0.5, 4.0),
        "gain_two": jnp.clip(1.0 + 0.1 * jax.random.normal(key_of[10], (D,), jnp.float32), 0.5, 1.5),
        "w_route": bell_draw(key_of[11], (D, RDIM), D ** -0.5, 0.21875),
        "embed": bell_draw(key_of[12], (EXPERTS, RDIM), 1.0, 6.0, (), jnp.float32),
        "w_in": bell_draw(key_of[13], (EXPERTS, D, FF), D ** -0.5, 0.21875, ((0, 16), (2, 2))),
        "w_outer": bell_draw(key_of[14], (EXPERTS, FF, D), (max(1, FF // (EXPERTS * EXPERTS))) ** -0.5, 1.75, ((0, 16), (1, 2))),
    }


@jax.custom_vjp
def low(v):
    return lax.optimization_barrier(v.astype(jnp.bfloat16)).astype(jnp.float32)

@jax.custom_vjp
def low_back(v):
    return v

def low_keep(v):
    return (low(v), None)

def low_pass(kept, grad):
    return (grad,)

def back_keep(v):
    return (v, None)

def back_low(kept, grad):
    return (low(grad),)
low.defvjp(low_keep, low_pass)
low_back.defvjp(back_keep, back_low)

def layer_norm(values, gain_vec):
    centred = values - lax.optimization_barrier(jnp.mean(values, axis=-1, keepdims=True))
    spread_sq = lax.optimization_barrier(jnp.mean(centred * centred, axis=-1, keepdims=True))
    return centred * lax.rsqrt(spread_sq + 1e-05) * gain_vec

def product(left, right):
    return jnp.dot(left, right, precision=lax.Precision.HIGHEST, preferred_element_type=jnp.float32)

def gate_from(projected, embed_rows, route_row):
    unit_rows = projected * lax.rsqrt(lax.optimization_barrier(jnp.sum(projected * projected, axis=-1, keepdims=True)) + 1.0)
    anchor = embed_rows * lax.rsqrt(lax.optimization_barrier(jnp.sum(embed_rows * embed_rows, axis=-1, keepdims=True)) + 1.0)
    logits = 3.0 * product(unit_rows, anchor.T)
    soft_rows = jax.nn.softmax(logits, axis=-1)
    picked = route_row[:, None] == jnp.arange(soft_rows.shape[1], dtype=jnp.int32)[None, :]
    return lax.optimization_barrier(jnp.sum(jnp.where(picked, soft_rows, 0.0), axis=-1))

def attend_one(queries, keys_in, values_in):
    score_scale = HEAD_DIM ** (-0.5)
    scores = low_back(jnp.einsum('qhd,khd->hqk', queries, keys_in, precision=lax.Precision.HIGHEST) * score_scale)
    soft_rows = low(jax.nn.softmax(scores, axis=-1))
    return jnp.einsum('hqk,khd->qhd', soft_rows, values_in, precision=lax.Precision.HIGHEST)

def expert_one(row_block, first_layer, second_layer):
    pre_act = low_back(product(row_block, first_layer))
    hidden = low(jax.nn.gelu(pre_act, approximate=False))
    return low(low_back(product(hidden, second_layer)))

def forward(params, inputs, route_row, slot_row, keep_row):
    gain_a, wq_full, wk_full, wv_full, wo_full, gain_b, route_weight, embed_rows, first_layers, second_layers = params
    tok_count = inputs.shape[0]
    normed_one = low(layer_norm(inputs, gain_a))
    queries = low(low_back(product(normed_one, wq_full)))
    keys_in = low(low_back(product(normed_one, wk_full)))
    values_in = low(low_back(product(normed_one, wv_full)))
    seq_count = tok_count // LENGTH
    head_shape = (seq_count, LENGTH, HEADS, HEAD_DIM)
    mixed_rows = lax.map(lambda group: jax.checkpoint(attend_one)(*group), (queries.reshape(head_shape), keys_in.reshape(head_shape), values_in.reshape(head_shape)))
    mixed_rows = low(low_back(mixed_rows.reshape(tok_count, D)))
    first_sum = inputs + low_back(product(mixed_rows, wo_full))
    normed_two = low(layer_norm(first_sum, gain_b))
    gate_prob = gate_from(product(normed_two, route_weight), embed_rows, route_row)
    sources = tok_count // TOK_MB
    slot_index = jnp.where(keep_row > 0, route_row * CAP + slot_row, EXPERTS * CAP).astype(jnp.int32)
    slot_index = slot_index.reshape(sources, TOK_MB)

    def scatter_block(block_rows, block_index):
        return jnp.zeros((EXPERTS * CAP, D), jnp.float32).at[block_index].add(block_rows, mode='drop')
    sent_rows = low_back(jax.vmap(scatter_block)(normed_two.reshape(sources, TOK_MB, D), slot_index))
    per_expert = jnp.transpose(sent_rows.reshape(sources, EXPERTS, CAP, D), (1, 0, 2, 3)).reshape(EXPERTS, sources * CAP, D)
    results = lax.map(lambda group: jax.checkpoint(expert_one)(*group), (per_expert, first_layers, second_layers))
    back_rows = jnp.transpose(results.reshape(EXPERTS, sources, CAP, D), (1, 0, 2, 3)).reshape(sources, EXPERTS * CAP, D)

    def take_block(buffer_rows, block_index):
        return jnp.take(buffer_rows, block_index, axis=0, mode='fill', fill_value=0.0)
    returned = jax.vmap(take_block)(back_rows, slot_index).reshape(tok_count, D)
    return first_sum + gate_prob[:, None] * returned

def reference(tokens, grad_out, route_ids, slot_ids, keep_ids, gain_one, w_query, w_key, w_value, w_out, gain_two, w_route, embed, w_in, w_outer):
    params = tuple((item.astype(jnp.float32) for item in (gain_one, w_query, w_key, w_value, w_out, gain_two, w_route, embed, w_in, w_outer)))
    totals = tuple((jnp.zeros(item.shape, jnp.float32) for item in params))
    outputs = []
    input_grads = []
    for micro_step in range(MICRO):

        def forward_one(weights, inputs):
            return forward(weights, inputs, route_ids[micro_step], slot_ids[micro_step], keep_ids[micro_step])
        result_rows, pullback = jax.vjp(forward_one, params, tokens[micro_step].astype(jnp.float32))
        grad_params, grad_inputs = pullback(grad_out[micro_step].astype(jnp.float32))
        totals = tuple((total + part_grad for total, part_grad in zip(totals, grad_params)))
        outputs.append(result_rows.astype(jnp.bfloat16))
        input_grads.append(grad_inputs.astype(jnp.bfloat16))
    return (jnp.stack(outputs), jnp.stack(input_grads), totals[0], totals[1], totals[2], totals[3], totals[4], totals[5], totals[6], totals[7], totals[8], totals[9])
```

```python
import functools

import jax
import jax.numpy as jnp
from jax import lax
from jax.experimental import pallas as pl
from jax.experimental.pallas import tpu as pltpu
from jax.sharding import PartitionSpec as P

D = 768
HEADS = 12
HEAD_DIM = 64
LENGTH = 1024
PAIR = 2 * HEAD_DIM
NN = (((1,), (0,)), ((), ()))
NT = (((1,), (1,)), ((), ()))
TN = (((0,), (0,)), ((), ()))
LOW = jnp.bfloat16
F32 = jnp.float32
VMEM_BYTES = 60 << 20


def dot(left, right, dims=NN, precise=None):
    return lax.dot_general(left, right, dims, precision=precise, preferred_element_type=F32)


def layer_norm(values, gain_vec):
    centred = values - jnp.mean(values, axis=-1, keepdims=True)
    spread_sq = jnp.mean(centred * centred, axis=-1, keepdims=True)
    return centred * lax.rsqrt(spread_sq + 1e-05) * gain_vec


def gate_from(projected, embed_rows, route_row):
    unit_rows = projected * lax.rsqrt(jnp.sum(projected * projected, axis=-1, keepdims=True) + 1.0)
    anchor = embed_rows * lax.rsqrt(jnp.sum(embed_rows * embed_rows, axis=-1, keepdims=True) + 1.0)
    logits = 3.0 * jnp.dot(
        unit_rows, anchor.T, precision=lax.Precision.HIGHEST, preferred_element_type=F32
    )
    soft_rows = jax.nn.softmax(logits, axis=-1)
    picked = route_row[:, None] == jnp.arange(soft_rows.shape[1], dtype=jnp.int32)[None, :]
    return jnp.sum(jnp.where(picked, soft_rows, 0.0), axis=-1)


def attention_forward_kernel(q_ref, k_ref, v_ref, mixed_ref, soft_ref, inv_ref, *, rows):
    lane = lax.broadcasted_iota(jnp.int32, (1, PAIR), 1)
    keys, values = k_ref[...], v_ref[...]
    none = jnp.zeros_like(keys)
    for block in range(LENGTH // rows):
        part = slice(block * rows, (block + 1) * rows)
        query = q_ref[part, :] * LOW(HEAD_DIM**-0.5)
        mixed, inverses = None, []
        for head in range(2):
            mine = (lane < HEAD_DIM) if head == 0 else (lane >= HEAD_DIM)
            scores = dot(query, jnp.where(mine, keys, none), NT)
            top = jnp.max(scores, axis=1, keepdims=True)
            weights = jnp.exp(scores - top)
            inverse = 1.0 / jnp.sum(weights, axis=1, keepdims=True)
            weights = weights.astype(LOW)
            soft_ref[head, part, :] = weights
            inverses.append(jnp.broadcast_to(inverse, (rows, PAIR)))
            term = dot(weights, jnp.where(mine, values, none)) * inverse
            mixed = term if mixed is None else mixed + term
        mixed_ref[part, :] = mixed.astype(LOW)
        inv_ref[part, :] = jnp.where(lane < HEAD_DIM, inverses[0], inverses[1])


def attention_forward(qkv_rows):
    pairs = D // PAIR
    columns = lambda first: pl.BlockSpec((LENGTH, PAIR), lambda i: (0, first + i))
    return pl.pallas_call(
        functools.partial(attention_forward_kernel, rows=512),
        grid=(pairs,),
        in_specs=[columns(0), columns(pairs), columns(2 * pairs)],
        out_specs=[columns(0), pl.BlockSpec((2, LENGTH, LENGTH), lambda i: (i, 0, 0)), columns(0)],
        out_shape=[
            jax.ShapeDtypeStruct((LENGTH, D), LOW),
            jax.ShapeDtypeStruct((HEADS, LENGTH, LENGTH), LOW),
            jax.ShapeDtypeStruct((LENGTH, D), F32),
        ],
        compiler_params=pltpu.CompilerParams(vmem_limit_bytes=VMEM_BYTES),
        cost_estimate=pl.CostEstimate(
            flops=20 * 10**9, bytes_accessed=30 * 2**20, transcendentals=HEADS * LENGTH * LENGTH
        ),
        name="attention_forward",
    )(qkv_rows, qkv_rows, qkv_rows)


def attention_backward_kernel(
    q_ref, k_ref, v_ref, grad_ref, mixed_ref, soft_ref, inv_ref, dq_ref, dk_ref, dv_ref, *, rows
):
    lane = lax.broadcasted_iota(jnp.int32, (1, PAIR), 1)
    scale = LOW(HEAD_DIM**-0.5)
    keys, values = k_ref[...], v_ref[...]
    none = jnp.zeros_like(keys)
    dk_parts, dv_parts = [None, None], [None, None]
    for block in range(LENGTH // rows):
        part = slice(block * rows, (block + 1) * rows)
        query_t = (q_ref[part, :] * scale).T
        scaled = grad_ref[part, :].astype(F32) * inv_ref[part, :]
        inner = scaled * mixed_ref[part, :].astype(F32)
        scaled = scaled.astype(LOW)
        scaled_t = scaled.T
        grad_query = None
        for head in range(2):
            mine = (lane < HEAD_DIM) if head == 0 else (lane >= HEAD_DIM)
            own = slice(head * HEAD_DIM, (head + 1) * HEAD_DIM)
            weights = soft_ref[head, part, :]
            grad_soft = dot(scaled, jnp.where(mine, values, none), NT)
            centre = jnp.sum(jnp.where(mine, inner, 0.0), axis=1, keepdims=True)
            grad_scores = (weights.astype(F32) * (grad_soft - centre)).astype(LOW)
            term = dot(grad_scores, jnp.where(mine, keys, none))
            grad_query = term if grad_query is None else grad_query + term
            dk = dot(query_t[own, :], grad_scores)
            dv = dot(scaled_t[own, :], weights)
            dk_parts[head] = dk if dk_parts[head] is None else dk_parts[head] + dk
            dv_parts[head] = dv if dv_parts[head] is None else dv_parts[head] + dv
        dq_ref[part, :] = (grad_query * HEAD_DIM**-0.5).astype(LOW)
    dk_ref[...] = jnp.concatenate(dk_parts, axis=0).T.astype(LOW)
    dv_ref[...] = jnp.concatenate(dv_parts, axis=0).T.astype(LOW)


def attention_backward(qkv_rows, grad_mixed, mixed_rows, soft, inverses):
    pairs = D // PAIR
    columns = lambda first: pl.BlockSpec((LENGTH, PAIR), lambda i: (0, first + i))
    return pl.pallas_call(
        functools.partial(attention_backward_kernel, rows=512),
        grid=(pairs,),
        in_specs=[
            columns(0),
            columns(pairs),
            columns(2 * pairs),
            columns(0),
            columns(0),
            pl.BlockSpec((2, LENGTH, LENGTH), lambda i: (i, 0, 0)),
            columns(0),
        ],
        out_specs=[columns(0)] * 3,
        out_shape=[jax.ShapeDtypeStruct((LENGTH, D), LOW)] * 3,
        compiler_params=pltpu.CompilerParams(vmem_limit_bytes=VMEM_BYTES),
        cost_estimate=pl.CostEstimate(
            flops=25 * 10**9, bytes_accessed=36 * 2**20, transcendentals=0
        ),
        name="attention_backward",
    )(qkv_rows, qkv_rows, qkv_rows, grad_mixed, mixed_rows, soft, inverses)


def gelu_and_slope(values):
    ratio = 1.0 / (1.0 + jnp.abs(values) * (0.3275911 * 0.7071067811865476))
    bell = jnp.exp(values * values * -0.5)
    series = 0.5 * 1.061405429
    for factor in (-1.453152027, 1.421413741, -0.284496736, 0.254829592):
        series = series * ratio + 0.5 * factor
    tail = series * ratio * bell
    below = jnp.where(values >= 0.0, 1.0 - tail, tail)
    return values * below, below + values * bell * 0.3989422804014327


def expert_kernel(rows_ref, cot_ref, gate_ref, in_ref, outer_ref, *rest, more, steps):
    if more:
        old_in, old_outer = rest[:2]
        rest = rest[2:]
    result_ref, sent_ref, din_ref, douter_ref, grad_sc, rows_t, acc_result, acc_sent = rest
    step = pl.program_id(0)

    @pl.when(step == 0)
    def _():
        grad_sc[...] = (cot_ref[...].astype(F32) * gate_ref[...]).astype(LOW)
        rows_t[...] = rows_ref[...].T
        acc_result[...] = jnp.zeros_like(acc_result)
        acc_sent[...] = jnp.zeros_like(acc_sent)

    first, second = in_ref[0], outer_ref[0]
    hidden, slope = gelu_and_slope(dot(rows_ref[...], first))
    hidden = hidden.astype(LOW)
    grad_rows = grad_sc[...]
    grad_pre = (dot(grad_rows, second, NT) * slope).astype(LOW)
    acc_result[...] += dot(hidden, second)
    acc_sent[...] += dot(grad_pre, first, NT)
    din = dot(rows_t[...], grad_pre)
    douter = dot(hidden, grad_rows, TN)
    if more:
        din += old_in[0]
        douter += old_outer[0]
    din_ref[0] = din
    douter_ref[0] = douter

    @pl.when(step == steps - 1)
    def _():
        result_ref[...] = acc_result[...].astype(LOW)
        sent_ref[...] = acc_sent[...].astype(LOW)


def expert_stage(rows, cot, gate, all_in, all_outer, old=()):
    count, width, units = all_in.shape
    height = rows.shape[0]
    tile = min(512, units)
    per = units // tile
    steps = count * per
    whole = lambda shape: pl.BlockSpec(shape, lambda i: (0,) * len(shape))
    in_spec = pl.BlockSpec((1, width, tile), lambda i: (i // per, 0, i % per))
    outer_spec = pl.BlockSpec((1, tile, width), lambda i: (i // per, i % per, 0))
    return pl.pallas_call(
        functools.partial(expert_kernel, more=bool(old), steps=steps),
        grid=(steps,),
        in_specs=[whole((height, width)), whole((height, width)), whole((height, 1)), in_spec, outer_spec]
        + ([in_spec, outer_spec] if old else []),
        out_specs=[whole((height, width)), whole((height, width)), in_spec, outer_spec],
        out_shape=[
            jax.ShapeDtypeStruct((height, width), LOW),
            jax.ShapeDtypeStruct((height, width), LOW),
            jax.ShapeDtypeStruct(all_in.shape, F32),
            jax.ShapeDtypeStruct(all_outer.shape, F32),
        ],
        scratch_shapes=[
            pltpu.VMEM((height, width), LOW),
            pltpu.VMEM((width, height), LOW),
            pltpu.VMEM((height, width), F32),
            pltpu.VMEM((height, width), F32),
        ],
        compiler_params=pltpu.CompilerParams(vmem_limit_bytes=VMEM_BYTES),
        cost_estimate=pl.CostEstimate(
            flops=12 * height * width * units * count, bytes_accessed=34 * 2**20, transcendentals=0
        ),
        name="expert_stage",
    )(rows, cot, gate, all_in, all_outer, *old)


def local(
    tokens,
    grad_out,
    route_ids,
    slot_ids,
    keep_ids,
    gain_one,
    w_query,
    w_key,
    w_value,
    w_out,
    gain_two,
    w_route,
    embed,
    w_in,
    w_outer,
):
    micro_count, tok_count, feat_width = tokens.shape
    narrow_count = lax.axis_size("narrow")
    expert_count = embed.shape[0]
    slot_cap = max(2, tok_count // expert_count)
    slots = expert_count * slot_cap
    w_qkv = jnp.concatenate([w_query, w_key, w_value], axis=1)
    route_float = w_route.astype(F32)
    all_in = lax.all_gather(w_in[0], "narrow", axis=0, tiled=False)
    all_outer = lax.all_gather(w_outer[0], "narrow", axis=0, tiled=False)
    slot_columns = jnp.arange(slots, dtype=jnp.int32)

    def exchange(rows):
        boxes = rows.reshape((expert_count, slot_cap) + rows.shape[1:])
        boxes = lax.all_to_all(boxes, "wide", split_axis=0, concat_axis=0, tiled=True)
        return boxes.reshape(rows.shape)

    tables, cots = [], []
    for m in range(micro_count):
        slot_index = jnp.where(keep_ids[m] > 0, route_ids[m] * slot_cap + slot_ids[m], -1)
        table = (slot_index[:, None] == slot_columns[None, :]).astype(LOW)
        tables.append(table)
        cots.append(exchange(dot(table, grad_out[m], TN).astype(LOW)))

    ahead = []
    for m in range(micro_count):
        inputs = tokens[m].astype(F32)
        normed_one, pull_one = jax.vjp(layer_norm, inputs, gain_one)
        normed_low = normed_one.astype(LOW)
        qkv_rows = dot(normed_low, w_qkv).astype(LOW)
        mixed_rows, soft, inverses = attention_forward(qkv_rows)
        first_sum = inputs + dot(mixed_rows, w_out)
        normed_two, pull_two = jax.vjp(layer_norm, first_sum, gain_two)
        second_low = normed_two.astype(LOW)
        projected = dot(second_low, w_route)
        gate_prob, pull_gate = jax.vjp(
            lambda proj_in, embed_in: gate_from(proj_in, embed_in, route_ids[m]), projected, embed
        )
        sent = exchange(dot(tables[m], second_low, TN).astype(LOW))
        gates = exchange(jnp.sum(tables[m].astype(F32) * gate_prob[:, None], axis=0)[:, None])
        ahead.append(
            (normed_low, pull_one, qkv_rows, mixed_rows, soft, inverses, first_sum, pull_two,
             second_low, gate_prob, pull_gate, sent, gates)
        )

    back = []
    expert_grads = ()
    for m in range(micro_count):
        sent, gates = ahead[m][-2:]
        result, grad_sent, *expert_grads = expert_stage(
            sent, cots[m], gates, all_in, all_outer, tuple(expert_grads)
        )
        back.append((exchange(result), exchange(grad_sent)))
    part_in, part_outer = expert_grads
    grad_in = lax.psum_scatter(part_in.astype(LOW), "narrow", scatter_dimension=0, tiled=False)
    grad_outer = lax.psum_scatter(part_outer.astype(LOW), "narrow", scatter_dimension=0, tiled=False)

    outputs, input_grads, sums = [], [], None
    for m in range(micro_count):
        (normed_low, pull_one, qkv_rows, mixed_rows, soft, inverses, first_sum, pull_two,
         second_low, gate_prob, pull_gate, _, _) = ahead[m]
        back_rows, back_grads = back[m]
        table = tables[m]
        returned = dot(table, back_rows)
        outputs.append((first_sum + gate_prob[:, None] * returned).astype(LOW))
        grad_sum = grad_out[m].astype(F32)
        grad_gate = jnp.sum(grad_sum * returned, axis=-1)
        grad_projected, grad_embed = pull_gate(grad_gate)
        grad_second = dot(table, back_grads) + dot(
            grad_projected, route_float, NT, lax.Precision.HIGHEST
        )
        grad_route = dot(second_low.astype(F32), grad_projected, TN, lax.Precision.HIGHEST)
        grad_first_norm, grad_gain_two = pull_two(grad_second)
        grad_first = grad_sum + grad_first_norm
        grad_branch = grad_first.astype(LOW)
        grad_wo = dot(mixed_rows, grad_branch, TN)
        grad_mixed = dot(grad_branch, w_out, NT).astype(LOW)
        grad_qkv = jnp.concatenate(
            attention_backward(qkv_rows, grad_mixed, mixed_rows, soft, inverses), axis=1
        )
        grad_wqkv = dot(normed_low, grad_qkv, TN)
        grad_input_norm, grad_gain_one = pull_one(dot(grad_qkv, w_qkv, NT))
        input_grads.append((grad_first + grad_input_norm).astype(LOW))
        terms = (grad_gain_one, grad_wqkv, grad_wo, grad_gain_two, grad_route, grad_embed)
        sums = terms if sums is None else tuple(a + b for a, b in zip(sums, terms))
    gain_one_sum, wqkv_sum, wo_sum, gain_two_sum, route_sum, embed_sum = sums
    wqkv_sum, wo_sum = lax.psum((wqkv_sum.astype(LOW), wo_sum.astype(LOW)), ("wide", "narrow"))
    gain_one_sum, gain_two_sum, route_sum, embed_sum = lax.psum(
        (gain_one_sum, gain_two_sum, route_sum, embed_sum), ("wide", "narrow")
    )
    wqkv_sum = wqkv_sum.astype(F32)
    return (
        jnp.stack(outputs),
        jnp.stack(input_grads),
        gain_one_sum,
        wqkv_sum[:, :feat_width],
        wqkv_sum[:, feat_width : 2 * feat_width],
        wqkv_sum[:, 2 * feat_width :],
        wo_sum.astype(F32),
        gain_two_sum,
        route_sum,
        embed_sum,
        grad_in.astype(F32)[None],
        grad_outer.astype(F32)[None],
    )


def solution(mesh):
    tokens_spec = P(None, ("wide", "narrow"), None)
    ids_spec = P(None, ("wide", "narrow"))
    in_spec, outer_spec = P("wide", None, "narrow"), P("wide", "narrow", None)
    return jax.shard_map(
        local,
        mesh=mesh,
        in_specs=(tokens_spec,) * 2 + (ids_spec,) * 3 + (P(),) * 8 + (in_spec, outer_spec),
        out_specs=(tokens_spec,) * 2 + (P(),) * 8 + (in_spec, outer_spec),
        check_vma=False,
    )
```

```python
import functools

import jax
import jax.numpy as jnp
from jax import lax
from jax.experimental import pallas as pl
from jax.experimental.pallas import tpu as pltpu
from jax.sharding import PartitionSpec as P

D = 768
HEADS = 12
HEAD_DIM = 64
LENGTH = 1024
PAIR = 2 * HEAD_DIM
NN = (((1,), (0,)), ((), ()))
NT = (((1,), (1,)), ((), ()))
TN = (((0,), (0,)), ((), ()))
LOW = jnp.bfloat16
F32 = jnp.float32
VMEM_BYTES = 60 << 20


def dot(left, right, dims=NN, precise=None):
    return lax.dot_general(left, right, dims, precision=precise, preferred_element_type=F32)


def layer_norm(values, gain_vec):
    centred = values - jnp.mean(values, axis=-1, keepdims=True)
    spread_sq = jnp.mean(centred * centred, axis=-1, keepdims=True)
    return centred * lax.rsqrt(spread_sq + 1e-05) * gain_vec


def gate_from(projected, embed_rows, route_row):
    unit_rows = projected * lax.rsqrt(jnp.sum(projected * projected, axis=-1, keepdims=True) + 1.0)
    anchor = embed_rows * lax.rsqrt(jnp.sum(embed_rows * embed_rows, axis=-1, keepdims=True) + 1.0)
    logits = 3.0 * jnp.dot(
        unit_rows, anchor.T, precision=lax.Precision.HIGHEST, preferred_element_type=F32
    )
    soft_rows = jax.nn.softmax(logits, axis=-1)
    picked = route_row[:, None] == jnp.arange(soft_rows.shape[1], dtype=jnp.int32)[None, :]
    return jnp.sum(jnp.where(picked, soft_rows, 0.0), axis=-1)


MESH = pl.DeviceIdType.MESH


def call_with_moves(body, moves, cid, *, grid, in_specs, out_specs, out_shape, scratch_shapes=(), cost, name, args):
    members = lax.axis_size("wide")
    n_in, n_out, n_moves, n_scratch = len(in_specs), len(out_specs), len(moves), len(scratch_shapes)

    def kernel(*refs):
        ins, refs = refs[:n_in], refs[n_in:]
        sources, refs = refs[:n_moves], refs[n_moves:]
        outs, refs = refs[:n_out], refs[n_out:]
        targets, refs = refs[:n_moves], refs[n_moves:]
        scratch, refs = refs[:n_scratch], refs[n_scratch:]
        stages, (send_sem, recv_sem, own_sem) = refs[:n_moves], refs[n_moves:]
        me = lax.axis_index("wide")
        step = pl.program_id(0)

        def remote(i, d):
            peer = lax.rem(me + d, members)
            return pltpu.make_async_remote_copy(
                src_ref=sources[i].at[peer],
                dst_ref=targets[i].at[me],
                send_sem=send_sem.at[i, d],
                recv_sem=recv_sem.at[i, d],
                device_id={"wide": peer},
                device_id_type=MESH,
            )

        @pl.when(step == 0)
        def _():
            barrier = pltpu.get_barrier_semaphore()
            for d in range(1, members):
                pl.semaphore_signal(
                    barrier, inc=1, device_id={"wide": lax.rem(me + d, members)}, device_id_type=MESH
                )
            pl.semaphore_wait(barrier, members - 1)
            for i in range(n_moves):
                for d in range(1, members):
                    remote(i, d).start()
                pltpu.make_async_copy(sources[i].at[me], stages[i], own_sem.at[i]).start()

        body(*ins, *outs, *scratch)

        @pl.when(step == grid[0] - 1)
        def _():
            for i in range(n_moves):
                pltpu.make_async_copy(sources[i].at[me], stages[i], own_sem.at[i]).wait()
                pltpu.make_async_copy(stages[i], targets[i].at[me], own_sem.at[i]).start()
            for i in range(n_moves):
                pltpu.make_async_copy(stages[i], targets[i].at[me], own_sem.at[i]).wait()
                for d in range(1, members):
                    remote(i, d).wait()

    anywhere = pl.BlockSpec(memory_space=pl.ANY)
    results = pl.pallas_call(
        kernel,
        grid=grid,
        in_specs=list(in_specs) + [anywhere] * n_moves,
        out_specs=list(out_specs) + [anywhere] * n_moves,
        out_shape=list(out_shape) + [jax.ShapeDtypeStruct(a.shape, a.dtype) for a in moves],
        scratch_shapes=list(scratch_shapes)
        + [pltpu.VMEM(a.shape[1:], a.dtype) for a in moves]
        + [
            pltpu.SemaphoreType.DMA((n_moves, members)),
            pltpu.SemaphoreType.DMA((n_moves, members)),
            pltpu.SemaphoreType.DMA((n_moves,)),
        ],
        compiler_params=pltpu.CompilerParams(
            vmem_limit_bytes=VMEM_BYTES, collective_id=cid, has_side_effects=True
        ),
        cost_estimate=cost,
        name=name,
    )(*args, *moves)
    return results[:n_out], results[n_out:]


def attention_forward_kernel(q_ref, k_ref, v_ref, mixed_ref, soft_ref, inv_ref, *, rows):
    lane = lax.broadcasted_iota(jnp.int32, (1, PAIR), 1)
    keys, values = k_ref[...], v_ref[...]
    none = jnp.zeros_like(keys)
    for block in range(LENGTH // rows):
        part = slice(block * rows, (block + 1) * rows)
        query = q_ref[part, :] * LOW(HEAD_DIM**-0.5)
        mixed, inverses = None, []
        for head in range(2):
            mine = (lane < HEAD_DIM) if head == 0 else (lane >= HEAD_DIM)
            scores = dot(query, jnp.where(mine, keys, none), NT)
            top = jnp.max(scores, axis=1, keepdims=True)
            weights = jnp.exp(scores - top)
            inverse = 1.0 / jnp.sum(weights, axis=1, keepdims=True)
            weights = weights.astype(LOW)
            soft_ref[head, part, :] = weights
            inverses.append(jnp.broadcast_to(inverse, (rows, PAIR)))
            term = dot(weights, jnp.where(mine, values, none)) * inverse
            mixed = term if mixed is None else mixed + term
        mixed_ref[part, :] = mixed.astype(LOW)
        inv_ref[part, :] = jnp.where(lane < HEAD_DIM, inverses[0], inverses[1])


def attention_forward(qkv_rows, moves, cid):
    pairs = D // PAIR
    columns = lambda first: pl.BlockSpec((LENGTH, PAIR), lambda i: (0, first + i))
    return call_with_moves(
        functools.partial(attention_forward_kernel, rows=512),
        moves,
        cid,
        grid=(pairs,),
        in_specs=[columns(0), columns(pairs), columns(2 * pairs)],
        out_specs=[columns(0), pl.BlockSpec((2, LENGTH, LENGTH), lambda i: (i, 0, 0)), columns(0)],
        out_shape=[
            jax.ShapeDtypeStruct((LENGTH, D), LOW),
            jax.ShapeDtypeStruct((HEADS, LENGTH, LENGTH), LOW),
            jax.ShapeDtypeStruct((LENGTH, D), F32),
        ],
        cost=pl.CostEstimate(
            flops=20 * 10**9, bytes_accessed=30 * 2**20, transcendentals=HEADS * LENGTH * LENGTH
        ),
        name="attention_forward",
        args=(qkv_rows, qkv_rows, qkv_rows),
    )


def attention_backward_kernel(
    q_ref, k_ref, v_ref, grad_ref, mixed_ref, soft_ref, inv_ref, dq_ref, dk_ref, dv_ref, *, rows
):
    lane = lax.broadcasted_iota(jnp.int32, (1, PAIR), 1)
    scale = LOW(HEAD_DIM**-0.5)
    keys, values = k_ref[...], v_ref[...]
    none = jnp.zeros_like(keys)
    dk_parts, dv_parts = [None, None], [None, None]
    for block in range(LENGTH // rows):
        part = slice(block * rows, (block + 1) * rows)
        query_t = (q_ref[part, :] * scale).T
        scaled = grad_ref[part, :].astype(F32) * inv_ref[part, :]
        inner = scaled * mixed_ref[part, :].astype(F32)
        scaled = scaled.astype(LOW)
        scaled_t = scaled.T
        grad_query = None
        for head in range(2):
            mine = (lane < HEAD_DIM) if head == 0 else (lane >= HEAD_DIM)
            own = slice(head * HEAD_DIM, (head + 1) * HEAD_DIM)
            weights = soft_ref[head, part, :]
            grad_soft = dot(scaled, jnp.where(mine, values, none), NT)
            centre = jnp.sum(jnp.where(mine, inner, 0.0), axis=1, keepdims=True)
            grad_scores = (weights.astype(F32) * (grad_soft - centre)).astype(LOW)
            term = dot(grad_scores, jnp.where(mine, keys, none))
            grad_query = term if grad_query is None else grad_query + term
            dk = dot(query_t[own, :], grad_scores)
            dv = dot(scaled_t[own, :], weights)
            dk_parts[head] = dk if dk_parts[head] is None else dk_parts[head] + dk
            dv_parts[head] = dv if dv_parts[head] is None else dv_parts[head] + dv
        dq_ref[part, :] = (grad_query * HEAD_DIM**-0.5).astype(LOW)
    dk_ref[...] = jnp.concatenate(dk_parts, axis=0).T.astype(LOW)
    dv_ref[...] = jnp.concatenate(dv_parts, axis=0).T.astype(LOW)


def attention_backward(qkv_rows, grad_mixed, mixed_rows, soft, inverses, moves, cid):
    pairs = D // PAIR
    columns = lambda first: pl.BlockSpec((LENGTH, PAIR), lambda i: (0, first + i))
    return call_with_moves(
        functools.partial(attention_backward_kernel, rows=512),
        moves,
        cid,
        grid=(pairs,),
        in_specs=[
            columns(0),
            columns(pairs),
            columns(2 * pairs),
            columns(0),
            columns(0),
            pl.BlockSpec((2, LENGTH, LENGTH), lambda i: (i, 0, 0)),
            columns(0),
        ],
        out_specs=[columns(0)] * 3,
        out_shape=[jax.ShapeDtypeStruct((LENGTH, D), LOW)] * 3,
        cost=pl.CostEstimate(flops=25 * 10**9, bytes_accessed=36 * 2**20, transcendentals=0),
        name="attention_backward",
        args=(qkv_rows, qkv_rows, qkv_rows, grad_mixed, mixed_rows, soft, inverses),
    )


def gelu_and_slope(values):
    ratio = 1.0 / (1.0 + jnp.abs(values) * (0.3275911 * 0.7071067811865476))
    bell = jnp.exp(values * values * -0.5)
    series = 0.5 * 1.061405429
    for factor in (-1.453152027, 1.421413741, -0.284496736, 0.254829592):
        series = series * ratio + 0.5 * factor
    tail = series * ratio * bell
    below = jnp.where(values >= 0.0, 1.0 - tail, tail)
    return values * below, below + values * bell * 0.3989422804014327


def diagonal(slot_cap):
    shape = (slot_cap, 128)
    return lax.broadcasted_iota(jnp.int32, shape, 0) == lax.broadcasted_iota(jnp.int32, shape, 1)


def expert_kernel(rows_ref, cot_ref, gate_ref, in_ref, outer_ref, *rest, more, steps, slot_cap):
    if more:
        old_in, old_outer = rest[:2]
        rest = rest[2:]
    result_ref, sent_ref, dots_ref, din_ref, douter_ref, grad_sc, rows_t, acc_result, acc_sent = rest
    step = pl.program_id(0)
    sources = rows_ref.shape[0] // slot_cap

    @pl.when(step == 0)
    def _():
        for w in range(sources):
            part = slice(w * slot_cap, (w + 1) * slot_cap)
            gate = jnp.sum(jnp.where(diagonal(slot_cap), gate_ref[w, 0:1, :], 0.0), axis=1, keepdims=True)
            grad_sc[part, :] = (cot_ref[part, :].astype(F32) * gate).astype(LOW)
        rows_t[...] = rows_ref[...].T
        acc_result[...] = jnp.zeros_like(acc_result)
        acc_sent[...] = jnp.zeros_like(acc_sent)

    first, second = in_ref[0], outer_ref[0]
    hidden, slope = gelu_and_slope(dot(rows_ref[...], first))
    hidden = hidden.astype(LOW)
    grad_rows = grad_sc[...]
    grad_pre = (dot(grad_rows, second, NT) * slope).astype(LOW)
    acc_result[...] += dot(hidden, second)
    acc_sent[...] += dot(grad_pre, first, NT)
    din = dot(rows_t[...], grad_pre)
    douter = dot(hidden, grad_rows, TN)
    if more:
        din += old_in[0]
        douter += old_outer[0]
    din_ref[0] = din
    douter_ref[0] = douter

    @pl.when(step == steps - 1)
    def _():
        result = acc_result[...].astype(LOW)
        result_ref[...] = result
        sent_ref[...] = acc_sent[...].astype(LOW)
        for w in range(sources):
            part = slice(w * slot_cap, (w + 1) * slot_cap)
            products = cot_ref[part, :].astype(F32) * result[part, :].astype(F32)
            column = jnp.sum(products, axis=1, keepdims=True)
            row = jnp.sum(jnp.where(diagonal(slot_cap), column, 0.0), axis=0, keepdims=True)
            dots_ref[w] = jnp.broadcast_to(row, (8, 128))


def expert_stage(rows, cot, gates, all_in, all_outer, old, slot_cap, moves, cid):
    count, width, units = all_in.shape
    height = rows.shape[0]
    tile = min(512, units)
    per = units // tile
    steps = count * per
    whole = lambda shape: pl.BlockSpec(shape, lambda i: (0,) * len(shape))
    in_spec = pl.BlockSpec((1, width, tile), lambda i: (i // per, 0, i % per))
    outer_spec = pl.BlockSpec((1, tile, width), lambda i: (i // per, i % per, 0))
    return call_with_moves(
        functools.partial(expert_kernel, more=bool(old), steps=steps, slot_cap=slot_cap),
        moves,
        cid,
        grid=(steps,),
        in_specs=[whole((height, width)), whole((height, width)), whole(gates.shape), in_spec, outer_spec]
        + ([in_spec, outer_spec] if old else []),
        out_specs=[whole((height, width)), whole((height, width)), whole(gates.shape), in_spec, outer_spec],
        out_shape=[
            jax.ShapeDtypeStruct((height, width), LOW),
            jax.ShapeDtypeStruct((height, width), LOW),
            jax.ShapeDtypeStruct(gates.shape, F32),
            jax.ShapeDtypeStruct(all_in.shape, F32),
            jax.ShapeDtypeStruct(all_outer.shape, F32),
        ],
        scratch_shapes=[
            pltpu.VMEM((height, width), LOW),
            pltpu.VMEM((width, height), LOW),
            pltpu.VMEM((height, width), F32),
            pltpu.VMEM((height, width), F32),
        ],
        cost=pl.CostEstimate(
            flops=12 * height * width * units * count, bytes_accessed=34 * 2**20, transcendentals=0
        ),
        name="expert_stage",
        args=(rows, cot, gates, all_in, all_outer, *old),
    )


def local(
    tokens,
    grad_out,
    route_ids,
    slot_ids,
    keep_ids,
    gain_one,
    w_query,
    w_key,
    w_value,
    w_out,
    gain_two,
    w_route,
    embed,
    w_in,
    w_outer,
):
    micro_count, tok_count, feat_width = tokens.shape
    narrow_count = lax.axis_size("narrow")
    expert_count = embed.shape[0]
    slot_cap = max(2, tok_count // expert_count)
    slots = expert_count * slot_cap
    w_qkv = jnp.concatenate([w_query, w_key, w_value], axis=1)
    route_float = w_route.astype(F32)
    all_in = lax.all_gather(w_in[0], "narrow", axis=0, tiled=False)
    all_outer = lax.all_gather(w_outer[0], "narrow", axis=0, tiled=False)
    slot_columns = jnp.arange(slots, dtype=jnp.int32)

    def boxes(rows):
        return rows.reshape((expert_count, slot_cap) + rows.shape[1:])

    def flat(boxed):
        return boxed.reshape((expert_count * slot_cap,) + boxed.shape[2:])

    tables, cot_boxes = [], []
    for m in range(micro_count):
        slot_index = jnp.where(keep_ids[m] > 0, route_ids[m] * slot_cap + slot_ids[m], -1)
        table = (slot_index[:, None] == slot_columns[None, :]).astype(LOW)
        tables.append(table)
        cot_boxes.append(boxes(dot(table, grad_out[m], TN).astype(LOW)))

    ahead, send = [], []
    for m in range(micro_count):
        inputs = tokens[m].astype(F32)
        normed_one, pull_one = jax.vjp(layer_norm, inputs, gain_one)
        normed_low = normed_one.astype(LOW)
        qkv_rows = dot(normed_low, w_qkv).astype(LOW)
        if m == 0:
            (mixed_rows, soft, inverses), (cot_0,) = attention_forward(qkv_rows, (cot_boxes[0],), 1)
        else:
            (mixed_rows, soft, inverses), (sent_0, gates_0, cot_1) = attention_forward(
                qkv_rows, (*send[0], cot_boxes[1]), 2
            )
        first_sum = inputs + dot(mixed_rows, w_out)
        normed_two, pull_two = jax.vjp(layer_norm, first_sum, gain_two)
        second_low = normed_two.astype(LOW)
        projected = dot(second_low, w_route)
        gate_prob, pull_gate = jax.vjp(
            lambda proj_in, embed_in: gate_from(proj_in, embed_in, route_ids[m]), projected, embed
        )
        gates = jnp.sum(tables[m].astype(F32) * gate_prob[:, None], axis=0)
        gates = jnp.pad(gates.reshape(expert_count, 1, slot_cap), ((0, 0), (0, 7), (0, 128 - slot_cap)))
        send.append((boxes(dot(tables[m], second_low, TN).astype(LOW)), gates))
        ahead.append(
            (normed_low, pull_one, qkv_rows, mixed_rows, soft, inverses, first_sum, pull_two,
             second_low, gate_prob, pull_gate)
        )

    (result_0, grad_0, dots_0, *expert_grads), (sent_1, gates_1) = expert_stage(
        flat(sent_0), flat(cot_0), gates_0, all_in, all_outer, (), slot_cap, send[1], 3
    )
    (result_1, grad_1, dots_1, part_in, part_outer), (home_grad_0, home_dots_0) = expert_stage(
        flat(sent_1), flat(cot_1), gates_1, all_in, all_outer, tuple(expert_grads), slot_cap,
        (boxes(grad_0), dots_0), 4
    )
    grad_in = lax.psum_scatter(part_in.astype(LOW), "narrow", scatter_dimension=0, tiled=False)
    grad_outer = lax.psum_scatter(part_outer.astype(LOW), "narrow", scatter_dimension=0, tiled=False)

    input_grads, sums = [], None
    for m in range(micro_count):
        (normed_low, pull_one, qkv_rows, mixed_rows, soft, inverses, first_sum, pull_two,
         second_low, gate_prob, pull_gate) = ahead[m]
        home_grad, home_dots = (home_grad_0, home_dots_0) if m == 0 else (home_grad_1, home_dots_1)
        table = tables[m]
        grad_sum = grad_out[m].astype(F32)
        slot_dots = home_dots[:, 0, :slot_cap].reshape(slots)
        grad_gate = jnp.sum(table.astype(F32) * slot_dots[None, :], axis=-1)
        grad_projected, grad_embed = pull_gate(grad_gate)
        grad_second = dot(table, flat(home_grad)) + dot(
            grad_projected, route_float, NT, lax.Precision.HIGHEST
        )
        grad_route = dot(second_low.astype(F32), grad_projected, TN, lax.Precision.HIGHEST)
        grad_first_norm, grad_gain_two = pull_two(grad_second)
        grad_first = grad_sum + grad_first_norm
        grad_branch = grad_first.astype(LOW)
        grad_wo = dot(mixed_rows, grad_branch, TN)
        grad_mixed = dot(grad_branch, w_out, NT).astype(LOW)
        if m == 0:
            grads, (home_grad_1, home_dots_1, home_result_0) = attention_backward(
                qkv_rows, grad_mixed, mixed_rows, soft, inverses, (boxes(grad_1), dots_1, boxes(result_0)), 5
            )
        else:
            grads, (home_result_1,) = attention_backward(
                qkv_rows, grad_mixed, mixed_rows, soft, inverses, (boxes(result_1),), 6
            )
        grad_qkv = jnp.concatenate(grads, axis=1)
        grad_wqkv = dot(normed_low, grad_qkv, TN)
        grad_input_norm, grad_gain_one = pull_one(dot(grad_qkv, w_qkv, NT))
        input_grads.append((grad_first + grad_input_norm).astype(LOW))
        terms = (grad_gain_one, grad_wqkv, grad_wo, grad_gain_two, grad_route, grad_embed)
        sums = terms if sums is None else tuple(a + b for a, b in zip(sums, terms))
    outputs = []
    for m, home_result in enumerate((home_result_0, home_result_1)):
        first_sum, gate_prob = ahead[m][6], ahead[m][9]
        returned = dot(tables[m], flat(home_result))
        outputs.append((first_sum + gate_prob[:, None] * returned).astype(LOW))
    gain_one_sum, wqkv_sum, wo_sum, gain_two_sum, route_sum, embed_sum = sums
    wqkv_sum, wo_sum = lax.psum((wqkv_sum.astype(LOW), wo_sum.astype(LOW)), ("wide", "narrow"))
    gain_one_sum, gain_two_sum, route_sum, embed_sum = lax.psum(
        (gain_one_sum, gain_two_sum, route_sum, embed_sum), ("wide", "narrow")
    )
    wqkv_sum = wqkv_sum.astype(F32)
    return (
        jnp.stack(outputs),
        jnp.stack(input_grads),
        gain_one_sum,
        wqkv_sum[:, :feat_width],
        wqkv_sum[:, feat_width : 2 * feat_width],
        wqkv_sum[:, 2 * feat_width :],
        wo_sum.astype(F32),
        gain_two_sum,
        route_sum,
        embed_sum,
        grad_in.astype(F32)[None],
        grad_outer.astype(F32)[None],
    )


def solution(mesh):
    tokens_spec = P(None, ("wide", "narrow"), None)
    ids_spec = P(None, ("wide", "narrow"))
    in_spec, outer_spec = P("wide", None, "narrow"), P("wide", "narrow", None)
    return jax.shard_map(
        local,
        mesh=mesh,
        in_specs=(tokens_spec,) * 2 + (ids_spec,) * 3 + (P(),) * 8 + (in_spec, outer_spec),
        out_specs=(tokens_spec,) * 2 + (P(),) * 8 + (in_spec, outer_spec),
        check_vma=False,
    )
```

```python
import functools

import jax
import jax.numpy as jnp
from jax import lax
from jax.experimental import pallas as pl
from jax.experimental.pallas import tpu as pltpu
from jax.sharding import PartitionSpec as P

D = 768
HEADS = 12
HEAD_DIM = 64
LENGTH = 1024
PAIR = 2 * HEAD_DIM
NN = (((1,), (0,)), ((), ()))
NT = (((1,), (1,)), ((), ()))
TN = (((0,), (0,)), ((), ()))
LOW = jnp.bfloat16
F32 = jnp.float32
VMEM_BYTES = 60 << 20


def dot(left, right, dims=NN, precise=None):
    return lax.dot_general(left, right, dims, precision=precise, preferred_element_type=F32)


def layer_norm(values, gain_vec):
    centred = values - jnp.mean(values, axis=-1, keepdims=True)
    spread_sq = jnp.mean(centred * centred, axis=-1, keepdims=True)
    return centred * lax.rsqrt(spread_sq + 1e-05) * gain_vec


def gate_from(projected, embed_rows, route_row):
    unit_rows = projected * lax.rsqrt(jnp.sum(projected * projected, axis=-1, keepdims=True) + 1.0)
    anchor = embed_rows * lax.rsqrt(jnp.sum(embed_rows * embed_rows, axis=-1, keepdims=True) + 1.0)
    logits = 3.0 * jnp.dot(
        unit_rows, anchor.T, precision=lax.Precision.HIGHEST, preferred_element_type=F32
    )
    soft_rows = jax.nn.softmax(logits, axis=-1)
    picked = route_row[:, None] == jnp.arange(soft_rows.shape[1], dtype=jnp.int32)[None, :]
    return jnp.sum(jnp.where(picked, soft_rows, 0.0), axis=-1)


MESH = pl.DeviceIdType.MESH


def call_with_moves(
    body, moves, pushes, cid, *, grid, in_specs, out_specs, out_shape, scratch_shapes=(), cost, name, args
):
    members, spread = lax.axis_size("wide"), lax.axis_size("narrow")
    n_in, n_out, n_moves, n_scratch = len(in_specs), len(out_specs), len(moves), len(scratch_shapes)
    arrays = []
    for array, _, _ in pushes:
        if not any(array is known for known in arrays):
            arrays.append(array)
    which = [next(k for k, known in enumerate(arrays) if known is array) for array, _, _ in pushes]
    n_arrays, n_pushes = len(arrays), len(pushes)

    def kernel(*refs):
        ins, refs = refs[:n_in], refs[n_in:]
        sources, refs = refs[:n_moves], refs[n_moves:]
        pushed, refs = refs[:n_arrays], refs[n_arrays:]
        outs, refs = refs[:n_out], refs[n_out:]
        targets, refs = refs[:n_moves], refs[n_moves:]
        landings, refs = refs[:n_pushes], refs[n_pushes:]
        scratch, refs = refs[:n_scratch], refs[n_scratch:]
        stages, refs = refs[:n_moves], refs[n_moves:]
        send_sem, recv_sem, own_sem, push_send, push_recv = refs
        me, side = lax.axis_index("wide"), lax.axis_index("narrow")
        step = pl.program_id(0)

        def remote(i, d):
            peer = lax.rem(me + d, members)
            return pltpu.make_async_remote_copy(
                src_ref=sources[i].at[peer],
                dst_ref=targets[i].at[me],
                send_sem=send_sem.at[i, d],
                recv_sem=recv_sem.at[i, d],
                device_id={"wide": peer},
                device_id_type=MESH,
            )

        def push(k, j):
            return pltpu.make_async_remote_copy(
                src_ref=pushes[k][1](pushed[which[k]], j),
                dst_ref=landings[k].at[j],
                send_sem=push_send.at[k, j],
                recv_sem=push_recv.at[k, j],
                device_id={"narrow": lax.rem(side + j + 1, spread)},
                device_id_type=MESH,
            )

        @pl.when(step == 0)
        def _():
            barrier = pltpu.get_barrier_semaphore()
            count = 0
            if n_moves:
                for d in range(1, members):
                    pl.semaphore_signal(
                        barrier, inc=1, device_id={"wide": lax.rem(me + d, members)}, device_id_type=MESH
                    )
                count += members - 1
            if n_pushes:
                for j in range(spread - 1):
                    pl.semaphore_signal(
                        barrier, inc=1, device_id={"narrow": lax.rem(side + j + 1, spread)}, device_id_type=MESH
                    )
                count += spread - 1
            pl.semaphore_wait(barrier, count)
            for k in range(n_pushes):
                for j in range(spread - 1):
                    push(k, j).start()
            for i in range(n_moves):
                for d in range(1, members):
                    remote(i, d).start()
                pltpu.make_async_copy(sources[i].at[me], stages[i], own_sem.at[i]).start()

        body(*ins, *outs, *scratch)

        @pl.when(step == grid[0] - 1)
        def _():
            for i in range(n_moves):
                pltpu.make_async_copy(sources[i].at[me], stages[i], own_sem.at[i]).wait()
                pltpu.make_async_copy(stages[i], targets[i].at[me], own_sem.at[i]).start()
            for i in range(n_moves):
                pltpu.make_async_copy(stages[i], targets[i].at[me], own_sem.at[i]).wait()
                for d in range(1, members):
                    remote(i, d).wait()
            for k in range(n_pushes):
                for j in range(spread - 1):
                    push(k, j).wait()

    anywhere = pl.BlockSpec(memory_space=pl.ANY)
    results = pl.pallas_call(
        kernel,
        grid=grid,
        in_specs=list(in_specs) + [anywhere] * (n_moves + n_arrays),
        out_specs=list(out_specs) + [anywhere] * (n_moves + n_pushes),
        out_shape=list(out_shape)
        + [jax.ShapeDtypeStruct(a.shape, a.dtype) for a in moves]
        + [jax.ShapeDtypeStruct((spread - 1, *shape), a.dtype) for a, _, shape in pushes],
        scratch_shapes=list(scratch_shapes)
        + [pltpu.VMEM(a.shape[1:], a.dtype) for a in moves]
        + [
            pltpu.SemaphoreType.DMA((max(1, n_moves), members)),
            pltpu.SemaphoreType.DMA((max(1, n_moves), members)),
            pltpu.SemaphoreType.DMA((max(1, n_moves),)),
            pltpu.SemaphoreType.DMA((max(1, n_pushes), spread)),
            pltpu.SemaphoreType.DMA((max(1, n_pushes), spread)),
        ],
        compiler_params=pltpu.CompilerParams(
            vmem_limit_bytes=VMEM_BYTES, collective_id=cid, has_side_effects=True
        ),
        cost_estimate=cost,
        name=name,
    )(*args, *moves, *arrays)
    return results[:n_out], results[n_out : n_out + n_moves], results[n_out + n_moves :]


def reduce_orders(wide_count, narrow_count):
    bits = lambda axis, count: [(axis, 1 << k) for k in range(count.bit_length() - 1)]
    wide, narrow = bits("wide", wide_count), bits("narrow", narrow_count)
    core, x_bits, z_bits = wide[:1], wide[1:2], wide[2:]
    return (
        core + x_bits + narrow + z_bits,
        core + narrow + x_bits + z_bits,
        core + z_bits + x_bits + narrow,
    )


def halvings(order, rows, columns):
    plan = []
    for _ in order:
        if columns % 256 == 0:
            columns //= 2
            plan.append("columns")
        elif rows % 32 == 0:
            rows //= 2
            plan.append("rows")
        else:
            plan.append("whole")
    return plan


def reduce_kernel(*refs, orders, width, places):
    n_in = len(places)
    ins, refs = refs[:n_in], refs[n_in:]
    small_ref, out_ref, small_out, total, result, small_send, small_recv = refs[:7]
    refs = refs[7:]
    parts, stages = len(orders), len(orders[0])
    outgoing = [refs[p * stages : (p + 1) * stages] for p in range(parts)]
    incoming = [refs[(parts + p) * stages : (parts + p + 1) * stages] for p in range(parts)]
    send_sem, recv_sem, back_send, back_recv, small_sems, small_rsems = refs[2 * parts * stages :]
    index = {axis: lax.axis_index(axis) for axis in ("wide", "narrow")}
    rows = total.shape[0]

    def own_bit(axis, bit):
        return lax.rem(index[axis] // bit, 2)

    def partner(axis, bit):
        return {axis: index[axis] + bit - 2 * bit * own_bit(axis, bit)}

    barrier = pltpu.get_barrier_semaphore()
    for axis, bit in orders[0]:
        pl.semaphore_signal(barrier, inc=1, device_id=partner(axis, bit), device_id_type=MESH)
    pl.semaphore_wait(barrier, stages)

    for ref, place in zip(ins, places):
        total[:, place : place + ref.shape[1]] = ref[...]
    small_send[0] = small_ref[...]

    regions = [[(0, rows, p * width, width)] for p in range(parts)]

    def take(region):
        row, height, column, span = region
        if not isinstance(row, int):
            row = pl.multiple_of(row, 16)
        if not isinstance(column, int):
            column = pl.multiple_of(column, 128)
        return pl.ds(row, height), pl.ds(column, span)

    def half(region, how, pick):
        row, height, column, span = region
        if how == "columns":
            return row, height, column + pick * (span // 2), span // 2
        if how == "rows":
            return row + pick * (height // 2), height // 2, column, span
        return region

    plans = [halvings(order, rows, width) for order in orders]

    def there(p, s):
        axis, bit = orders[p][s]
        return pltpu.make_async_remote_copy(
            src_ref=outgoing[p][s],
            dst_ref=incoming[p][s],
            send_sem=send_sem.at[p, s],
            recv_sem=recv_sem.at[p, s],
            device_id=partner(axis, bit),
            device_id_type=MESH,
        )

    def small_there(s):
        axis, bit = orders[0][s]
        return pltpu.make_async_remote_copy(
            src_ref=small_send.at[s],
            dst_ref=small_recv.at[s],
            send_sem=small_sems.at[s],
            recv_sem=small_rsems.at[s],
            device_id=partner(axis, bit),
            device_id_type=MESH,
        )

    def launch(p, s):
        axis, bit = orders[p][s]
        mine = own_bit(axis, bit)
        region, how = regions[p][-1], plans[p][s]
        outgoing[p][s][...] = total[take(half(region, how, 1 - mine))].astype(LOW)
        there(p, s).start()
        regions[p].append(half(region, how, mine))

    for p in range(parts):
        launch(p, 0)
    small_there(0).start()
    for s in range(stages):
        for p in range(parts):
            there(p, s).wait()
            kept = take(regions[p][-1])
            base = outgoing[p][s][...].astype(F32) if plans[p][s] == "whole" else total[kept]
            value = base + incoming[p][s][...].astype(F32)
            if s + 1 < stages:
                total[kept] = value
                launch(p, s + 1)
            else:
                result[kept] = value.astype(LOW)
        small_there(s).wait()
        fresh = small_send[s] + small_recv[s]
        if s + 1 < stages:
            small_send[s + 1] = fresh
            small_there(s + 1).start()
        else:
            small_out[...] = fresh

    def back(p, s):
        axis, bit = orders[p][s]
        spot = take(regions[p][s + 1])
        return pltpu.make_async_remote_copy(
            src_ref=result.at[spot],
            dst_ref=result.at[spot],
            send_sem=back_send.at[p, s],
            recv_sem=back_recv.at[p, s],
            device_id=partner(axis, bit),
            device_id_type=MESH,
        )

    for s in reversed(range(stages)):
        for p in range(parts):
            if plans[p][s] != "whole":
                back(p, s).start()
        for p in range(parts):
            if plans[p][s] != "whole":
                back(p, s).wait()
    out_ref[...] = result[...]


def reduce_everywhere(big, small, cid):
    orders = reduce_orders(lax.axis_size("wide"), lax.axis_size("narrow"))
    places, columns = [], 0
    for array in big:
        places.append(columns)
        columns += array.shape[1]
    rows = big[0].shape[0]
    width, parts, stages = columns // len(orders), len(orders), len(orders[0])
    buffers = []
    for order in orders:
        height, span = rows, width
        for how in halvings(order, rows, width):
            height, span = (height // 2 if how == "rows" else height), (span // 2 if how == "columns" else span)
            buffers.append(pltpu.VMEM((height, span), LOW))
    vmem = pl.BlockSpec(memory_space=pltpu.VMEM)
    return pl.pallas_call(
        functools.partial(reduce_kernel, orders=orders, width=width, places=places),
        in_specs=[vmem] * (len(big) + 1),
        out_specs=[vmem, vmem],
        out_shape=[jax.ShapeDtypeStruct((rows, columns), LOW), jax.ShapeDtypeStruct(small.shape, F32)],
        scratch_shapes=[
            pltpu.VMEM((rows, columns), F32),
            pltpu.VMEM((rows, columns), LOW),
            pltpu.VMEM((stages, *small.shape), F32),
            pltpu.VMEM((stages, *small.shape), F32),
        ]
        + buffers
        + buffers
        + [pltpu.SemaphoreType.DMA((parts, stages))] * 4
        + [pltpu.SemaphoreType.DMA((stages,))] * 2,
        compiler_params=pltpu.CompilerParams(
            vmem_limit_bytes=VMEM_BYTES, collective_id=cid, has_side_effects=True
        ),
        cost_estimate=pl.CostEstimate(flops=10**9, bytes_accessed=20 * 2**20, transcendentals=0),
        name="reduce_everywhere",
    )(*big, small)


def join_kernel(own_ref, far_ref, out_ref):
    value = own_ref[...]
    for j in range(far_ref.shape[0]):
        value += far_ref[j].astype(F32)
    out_ref[0] = value


def join(own, fars, along):
    tiles = len(fars)
    spread = fars[0].shape[0]
    shape = list(own.shape)
    shape[along] //= tiles

    def kernel(own_ref, *rest):
        far_refs, out_ref = rest[:tiles], rest[tiles]
        for t in range(tiles):

            @pl.when(pl.program_id(0) == t)
            def _():
                join_kernel(own_ref, far_refs[t], out_ref)

    place = (lambda t: (0, t)) if along == 1 else (lambda t: (t, 0))
    return pl.pallas_call(
        kernel,
        grid=(tiles,),
        in_specs=[pl.BlockSpec(tuple(shape), place)]
        + [pl.BlockSpec((spread, *shape), lambda t: (0, 0, 0), pipeline_mode=pl.Buffered(1))] * tiles,
        out_specs=pl.BlockSpec((1, *shape), lambda t: (0, *place(t))),
        out_shape=jax.ShapeDtypeStruct((1, *own.shape), F32),
        compiler_params=pltpu.CompilerParams(vmem_limit_bytes=VMEM_BYTES),
        cost_estimate=pl.CostEstimate(flops=10**7, bytes_accessed=12 * 2**20, transcendentals=0),
        name="join",
    )(own, *fars)


def attention_forward_kernel(q_ref, k_ref, v_ref, mixed_ref, soft_ref, inv_ref, *, rows):
    lane = lax.broadcasted_iota(jnp.int32, (1, PAIR), 1)
    keys, values = k_ref[...], v_ref[...]
    none = jnp.zeros_like(keys)
    for block in range(LENGTH // rows):
        part = slice(block * rows, (block + 1) * rows)
        query = q_ref[part, :] * LOW(HEAD_DIM**-0.5)
        mixed, inverses = None, []
        for head in range(2):
            mine = (lane < HEAD_DIM) if head == 0 else (lane >= HEAD_DIM)
            scores = dot(query, jnp.where(mine, keys, none), NT)
            top = jnp.max(scores, axis=1, keepdims=True)
            weights = jnp.exp(scores - top)
            inverse = 1.0 / jnp.sum(weights, axis=1, keepdims=True)
            weights = weights.astype(LOW)
            soft_ref[head, part, :] = weights
            inverses.append(jnp.broadcast_to(inverse, (rows, PAIR)))
            term = dot(weights, jnp.where(mine, values, none)) * inverse
            mixed = term if mixed is None else mixed + term
        mixed_ref[part, :] = mixed.astype(LOW)
        inv_ref[part, :] = jnp.where(lane < HEAD_DIM, inverses[0], inverses[1])


def attention_forward(qkv_rows, moves, pushes, cid):
    pairs = D // PAIR
    columns = lambda first: pl.BlockSpec((LENGTH, PAIR), lambda i: (0, first + i))
    return call_with_moves(
        functools.partial(attention_forward_kernel, rows=512),
        moves,
        pushes,
        cid,
        grid=(pairs,),
        in_specs=[columns(0), columns(pairs), columns(2 * pairs)],
        out_specs=[columns(0), pl.BlockSpec((2, LENGTH, LENGTH), lambda i: (i, 0, 0)), columns(0)],
        out_shape=[
            jax.ShapeDtypeStruct((LENGTH, D), LOW),
            jax.ShapeDtypeStruct((HEADS, LENGTH, LENGTH), LOW),
            jax.ShapeDtypeStruct((LENGTH, D), F32),
        ],
        cost=pl.CostEstimate(
            flops=20 * 10**9, bytes_accessed=30 * 2**20, transcendentals=HEADS * LENGTH * LENGTH
        ),
        name="attention_forward",
        args=(qkv_rows, qkv_rows, qkv_rows),
    )


def attention_backward_kernel(
    q_ref, k_ref, v_ref, grad_ref, mixed_ref, soft_ref, inv_ref, dq_ref, dk_ref, dv_ref, *, rows
):
    lane = lax.broadcasted_iota(jnp.int32, (1, PAIR), 1)
    scale = LOW(HEAD_DIM**-0.5)
    keys, values = k_ref[...], v_ref[...]
    none = jnp.zeros_like(keys)
    dk_parts, dv_parts = [None, None], [None, None]
    for block in range(LENGTH // rows):
        part = slice(block * rows, (block + 1) * rows)
        query_t = (q_ref[part, :] * scale).T
        scaled = grad_ref[part, :].astype(F32) * inv_ref[part, :]
        inner = scaled * mixed_ref[part, :].astype(F32)
        scaled = scaled.astype(LOW)
        scaled_t = scaled.T
        grad_query = None
        for head in range(2):
            mine = (lane < HEAD_DIM) if head == 0 else (lane >= HEAD_DIM)
            own = slice(head * HEAD_DIM, (head + 1) * HEAD_DIM)
            weights = soft_ref[head, part, :]
            grad_soft = dot(scaled, jnp.where(mine, values, none), NT)
            centre = jnp.sum(jnp.where(mine, inner, 0.0), axis=1, keepdims=True)
            grad_scores = (weights.astype(F32) * (grad_soft - centre)).astype(LOW)
            term = dot(grad_scores, jnp.where(mine, keys, none))
            grad_query = term if grad_query is None else grad_query + term
            dk = dot(query_t[own, :], grad_scores)
            dv = dot(scaled_t[own, :], weights)
            dk_parts[head] = dk if dk_parts[head] is None else dk_parts[head] + dk
            dv_parts[head] = dv if dv_parts[head] is None else dv_parts[head] + dv
        dq_ref[part, :] = (grad_query * HEAD_DIM**-0.5).astype(LOW)
    dk_ref[...] = jnp.concatenate(dk_parts, axis=0).T.astype(LOW)
    dv_ref[...] = jnp.concatenate(dv_parts, axis=0).T.astype(LOW)


def attention_backward(qkv_rows, grad_mixed, mixed_rows, soft, inverses, moves, pushes, cid):
    pairs = D // PAIR
    columns = lambda first: pl.BlockSpec((LENGTH, PAIR), lambda i: (0, first + i))
    return call_with_moves(
        functools.partial(attention_backward_kernel, rows=512),
        moves,
        pushes,
        cid,
        grid=(pairs,),
        in_specs=[
            columns(0),
            columns(pairs),
            columns(2 * pairs),
            columns(0),
            columns(0),
            pl.BlockSpec((2, LENGTH, LENGTH), lambda i: (i, 0, 0)),
            columns(0),
        ],
        out_specs=[columns(0)] * 3,
        out_shape=[jax.ShapeDtypeStruct((LENGTH, D), LOW)] * 3,
        cost=pl.CostEstimate(flops=25 * 10**9, bytes_accessed=36 * 2**20, transcendentals=0),
        name="attention_backward",
        args=(qkv_rows, qkv_rows, qkv_rows, grad_mixed, mixed_rows, soft, inverses),
    )


def gelu_and_slope(values):
    ratio = 1.0 / (1.0 + jnp.abs(values) * (0.3275911 * 0.7071067811865476))
    bell = jnp.exp(values * values * -0.5)
    series = 0.5 * 1.061405429
    for factor in (-1.453152027, 1.421413741, -0.284496736, 0.254829592):
        series = series * ratio + 0.5 * factor
    tail = series * ratio * bell
    below = jnp.where(values >= 0.0, 1.0 - tail, tail)
    return values * below, below + values * bell * 0.3989422804014327


def diagonal(slot_cap):
    shape = (slot_cap, 128)
    return lax.broadcasted_iota(jnp.int32, shape, 0) == lax.broadcasted_iota(jnp.int32, shape, 1)


def expert_kernel(*refs, more, last, per, steps, slot_cap):
    rows_ref, cot_ref, gate_ref, own_in, own_outer = refs[:5]
    far_in, far_outer = refs[5 : 5 + per], refs[5 + per : 5 + 2 * per]
    refs = refs[5 + 2 * per :]
    if more:
        old_in, old_outer = refs[:2]
        refs = refs[2:]
    result_ref, sent_ref, dots_ref, din_ref, douter_ref = refs[:5]
    refs = refs[5:]
    if last:
        far_din, far_douter = refs[:2]
        refs = refs[2:]
    grad_sc, rows_t, acc_result, acc_sent, first_buf, second_buf, sems = refs
    step = pl.program_id(0)
    slot = lax.rem(step, 2)
    sources = rows_ref.shape[0] // slot_cap
    tile = first_buf.shape[2]

    def fetch(i):
        if i < per:
            first = own_in.at[:, i * tile : (i + 1) * tile]
            second = own_outer.at[i * tile : (i + 1) * tile, :]
        else:
            first, second = far_in[i % per].at[i // per - 1], far_outer[i % per].at[i // per - 1]
        return (
            pltpu.make_async_copy(first, first_buf.at[i % 2], sems.at[0, i % 2]),
            pltpu.make_async_copy(second, second_buf.at[i % 2], sems.at[1, i % 2]),
        )

    @pl.when(step == 0)
    def _():
        for copy in fetch(0):
            copy.start()
        for w in range(sources):
            part = slice(w * slot_cap, (w + 1) * slot_cap)
            gate = jnp.sum(jnp.where(diagonal(slot_cap), gate_ref[w, 0:1, :], 0.0), axis=1, keepdims=True)
            grad_sc[part, :] = (cot_ref[part, :].astype(F32) * gate).astype(LOW)
        rows_t[...] = rows_ref[...].T
        acc_result[...] = jnp.zeros_like(acc_result)
        acc_sent[...] = jnp.zeros_like(acc_sent)

    for i in range(steps):

        @pl.when(step == i)
        def _():
            for copy in fetch(i):
                copy.wait()
            if i + 1 < steps:
                for copy in fetch(i + 1):
                    copy.start()

    first, second = first_buf[slot], second_buf[slot]
    hidden, slope = gelu_and_slope(dot(rows_ref[...], first))
    hidden = hidden.astype(LOW)
    grad_rows = grad_sc[...]
    grad_pre = (dot(grad_rows, second, NT) * slope).astype(LOW)
    acc_result[...] += dot(hidden, second)
    acc_sent[...] += dot(grad_pre, first, NT)
    din = dot(rows_t[...], grad_pre)
    douter = dot(hidden, grad_rows, TN)
    if more:
        din += old_in[...]
        douter += old_outer[...]
    if not last:
        din_ref[...] = din
        douter_ref[...] = douter
    else:

        @pl.when(step < per)
        def _():
            din_ref[...] = din
            douter_ref[...] = douter

        @pl.when(step >= per)
        def _():
            far_din[...] = din.astype(LOW)
            far_douter[...] = douter.astype(LOW)

    @pl.when(step == steps - 1)
    def _():
        result = acc_result[...].astype(LOW)
        result_ref[...] = result
        sent_ref[...] = acc_sent[...].astype(LOW)
        for w in range(sources):
            part = slice(w * slot_cap, (w + 1) * slot_cap)
            products = cot_ref[part, :].astype(F32) * result[part, :].astype(F32)
            column = jnp.sum(products, axis=1, keepdims=True)
            row = jnp.sum(jnp.where(diagonal(slot_cap), column, 0.0), axis=0, keepdims=True)
            dots_ref[w] = jnp.broadcast_to(row, (8, 128))


def tile_of(units):
    return min(512, units)


def expert_stage(rows, cot, gates, weights, old, last, slot_cap, moves, pushes, cid):
    own_in, own_outer, far_in, far_outer = weights
    width, units = own_in.shape
    count = lax.axis_size("narrow")
    height = rows.shape[0]
    tile = tile_of(units)
    per = units // tile
    steps = count * per
    whole = lambda shape: pl.BlockSpec(shape, lambda i: (0,) * len(shape))
    anywhere = pl.BlockSpec(memory_space=pl.ANY)
    din_spec = pl.BlockSpec((None, width, tile), lambda i: (i, 0, 0))
    douter_spec = pl.BlockSpec((None, tile, width), lambda i: (i, 0, 0))
    out_specs = [whole((height, width)), whole((height, width)), whole(gates.shape)]
    out_shape = [
        jax.ShapeDtypeStruct((height, width), LOW),
        jax.ShapeDtypeStruct((height, width), LOW),
        jax.ShapeDtypeStruct(gates.shape, F32),
    ]
    if last:
        near = lambda i: jnp.minimum(i, per - 1)
        away = lambda i: jnp.maximum(i - per, 0)
        out_specs += [
            pl.BlockSpec((width, tile), lambda i: (0, near(i))),
            pl.BlockSpec((tile, width), lambda i: (near(i), 0)),
            pl.BlockSpec((None, width, tile), lambda i: (away(i), 0, 0)),
            pl.BlockSpec((None, tile, width), lambda i: (away(i), 0, 0)),
        ]
        out_shape += [
            jax.ShapeDtypeStruct((width, units), F32),
            jax.ShapeDtypeStruct((units, width), F32),
            jax.ShapeDtypeStruct((steps - per, width, tile), LOW),
            jax.ShapeDtypeStruct((steps - per, tile, width), LOW),
        ]
    else:
        out_specs += [din_spec, douter_spec]
        out_shape += [
            jax.ShapeDtypeStruct((steps, width, tile), F32),
            jax.ShapeDtypeStruct((steps, tile, width), F32),
        ]
    return call_with_moves(
        functools.partial(
            expert_kernel, more=bool(old), last=last, per=per, steps=steps, slot_cap=slot_cap
        ),
        moves,
        pushes,
        cid,
        grid=(steps,),
        in_specs=[whole((height, width)), whole((height, width)), whole(gates.shape)]
        + [anywhere] * (2 + 2 * per)
        + ([din_spec, douter_spec] if old else []),
        out_specs=out_specs,
        out_shape=out_shape,
        scratch_shapes=[
            pltpu.VMEM((height, width), LOW),
            pltpu.VMEM((width, height), LOW),
            pltpu.VMEM((height, width), F32),
            pltpu.VMEM((height, width), F32),
            pltpu.VMEM((2, width, tile), LOW),
            pltpu.VMEM((2, tile, width), LOW),
            pltpu.SemaphoreType.DMA((2, 2)),
        ],
        cost=pl.CostEstimate(
            flops=12 * height * width * units * count, bytes_accessed=34 * 2**20, transcendentals=0
        ),
        name="expert_stage",
        args=(rows, cot, gates, own_in, own_outer, *far_in, *far_outer, *old),
    )


def local(
    tokens,
    grad_out,
    route_ids,
    slot_ids,
    keep_ids,
    gain_one,
    w_query,
    w_key,
    w_value,
    w_out,
    gain_two,
    w_route,
    embed,
    w_in,
    w_outer,
):
    micro_count, tok_count, feat_width = tokens.shape
    narrow_count = lax.axis_size("narrow")
    expert_count = embed.shape[0]
    slot_cap = max(2, tok_count // expert_count)
    slots = expert_count * slot_cap
    w_qkv = jnp.concatenate([w_query, w_key, w_value], axis=1)
    route_float = w_route.astype(F32)
    own_in, own_outer = w_in[0], w_outer[0]
    units = own_in.shape[1]
    tile = tile_of(units)
    per = units // tile
    weight_pushes = [
        (own_in, lambda ref, j, t=t: ref.at[:, t * tile : (t + 1) * tile], (feat_width, tile)) for t in range(per)
    ] + [
        (own_outer, lambda ref, j, t=t: ref.at[t * tile : (t + 1) * tile, :], (tile, feat_width)) for t in range(per)
    ]
    early = len(weight_pushes) // 3
    slot_columns = jnp.arange(slots, dtype=jnp.int32)

    def boxes(rows):
        return rows.reshape((expert_count, slot_cap) + rows.shape[1:])

    def flat(boxed):
        return boxed.reshape((expert_count * slot_cap,) + boxed.shape[2:])

    tables, cot_boxes = [], []
    for m in range(micro_count):
        slot_index = jnp.where(keep_ids[m] > 0, route_ids[m] * slot_cap + slot_ids[m], -1)
        table = (slot_index[:, None] == slot_columns[None, :]).astype(LOW)
        tables.append(table)
        cot_boxes.append(boxes(dot(table, grad_out[m], TN).astype(LOW)))

    ahead, send = [], []
    for m in range(micro_count):
        inputs = tokens[m].astype(F32)
        normed_one, pull_one = jax.vjp(layer_norm, inputs, gain_one)
        normed_low = normed_one.astype(LOW)
        qkv_rows = dot(normed_low, w_qkv).astype(LOW)
        if m == 0:
            (mixed_rows, soft, inverses), (cot_0,), far_a = attention_forward(
                qkv_rows, (cot_boxes[0],), weight_pushes[:early], 1
            )
        else:
            (mixed_rows, soft, inverses), (sent_0, gates_0, cot_1), far_b = attention_forward(
                qkv_rows, (*send[0], cot_boxes[1]), weight_pushes[early:], 2
            )
        first_sum = inputs + dot(mixed_rows, w_out)
        normed_two, pull_two = jax.vjp(layer_norm, first_sum, gain_two)
        second_low = normed_two.astype(LOW)
        projected = dot(second_low, w_route)
        gate_prob, pull_gate = jax.vjp(
            lambda proj_in, embed_in: gate_from(proj_in, embed_in, route_ids[m]), projected, embed
        )
        gates = jnp.sum(tables[m].astype(F32) * gate_prob[:, None], axis=0)
        gates = jnp.pad(gates.reshape(expert_count, 1, slot_cap), ((0, 0), (0, 7), (0, 128 - slot_cap)))
        send.append((boxes(dot(tables[m], second_low, TN).astype(LOW)), gates))
        ahead.append(
            (normed_low, pull_one, qkv_rows, mixed_rows, soft, inverses, first_sum, pull_two,
             second_low, gate_prob, pull_gate)
        )

    far = [*far_a, *far_b]
    weights = (own_in, own_outer, far[:per], far[per:])
    (result_0, grad_0, dots_0, *old), (sent_1, gates_1), _ = expert_stage(
        flat(sent_0), flat(cot_0), gates_0, weights, (), False, slot_cap, send[1], (), 3
    )
    (result_1, grad_1, dots_1, near_din, near_douter, far_din, far_douter), (home_grad_0, home_dots_0), _ = expert_stage(
        flat(sent_1), flat(cot_1), gates_1, weights, tuple(old), True, slot_cap, (boxes(grad_0), dots_0), (), 4
    )
    grad_pushes = [
        (far_din, lambda ref, j, t=t: ref.at[j * per + t], (feat_width, tile)) for t in range(per)
    ] + [
        (far_douter, lambda ref, j, t=t: ref.at[j * per + t], (tile, feat_width)) for t in range(per)
    ]
    later = len(grad_pushes) - early

    input_grads, sums = [], None
    for m in range(micro_count):
        (normed_low, pull_one, qkv_rows, mixed_rows, soft, inverses, first_sum, pull_two,
         second_low, gate_prob, pull_gate) = ahead[m]
        home_grad, home_dots = (home_grad_0, home_dots_0) if m == 0 else (home_grad_1, home_dots_1)
        table = tables[m]
        grad_sum = grad_out[m].astype(F32)
        slot_dots = home_dots[:, 0, :slot_cap].reshape(slots)
        grad_gate = jnp.sum(table.astype(F32) * slot_dots[None, :], axis=-1)
        grad_projected, grad_embed = pull_gate(grad_gate)
        grad_second = dot(table, flat(home_grad)) + dot(
            grad_projected, route_float, NT, lax.Precision.HIGHEST
        )
        grad_route = dot(second_low.astype(F32), grad_projected, TN, lax.Precision.HIGHEST)
        grad_first_norm, grad_gain_two = pull_two(grad_second)
        grad_first = grad_sum + grad_first_norm
        grad_branch = grad_first.astype(LOW)
        grad_wo = dot(mixed_rows, grad_branch, TN)
        grad_mixed = dot(grad_branch, w_out, NT).astype(LOW)
        if m == 0:
            grads, (home_grad_1, home_dots_1, home_result_0), got_a = attention_backward(
                qkv_rows, grad_mixed, mixed_rows, soft, inverses,
                (boxes(grad_1), dots_1, boxes(result_0)), grad_pushes[:later], 5
            )
        else:
            grads, (home_result_1,), got_b = attention_backward(
                qkv_rows, grad_mixed, mixed_rows, soft, inverses, (boxes(result_1),), grad_pushes[later:], 6
            )
        grad_qkv = jnp.concatenate(grads, axis=1)
        grad_wqkv = dot(normed_low, grad_qkv, TN)
        grad_input_norm, grad_gain_one = pull_one(dot(grad_qkv, w_qkv, NT))
        input_grads.append((grad_first + grad_input_norm).astype(LOW))
        terms = (grad_gain_one, grad_wqkv, grad_wo, grad_gain_two, grad_route, grad_embed)
        sums = terms if sums is None else tuple(a + b for a, b in zip(sums, terms))
    outputs = []
    for m, home_result in enumerate((home_result_0, home_result_1)):
        first_sum, gate_prob = ahead[m][6], ahead[m][9]
        returned = dot(tables[m], flat(home_result))
        outputs.append((first_sum + gate_prob[:, None] * returned).astype(LOW))
    gain_one_sum, wqkv_sum, wo_sum, gain_two_sum, route_sum, embed_sum = sums
    router_dim = route_sum.shape[1]
    small = jnp.concatenate(
        [
            route_sum.T,
            gain_one_sum[None],
            gain_two_sum[None],
            jnp.pad(embed_sum.reshape(1, -1), ((0, 0), (0, feat_width - embed_sum.size))),
            jnp.zeros((-(router_dim + 3) % 8, feat_width), F32),
        ],
        axis=0,
    )
    big, small = reduce_everywhere((wqkv_sum, wo_sum), small, 7)
    big = [big[:, k * feat_width : (k + 1) * feat_width].astype(F32) for k in range(4)]
    got = [*got_a, *got_b]
    return (
        jnp.stack(outputs),
        jnp.stack(input_grads),
        small[router_dim],
        *big,
        small[router_dim + 1],
        small[:router_dim].T,
        small[router_dim + 2, : embed.size].reshape(embed.shape),
        join(near_din, got[:per], 1),
        join(near_douter, got[per:], 0),
    )


def solution(mesh):
    tokens_spec = P(None, ("wide", "narrow"), None)
    ids_spec = P(None, ("wide", "narrow"))
    in_spec, outer_spec = P("wide", None, "narrow"), P("wide", "narrow", None)
    return jax.shard_map(
        local,
        mesh=mesh,
        in_specs=(tokens_spec,) * 2 + (ids_spec,) * 3 + (P(),) * 8 + (in_spec, outer_spec),
        out_specs=(tokens_spec,) * 2 + (P(),) * 8 + (in_spec, outer_spec),
        check_vma=False,
    )
```

```python
import functools

import jax
import jax.numpy as jnp
from jax import lax
from jax.experimental import pallas as pl
from jax.experimental.pallas import tpu as pltpu
from jax.sharding import PartitionSpec as P

D = 768
HEADS = 12
HEAD_DIM = 64
LENGTH = 1024
PAIR = 2 * HEAD_DIM
GROUP = 4
NN = (((1,), (0,)), ((), ()))
NT = (((1,), (1,)), ((), ()))
TN = (((0,), (0,)), ((), ()))
LOW = jnp.bfloat16
F32 = jnp.float32
VMEM_BYTES = 60 << 20


def dot(left, right, dims=NN, precise=None):
    return lax.dot_general(left, right, dims, precision=precise, preferred_element_type=F32)


def normalise(values):
    centred = values - jnp.mean(values, axis=-1, keepdims=True)
    inverse = lax.rsqrt(jnp.mean(centred * centred, axis=-1, keepdims=True) + 1e-05)
    return centred * inverse, inverse


def normalise_back(grad, normed, inverse):
    return inverse * (
        grad
        - jnp.mean(grad, axis=-1, keepdims=True)
        - normed * jnp.mean(grad * normed, axis=-1, keepdims=True)
    )


def three_parts(values):
    high = values.astype(LOW)
    rest = values - high.astype(F32)
    middle = rest.astype(LOW)
    return high, middle, (rest - middle.astype(F32)).astype(LOW)


def spread_parts(column):
    lane = lax.broadcasted_iota(jnp.int32, (1, 128), 1)
    high, middle, low = (part.astype(F32) for part in three_parts(column))
    return jnp.where(lane == 0, high, jnp.where(lane == 1, middle, jnp.where(lane == 2, low, 0.0))).astype(LOW)


def diagonal(rows):
    shape = (rows, 128)
    return lax.broadcasted_iota(jnp.int32, shape, 0) == lax.broadcasted_iota(jnp.int32, shape, 1)


def to_column(row):
    pieces = [
        jnp.sum(jnp.where(diagonal(128), row[:, first : first + 128], 0.0), axis=1, keepdims=True)
        for first in range(0, row.shape[1], 128)
    ]
    return jnp.concatenate(pieces, axis=0)


def unit_length(rows):
    inverse = lax.rsqrt(jnp.sum(rows * rows, axis=-1, keepdims=True) + 1.0)
    return rows * inverse, inverse


def route_probs(projected, embed_rows, route_column):
    unit, inverse = unit_length(projected)
    anchor, anchor_inverse = unit_length(embed_rows)
    logits = 3.0 * dot(unit, anchor, NT, lax.Precision.HIGHEST)
    weights = jnp.exp(logits - jnp.max(logits, axis=-1, keepdims=True))
    probs = weights / jnp.sum(weights, axis=-1, keepdims=True)
    lane = lax.broadcasted_iota(jnp.int32, (1, probs.shape[1]), 1)
    picked = route_column == lane
    gate = jnp.sum(jnp.where(picked, probs, 0.0), axis=-1, keepdims=True)
    return unit, inverse, anchor, anchor_inverse, probs, picked, gate


def slot_rows(slot_row, first, count):
    slot = lax.broadcasted_iota(jnp.int32, (count, slot_row.shape[1]), 0) + first
    return jnp.where(slot == slot_row, 1.0, 0.0).astype(LOW)


def token_rows(slot_column, slots):
    lane = lax.broadcasted_iota(jnp.int32, (slot_column.shape[0], slots), 1)
    return jnp.where(lane == slot_column, 1.0, 0.0).astype(LOW)


MESH = pl.DeviceIdType.MESH


def call_with_moves(
    body, moves, pushes, cid, *, grid, in_specs, out_specs, out_shape, scratch_shapes=(), cost, name, args
):
    members, spread = lax.axis_size("wide"), lax.axis_size("narrow")
    n_in, n_out, n_moves, n_scratch = len(in_specs), len(out_specs), len(moves), len(scratch_shapes)
    arrays = []
    for array, _, _ in pushes:
        if not any(array is known for known in arrays):
            arrays.append(array)
    which = [next(k for k, known in enumerate(arrays) if known is array) for array, _, _ in pushes]
    n_arrays, n_pushes = len(arrays), len(pushes)

    def kernel(*refs):
        ins, refs = refs[:n_in], refs[n_in:]
        sources, refs = refs[:n_moves], refs[n_moves:]
        pushed, refs = refs[:n_arrays], refs[n_arrays:]
        outs, refs = refs[:n_out], refs[n_out:]
        targets, refs = refs[:n_moves], refs[n_moves:]
        landings, refs = refs[:n_pushes], refs[n_pushes:]
        scratch, refs = refs[:n_scratch], refs[n_scratch:]
        stages, refs = refs[:n_moves], refs[n_moves:]
        send_sem, recv_sem, own_sem, push_send, push_recv = refs
        me, side = lax.axis_index("wide"), lax.axis_index("narrow")
        step = pl.program_id(0)

        def remote(i, d):
            peer = lax.rem(me + d, members)
            return pltpu.make_async_remote_copy(
                src_ref=sources[i].at[peer],
                dst_ref=targets[i].at[me],
                send_sem=send_sem.at[i, d],
                recv_sem=recv_sem.at[i, d],
                device_id={"wide": peer},
                device_id_type=MESH,
            )

        def push(k, j):
            return pltpu.make_async_remote_copy(
                src_ref=pushes[k][1](pushed[which[k]], j),
                dst_ref=landings[k].at[j],
                send_sem=push_send.at[k, j],
                recv_sem=push_recv.at[k, j],
                device_id={"narrow": lax.rem(side + j + 1, spread)},
                device_id_type=MESH,
            )

        @pl.when(step == 0)
        def _():
            barrier = pltpu.get_barrier_semaphore()
            count = 0
            if n_moves:
                for d in range(1, members):
                    pl.semaphore_signal(
                        barrier, inc=1, device_id={"wide": lax.rem(me + d, members)}, device_id_type=MESH
                    )
                count += members - 1
            if n_pushes:
                for j in range(spread - 1):
                    pl.semaphore_signal(
                        barrier, inc=1, device_id={"narrow": lax.rem(side + j + 1, spread)}, device_id_type=MESH
                    )
                count += spread - 1
            pl.semaphore_wait(barrier, count)
            for k in range(n_pushes):
                for j in range(spread - 1):
                    push(k, j).start()
            for i in range(n_moves):
                for d in range(1, members):
                    remote(i, d).start()
                pltpu.make_async_copy(sources[i].at[me], stages[i], own_sem.at[i]).start()

        body(*ins, *outs, *scratch)

        @pl.when(step == grid[0] - 1)
        def _():
            for i in range(n_moves):
                pltpu.make_async_copy(sources[i].at[me], stages[i], own_sem.at[i]).wait()
                pltpu.make_async_copy(stages[i], targets[i].at[me], own_sem.at[i]).start()
            for i in range(n_moves):
                pltpu.make_async_copy(stages[i], targets[i].at[me], own_sem.at[i]).wait()
                for d in range(1, members):
                    remote(i, d).wait()
            for k in range(n_pushes):
                for j in range(spread - 1):
                    push(k, j).wait()

    anywhere = pl.BlockSpec(memory_space=pl.ANY)
    results = pl.pallas_call(
        kernel,
        grid=grid,
        in_specs=list(in_specs) + [anywhere] * (n_moves + n_arrays),
        out_specs=list(out_specs) + [anywhere] * (n_moves + n_pushes),
        out_shape=list(out_shape)
        + [jax.ShapeDtypeStruct(a.shape, a.dtype) for a in moves]
        + [jax.ShapeDtypeStruct((spread - 1, *shape), a.dtype) for a, _, shape in pushes],
        scratch_shapes=list(scratch_shapes)
        + [pltpu.VMEM(a.shape[1:], a.dtype) for a in moves]
        + [
            pltpu.SemaphoreType.DMA((max(1, n_moves), members)),
            pltpu.SemaphoreType.DMA((max(1, n_moves), members)),
            pltpu.SemaphoreType.DMA((max(1, n_moves),)),
            pltpu.SemaphoreType.DMA((max(1, n_pushes), spread)),
            pltpu.SemaphoreType.DMA((max(1, n_pushes), spread)),
        ],
        compiler_params=pltpu.CompilerParams(
            vmem_limit_bytes=VMEM_BYTES, collective_id=cid, has_side_effects=True
        ),
        cost_estimate=cost,
        name=name,
    )(*args, *moves, *arrays)
    return results[:n_out], results[n_out : n_out + n_moves], results[n_out + n_moves :]


def reduce_orders(wide_count, narrow_count):
    bits = lambda axis, count: [(axis, 1 << k) for k in range(count.bit_length() - 1)]
    wide, narrow = bits("wide", wide_count), bits("narrow", narrow_count)
    core, x_bits, z_bits = wide[:1], wide[1:2], wide[2:]
    return (
        core + x_bits + narrow + z_bits,
        core + narrow + x_bits + z_bits,
        core + z_bits + x_bits + narrow,
    )


def halvings(order, rows, columns):
    plan = []
    for _ in order:
        if columns % 256 == 0:
            columns //= 2
            plan.append("columns")
        elif rows % 32 == 0:
            rows //= 2
            plan.append("rows")
        else:
            plan.append("whole")
    return plan


def reduce_kernel(*refs, orders, width, places, sets):
    ins = [refs[k * sets : (k + 1) * sets] for k in range(len(places))]
    refs = refs[len(places) * sets :]
    smalls, refs = refs[:sets], refs[sets:]
    out_ref, small_out, total, result, small_send, small_recv = refs[:6]
    refs = refs[6:]
    parts, stages = len(orders), len(orders[0])
    outgoing = [refs[p * stages : (p + 1) * stages] for p in range(parts)]
    incoming = [refs[(parts + p) * stages : (parts + p + 1) * stages] for p in range(parts)]
    send_sem, recv_sem, back_send, back_recv, small_sems, small_rsems = refs[2 * parts * stages :]
    index = {axis: lax.axis_index(axis) for axis in ("wide", "narrow")}
    rows = total.shape[0]

    def own_bit(axis, bit):
        return lax.rem(index[axis] // bit, 2)

    def partner(axis, bit):
        return {axis: index[axis] + bit - 2 * bit * own_bit(axis, bit)}

    barrier = pltpu.get_barrier_semaphore()
    for axis, bit in orders[0]:
        pl.semaphore_signal(barrier, inc=1, device_id=partner(axis, bit), device_id_type=MESH)
    pl.semaphore_wait(barrier, stages)

    for group, place in zip(ins, places):
        total[:, place : place + group[0].shape[1]] = sum(ref[...].astype(F32) for ref in group)
    small_send[0] = sum(ref[...] for ref in smalls)

    regions = [[(0, rows, p * width, width)] for p in range(parts)]

    def take(region):
        row, height, column, span = region
        if not isinstance(row, int):
            row = pl.multiple_of(row, 16)
        if not isinstance(column, int):
            column = pl.multiple_of(column, 128)
        return pl.ds(row, height), pl.ds(column, span)

    def half(region, how, pick):
        row, height, column, span = region
        if how == "columns":
            return row, height, column + pick * (span // 2), span // 2
        if how == "rows":
            return row + pick * (height // 2), height // 2, column, span
        return region

    plans = [halvings(order, rows, width) for order in orders]

    def there(p, s):
        axis, bit = orders[p][s]
        return pltpu.make_async_remote_copy(
            src_ref=outgoing[p][s],
            dst_ref=incoming[p][s],
            send_sem=send_sem.at[p, s],
            recv_sem=recv_sem.at[p, s],
            device_id=partner(axis, bit),
            device_id_type=MESH,
        )

    def small_there(s):
        axis, bit = orders[0][s]
        return pltpu.make_async_remote_copy(
            src_ref=small_send.at[s],
            dst_ref=small_recv.at[s],
            send_sem=small_sems.at[s],
            recv_sem=small_rsems.at[s],
            device_id=partner(axis, bit),
            device_id_type=MESH,
        )

    def launch(p, s):
        axis, bit = orders[p][s]
        mine = own_bit(axis, bit)
        region, how = regions[p][-1], plans[p][s]
        outgoing[p][s][...] = total[take(half(region, how, 1 - mine))].astype(LOW)
        there(p, s).start()
        regions[p].append(half(region, how, mine))

    for p in range(parts):
        launch(p, 0)
    small_there(0).start()
    for s in range(stages):
        for p in range(parts):
            there(p, s).wait()
            kept = take(regions[p][-1])
            base = outgoing[p][s][...].astype(F32) if plans[p][s] == "whole" else total[kept]
            value = base + incoming[p][s][...].astype(F32)
            if s + 1 < stages:
                total[kept] = value
                launch(p, s + 1)
            else:
                result[kept] = value.astype(LOW)
        small_there(s).wait()
        fresh = small_send[s] + small_recv[s]
        if s + 1 < stages:
            small_send[s + 1] = fresh
            small_there(s + 1).start()
        else:
            small_out[...] = fresh

    def back(p, s):
        axis, bit = orders[p][s]
        spot = take(regions[p][s + 1])
        return pltpu.make_async_remote_copy(
            src_ref=result.at[spot],
            dst_ref=result.at[spot],
            send_sem=back_send.at[p, s],
            recv_sem=back_recv.at[p, s],
            device_id=partner(axis, bit),
            device_id_type=MESH,
        )

    for s in reversed(range(stages)):
        for p in range(parts):
            if plans[p][s] != "whole":
                back(p, s).start()
        for p in range(parts):
            if plans[p][s] != "whole":
                back(p, s).wait()
    out_ref[...] = result[...]


def reduce_everywhere(big, small, cid):
    orders = reduce_orders(lax.axis_size("wide"), lax.axis_size("narrow"))
    places, columns = [], 0
    for group in big:
        places.append(columns)
        columns += group[0].shape[1]
    rows = big[0][0].shape[0]
    sets = len(small)
    width, parts, stages = columns // len(orders), len(orders), len(orders[0])
    buffers = []
    for order in orders:
        height, span = rows, width
        for how in halvings(order, rows, width):
            height, span = (height // 2 if how == "rows" else height), (span // 2 if how == "columns" else span)
            buffers.append(pltpu.VMEM((height, span), LOW))
    vmem = pl.BlockSpec(memory_space=pltpu.VMEM)
    return pl.pallas_call(
        functools.partial(reduce_kernel, orders=orders, width=width, places=places, sets=sets),
        in_specs=[vmem] * ((len(big) + 1) * sets),
        out_specs=[vmem, vmem],
        out_shape=[jax.ShapeDtypeStruct((rows, columns), LOW), jax.ShapeDtypeStruct(small[0].shape, F32)],
        scratch_shapes=[
            pltpu.VMEM((rows, columns), F32),
            pltpu.VMEM((rows, columns), LOW),
            pltpu.VMEM((stages, *small[0].shape), F32),
            pltpu.VMEM((stages, *small[0].shape), F32),
        ]
        + buffers
        + buffers
        + [pltpu.SemaphoreType.DMA((parts, stages))] * 4
        + [pltpu.SemaphoreType.DMA((stages,))] * 2,
        compiler_params=pltpu.CompilerParams(
            vmem_limit_bytes=VMEM_BYTES, collective_id=cid, has_side_effects=True
        ),
        cost_estimate=pl.CostEstimate(flops=10**9, bytes_accessed=20 * 2**20, transcendentals=0),
        name="reduce_everywhere",
    )(*(array for group in big for array in group), *small)


def join_kernel(own_ref, far_ref, out_ref):
    value = own_ref[...]
    for j in range(far_ref.shape[0]):
        value += far_ref[j].astype(F32)
    out_ref[0] = value


def join(own, fars, along):
    tiles = len(fars)
    spread = fars[0].shape[0]
    shape = list(own.shape)
    shape[along] //= tiles

    def kernel(own_ref, *rest):
        far_refs, out_ref = rest[:tiles], rest[tiles]
        for t in range(tiles):

            @pl.when(pl.program_id(0) == t)
            def _():
                join_kernel(own_ref, far_refs[t], out_ref)

    place = (lambda t: (0, t)) if along == 1 else (lambda t: (t, 0))
    return pl.pallas_call(
        kernel,
        grid=(tiles,),
        in_specs=[pl.BlockSpec(tuple(shape), place)]
        + [pl.BlockSpec((spread, *shape), lambda t: (0, 0, 0), pipeline_mode=pl.Buffered(1))] * tiles,
        out_specs=pl.BlockSpec((1, *shape), lambda t: (0, *place(t))),
        out_shape=jax.ShapeDtypeStruct((1, *own.shape), F32),
        compiler_params=pltpu.CompilerParams(vmem_limit_bytes=VMEM_BYTES),
        cost_estimate=pl.CostEstimate(flops=10**7, bytes_accessed=12 * 2**20, transcendentals=0),
        name="join",
    )(own, *fars)


def attend_pair(query, keys, values, soft_ref, place, rows):
    lane = lax.broadcasted_iota(jnp.int32, (1, PAIR), 1)
    none = jnp.zeros_like(keys)
    mixed_blocks, inverse_blocks = [], []
    for block in range(LENGTH // rows):
        part = slice(block * rows, (block + 1) * rows)
        scaled = query[part, :] * LOW(HEAD_DIM**-0.5)
        mixed, inverses = None, []
        for head in range(2):
            mine = (lane < HEAD_DIM) if head == 0 else (lane >= HEAD_DIM)
            scores = dot(scaled, jnp.where(mine, keys, none), NT)
            top = jnp.max(scores, axis=1, keepdims=True)
            weights = jnp.exp(scores - top)
            inverse = 1.0 / jnp.sum(weights, axis=1, keepdims=True)
            weights = weights.astype(LOW)
            soft_ref[place + head, part, :] = weights
            inverses.append(jnp.broadcast_to(inverse, (rows, PAIR)))
            term = dot(weights, jnp.where(mine, values, none)) * inverse
            mixed = term if mixed is None else mixed + term
        mixed_blocks.append(mixed)
        inverse_blocks.append(jnp.where(lane < HEAD_DIM, inverses[0], inverses[1]))
    return jnp.concatenate(mixed_blocks, axis=0), jnp.concatenate(inverse_blocks, axis=0)


def forward_kernel(
    tokens_ref, gain_one_ref, wq_ref, wk_ref, wv_ref, wo_ref, gain_two_ref, route_ref, embed_ref, slot_ref, id_ref,
    q_ref, k_ref, v_ref, soft_ref, inv_ref, mixed_ref, first_ref, sent_ref, gates_ref, projected_ref,
    normed, total, *, steps, slots, slot_cap,
):
    step = pl.program_id(0)

    @pl.when(step == 0)
    def _():
        values = tokens_ref[...].astype(F32)
        normed[...] = (normalise(values)[0] * gain_one_ref[...]).astype(LOW)
        total[...] = values

    rows = normed[...]
    q_ref[...] = dot(rows, wq_ref[...]).astype(LOW)
    k_ref[...] = dot(rows, wk_ref[...]).astype(LOW)
    v_ref[...] = dot(rows, wv_ref[...]).astype(LOW)
    for pair in range(GROUP // 2):
        lanes = slice(pair * PAIR, (pair + 1) * PAIR)
        mixed, inverse = attend_pair(q_ref[:, lanes], k_ref[:, lanes], v_ref[:, lanes], soft_ref, 2 * pair, 512)
        mixed_ref[:, lanes] = mixed.astype(LOW)
        inv_ref[:, lanes] = inverse
    total[...] += dot(mixed_ref[...], wo_ref[...])

    @pl.when(step == steps - 1)
    def _():
        first = total[...]
        first_ref[...] = first
        second = (normalise(first)[0] * gain_two_ref[...]).astype(LOW)
        projected = dot(second, route_ref[...])
        projected_ref[...] = projected
        route_column = to_column(id_ref[...].astype(F32)).astype(jnp.int32)
        gate = route_probs(projected, embed_ref[...], route_column)[-1]
        parts = spread_parts(gate)
        slot_row = slot_ref[...]
        block = 256
        for begin in range(0, slots, block):
            table = slot_rows(slot_row, begin, block)
            sent_ref[begin : begin + block, :] = dot(table, second).astype(LOW)
            gathered = jnp.sum(dot(table, parts), axis=1, keepdims=True)
            for w in range(begin // slot_cap, (begin + block) // slot_cap):
                column = gathered[w * slot_cap - begin : (w + 1) * slot_cap - begin, :]
                row = jnp.sum(jnp.where(diagonal(slot_cap), column, 0.0), axis=0, keepdims=True)
                gates_ref[w] = jnp.broadcast_to(row, (8, 128))


def forward_stage(m, tokens, gains, weights, w_route, embed, slot_index, route_ids, slot_cap, moves, pushes, cid):
    tok_count, width = tokens.shape[1:]
    experts = embed.shape[0]
    slots = experts * slot_cap
    steps = HEADS // GROUP
    span = GROUP * HEAD_DIM
    one = pl.Buffered(1)
    fixed = lambda shape: pl.BlockSpec(shape, lambda i: (0,) * len(shape), pipeline_mode=one)
    of_m = lambda *shape: pl.BlockSpec((None, *shape), lambda i: (m, 0, 0), pipeline_mode=one)
    columns = lambda height: pl.BlockSpec((height, span), lambda i: (0, i))
    whole = lambda *shape: pl.BlockSpec(shape, lambda i: (0,) * len(shape))
    gain_one, gain_two = gains
    wq, wk, wv, wo = weights
    low = lambda *shape: jax.ShapeDtypeStruct(shape, LOW)
    full = lambda *shape: jax.ShapeDtypeStruct(shape, F32)
    return call_with_moves(
        functools.partial(forward_kernel, steps=steps, slots=slots, slot_cap=slot_cap),
        moves,
        pushes,
        cid,
        grid=(steps,),
        in_specs=[
            of_m(tok_count, width), fixed((1, width)), columns(width), columns(width), columns(width),
            pl.BlockSpec((span, width), lambda i: (i, 0)), fixed((1, width)), fixed(w_route.shape),
            fixed(embed.shape), of_m(1, tok_count), of_m(1, tok_count),
        ],
        out_specs=[
            columns(tok_count), columns(tok_count), columns(tok_count),
            pl.BlockSpec((GROUP, LENGTH, LENGTH), lambda i: (i, 0, 0)),
            columns(tok_count), columns(tok_count), whole(tok_count, width), whole(slots, width),
            whole(experts, 8, 128), whole(tok_count, w_route.shape[1]),
        ],
        out_shape=[
            low(tok_count, width), low(tok_count, width), low(tok_count, width), low(HEADS, LENGTH, LENGTH),
            full(tok_count, width), low(tok_count, width), full(tok_count, width), low(slots, width),
            full(experts, 8, 128), full(tok_count, w_route.shape[1]),
        ],
        scratch_shapes=[pltpu.VMEM((tok_count, width), LOW), pltpu.VMEM((tok_count, width), F32)],
        cost=pl.CostEstimate(
            flops=30 * 10**9, bytes_accessed=50 * 2**20, transcendentals=HEADS * LENGTH * LENGTH
        ),
        name="forward_stage",
        args=(tokens, gain_one, wq, wk, wv, wo, gain_two, w_route, embed, slot_index, route_ids),
    )


def dispatch_kernel(slot_ref, rows_ref, *out_refs, slots):
    for m, out_ref in enumerate(out_refs):

        @pl.when(pl.program_id(0) == m)
        def _():
            for begin in range(0, slots, 256):
                table = slot_rows(slot_ref[...], begin, 256)
                out_ref[begin : begin + 256, :] = dot(table, rows_ref[...]).astype(LOW)


def dispatch(slot_index, rows, slots):
    micro_count, tok_count, width = rows.shape
    return pl.pallas_call(
        functools.partial(dispatch_kernel, slots=slots),
        grid=(micro_count,),
        in_specs=[
            pl.BlockSpec((None, 1, tok_count), lambda m: (m, 0, 0)),
            pl.BlockSpec((None, tok_count, width), lambda m: (m, 0, 0)),
        ],
        out_specs=[pl.BlockSpec((slots, width), lambda m: (0, 0))] * micro_count,
        out_shape=[jax.ShapeDtypeStruct((slots, width), LOW)] * micro_count,
        compiler_params=pltpu.CompilerParams(vmem_limit_bytes=VMEM_BYTES),
        cost_estimate=pl.CostEstimate(flops=3 * 10**9, bytes_accessed=6 * 2**20, transcendentals=0),
        name="dispatch",
    )(slot_index, rows)


def attend_pair_back(query, keys, values, grad, mixed, soft_ref, place, inverses, rows):
    lane = lax.broadcasted_iota(jnp.int32, (1, PAIR), 1)
    scale = LOW(HEAD_DIM**-0.5)
    none = jnp.zeros_like(keys)
    dk_parts, dv_parts, dq_blocks = [None, None], [None, None], []
    for block in range(LENGTH // rows):
        part = slice(block * rows, (block + 1) * rows)
        query_t = (query[part, :] * scale).T
        scaled = grad[part, :].astype(F32) * inverses[part, :]
        inner = scaled * mixed[part, :].astype(F32)
        scaled = scaled.astype(LOW)
        scaled_t = scaled.T
        grad_query = None
        for head in range(2):
            mine = (lane < HEAD_DIM) if head == 0 else (lane >= HEAD_DIM)
            own = slice(head * HEAD_DIM, (head + 1) * HEAD_DIM)
            weights = soft_ref[place + head, part, :]
            grad_soft = dot(scaled, jnp.where(mine, values, none), NT)
            centre = jnp.sum(jnp.where(mine, inner, 0.0), axis=1, keepdims=True)
            grad_scores = (weights.astype(F32) * (grad_soft - centre)).astype(LOW)
            term = dot(grad_scores, jnp.where(mine, keys, none))
            grad_query = term if grad_query is None else grad_query + term
            dk = dot(query_t[own, :], grad_scores)
            dv = dot(scaled_t[own, :], weights)
            dk_parts[head] = dk if dk_parts[head] is None else dk_parts[head] + dk
            dv_parts[head] = dv if dv_parts[head] is None else dv_parts[head] + dv
        dq_blocks.append(grad_query * HEAD_DIM**-0.5)
    return (
        jnp.concatenate(dq_blocks, axis=0),
        jnp.concatenate(dk_parts, axis=0).T,
        jnp.concatenate(dv_parts, axis=0).T,
    )


def backward_kernel(
    tokens_ref, cot_ref, gain_one_ref, wq_ref, wk_ref, wv_ref, wo_ref, gain_two_ref, route_ref, embed_ref, slot_ref,
    id_ref, first_ref, projected_ref, home_ref, dots_ref, q_ref, k_ref, v_ref, mixed_ref, soft_ref, inv_ref,
    dwq_ref, dwk_ref, dwv_ref, dwo_ref, gtok_ref, small_ref,
    grad_first, branch, normed_t, total, mixed_grad, dq_sc, dk_sc, dv_sc, soft_buf, soft_sem,
    *, steps, slots, slot_cap,
):
    step = pl.program_id(0)
    width = tokens_ref.shape[1]
    experts, router_dim = embed_ref.shape
    pairs = GROUP // 2

    def soft_pair(pair):
        at = step * GROUP + 2 * pair
        return pltpu.make_async_copy(soft_ref.at[pl.ds(at, 2)], soft_buf.at[pair % 2], soft_sem.at[pair % 2])

    @pl.when(step == 0)
    def _():
        soft_pair(0).start()
        normed_one = normalise(tokens_ref[...].astype(F32))[0]
        normed_t[...] = (normed_one * gain_one_ref[...]).astype(LOW).T
        slot_column = to_column(slot_ref[...].astype(F32)).astype(jnp.int32)
        route_column = to_column(id_ref[...].astype(F32)).astype(jnp.int32)
        columns = [
            jnp.sum(jnp.where(diagonal(slot_cap), dots_ref[w, 0:1, :], 0.0), axis=1, keepdims=True)
            for w in range(experts)
        ]
        dots = spread_parts(jnp.concatenate(columns, axis=0))
        grads = []
        block = 256
        for begin in range(0, slot_column.shape[0], block):
            table = token_rows(slot_column[begin : begin + block, :], slots)
            grad_first[begin : begin + block, :] = dot(table, home_ref[...])
            grads.append(jnp.sum(dot(table, dots), axis=1, keepdims=True))
        grad_gate = jnp.concatenate(grads, axis=0)
        projected, embed_rows = projected_ref[...], embed_ref[...]
        unit, inverse, anchor, anchor_inverse, probs, picked, gate = route_probs(
            projected, embed_rows, route_column
        )
        grad_logits = grad_gate * gate * (jnp.where(picked, 1.0, 0.0) - probs)
        grad_unit = 3.0 * dot(grad_logits, anchor, NN, lax.Precision.HIGHEST)
        grad_anchor = 3.0 * dot(grad_logits, unit, TN, lax.Precision.HIGHEST)
        grad_projected = inverse * grad_unit - inverse**3 * projected * jnp.sum(
            projected * grad_unit, axis=-1, keepdims=True
        )
        term_embed = anchor_inverse * grad_anchor - anchor_inverse**3 * embed_rows * jnp.sum(
            embed_rows * grad_anchor, axis=-1, keepdims=True
        )
        normed_two, inverse_two = normalise(first_ref[...])
        second = (normed_two * gain_two_ref[...]).astype(LOW)
        grad_second = grad_first[...]
        term_route = None
        for part in three_parts(grad_projected):
            grad_second += dot(part, route_ref[...], NT)
            term = dot(part, second, TN)
            term_route = term if term_route is None else term_route + term
        small_ref[...] = jnp.zeros_like(small_ref)
        small_ref[0:router_dim, 0:width] = term_route
        small_ref[router_dim + 1 : router_dim + 2, 0:width] = jnp.sum(grad_second * normed_two, axis=0, keepdims=True)
        small_ref[0:experts, width : width + router_dim] = term_embed
        value = cot_ref[...].astype(F32) + normalise_back(grad_second * gain_two_ref[...], normed_two, inverse_two)
        grad_first[...] = value
        branch[...] = value.astype(LOW)
        total[...] = jnp.zeros_like(total)

    rows = branch[...]
    dwo_ref[...] = dot(mixed_ref[...], rows, TN).astype(LOW)
    mixed_grad[...] = dot(rows, wo_ref[...], NT).astype(LOW)
    for pair in range(pairs):
        lanes = slice(pair * PAIR, (pair + 1) * PAIR)
        soft_pair(pair).wait()
        if pair + 1 < pairs:
            soft_pair(pair + 1).start()
        else:

            @pl.when(step + 1 < steps)
            def _():
                soft_pair(pairs).start()

        dq, dk, dv = attend_pair_back(
            q_ref[:, lanes], k_ref[:, lanes], v_ref[:, lanes], mixed_grad[:, lanes], mixed_ref[:, lanes],
            soft_buf.at[pair % 2], 0, inv_ref[:, lanes], 512,
        )
        dq_sc[:, lanes] = dq.astype(LOW)
        dk_sc[:, lanes] = dk.astype(LOW)
        dv_sc[:, lanes] = dv.astype(LOW)
    normed_rows = normed_t[...]
    for grad_ref, weight_ref, out_ref in (
        (dq_sc, wq_ref, dwq_ref), (dk_sc, wk_ref, dwk_ref), (dv_sc, wv_ref, dwv_ref)
    ):
        grad = grad_ref[...]
        out_ref[...] = dot(normed_rows, grad).astype(LOW)
        total[...] += dot(grad, weight_ref[...], NT)

    @pl.when(step == steps - 1)
    def _():
        normed_one, inverse_one = normalise(tokens_ref[...].astype(F32))
        grad = total[...]
        small_ref[router_dim : router_dim + 1, 0:width] = jnp.sum(grad * normed_one, axis=0, keepdims=True)
        gtok_ref[...] = (
            grad_first[...] + normalise_back(grad * gain_one_ref[...], normed_one, inverse_one)
        ).astype(LOW)


def backward_stage(
    m, tokens, grad_out, gains, weights, w_route, embed, slot_index, route_ids, kept, home, slot_cap, moves, pushes, cid
):
    tok_count, width = tokens.shape[1:]
    experts, router_dim = embed.shape
    slots = experts * slot_cap
    steps = HEADS // GROUP
    span = GROUP * HEAD_DIM
    one = pl.Buffered(1)
    fixed = lambda shape: pl.BlockSpec(shape, lambda i: (0,) * len(shape), pipeline_mode=one)
    of_m = lambda *shape: pl.BlockSpec((None, *shape), lambda i: (m, 0, 0), pipeline_mode=one)
    columns = lambda height: pl.BlockSpec((height, span), lambda i: (0, i))
    lines = pl.BlockSpec((span, width), lambda i: (i, 0))
    gain_one, gain_two = gains
    wq, wk, wv, wo = weights
    first, projected, q, k, v, mixed, soft, inverses = kept
    low = lambda *shape: jax.ShapeDtypeStruct(shape, LOW)
    small = (-(-max(experts, router_dim + 2) // 8) * 8, width + 128)
    return call_with_moves(
        functools.partial(backward_kernel, steps=steps, slots=slots, slot_cap=slot_cap),
        moves,
        pushes,
        cid,
        grid=(steps,),
        in_specs=[
            of_m(tok_count, width), of_m(tok_count, width), fixed((1, width)), columns(width), columns(width),
            columns(width), lines, fixed((1, width)), fixed(w_route.shape), fixed(embed.shape), of_m(1, tok_count),
            of_m(1, tok_count), fixed(first.shape), fixed(projected.shape), fixed(home[0].shape), fixed(home[1].shape),
            columns(tok_count), columns(tok_count), columns(tok_count), columns(tok_count),
            pl.BlockSpec(memory_space=pl.ANY), columns(tok_count),
        ],
        out_specs=[
            columns(width), columns(width), columns(width), lines, fixed((tok_count, width)), fixed(small),
        ],
        out_shape=[
            low(width, width), low(width, width), low(width, width), low(width, width), low(tok_count, width),
            jax.ShapeDtypeStruct(small, F32),
        ],
        scratch_shapes=[
            pltpu.VMEM((tok_count, width), F32), pltpu.VMEM((tok_count, width), LOW),
            pltpu.VMEM((width, tok_count), LOW), pltpu.VMEM((tok_count, width), F32),
        ]
        + [pltpu.VMEM((tok_count, span), LOW)] * 4
        + [pltpu.VMEM((2, 2, LENGTH, LENGTH), LOW), pltpu.SemaphoreType.DMA((2,))],
        cost=pl.CostEstimate(flops=40 * 10**9, bytes_accessed=50 * 2**20, transcendentals=0),
        name="backward_stage",
        args=(
            tokens, grad_out, gain_one, wq, wk, wv, wo, gain_two, w_route, embed, slot_index, route_ids, first,
            projected, *home, q, k, v, mixed, soft, inverses,
        ),
    )


def finish_kernel(*refs, micro_count, slots):
    slot_ref, id_ref, embed_ref = refs[:3]
    ins, (out_ref, grad_ref) = refs[3:-2], refs[-2:]
    for m in range(micro_count):
        first_ref, projected_ref, home_ref, gtok_ref = ins[4 * m : 4 * m + 4]

        @pl.when(pl.program_id(0) == m)
        def _():
            slot_column = to_column(slot_ref[...].astype(F32)).astype(jnp.int32)
            route_column = to_column(id_ref[...].astype(F32)).astype(jnp.int32)
            gate = route_probs(projected_ref[...], embed_ref[...], route_column)[-1]
            returned = dot(token_rows(slot_column, slots), home_ref[...])
            out_ref[...] = (first_ref[...] + gate * returned).astype(LOW)
            grad_ref[...] = gtok_ref[...]


def finish(slot_index, route_ids, embed, parts, slots):
    micro_count, _, tok_count = slot_index.shape
    width = parts[0][0].shape[1]
    rows = 256
    blocks = tok_count // rows
    row = pl.BlockSpec((None, 1, rows), lambda m, i: (m, 0, i))
    whole = lambda shape: pl.BlockSpec(shape, lambda m, i: (0, 0))
    in_specs, args = [row, row, whole(embed.shape)], [slot_index, route_ids, embed]
    for at, (first, projected, home, gtok) in enumerate(parts):
        place = lambda m, i, at=at: (jnp.where(m == at, i, jnp.where(m < at, 0, blocks - 1)), 0)
        in_specs += [
            pl.BlockSpec((rows, width), place), pl.BlockSpec((rows, projected.shape[1]), place), whole(home.shape),
            pl.BlockSpec((rows, width), place),
        ]
        args += [first, projected, home, gtok]
    out = pl.BlockSpec((None, rows, width), lambda m, i: (m, i, 0))
    return pl.pallas_call(
        functools.partial(finish_kernel, micro_count=micro_count, slots=slots),
        grid=(micro_count, blocks),
        in_specs=in_specs,
        out_specs=[out, out],
        out_shape=[jax.ShapeDtypeStruct((micro_count, tok_count, width), LOW)] * 2,
        compiler_params=pltpu.CompilerParams(vmem_limit_bytes=VMEM_BYTES),
        cost_estimate=pl.CostEstimate(flops=3 * 10**9, bytes_accessed=18 * 2**20, transcendentals=0),
        name="finish",
    )(*args)


def gelu_and_slope(values):
    ratio = 1.0 / (1.0 + jnp.abs(values) * (0.3275911 * 0.7071067811865476))
    bell = jnp.exp(values * values * -0.5)
    series = 0.5 * 1.061405429
    for factor in (-1.453152027, 1.421413741, -0.284496736, 0.254829592):
        series = series * ratio + 0.5 * factor
    tail = series * ratio * bell
    below = jnp.where(values >= 0.0, 1.0 - tail, tail)
    return values * below, below + values * bell * 0.3989422804014327


def expert_kernel(*refs, more, last, per, steps, slot_cap):
    rows_ref, cot_ref, gate_ref, own_in, own_outer = refs[:5]
    far_in, far_outer = refs[5 : 5 + per], refs[5 + per : 5 + 2 * per]
    refs = refs[5 + 2 * per :]
    if more:
        old_in, old_outer = refs[:2]
        refs = refs[2:]
    result_ref, sent_ref, dots_ref, din_ref, douter_ref = refs[:5]
    refs = refs[5:]
    if last:
        far_din, far_douter = refs[:2]
        refs = refs[2:]
    grad_sc, rows_t, acc_result, acc_sent, first_buf, second_buf, sems = refs
    step = pl.program_id(0)
    slot = lax.rem(step, 2)
    sources = rows_ref.shape[0] // slot_cap
    tile = first_buf.shape[2]

    def fetch(i):
        if i < per:
            first = own_in.at[:, i * tile : (i + 1) * tile]
            second = own_outer.at[i * tile : (i + 1) * tile, :]
        else:
            first, second = far_in[i % per].at[i // per - 1], far_outer[i % per].at[i // per - 1]
        return (
            pltpu.make_async_copy(first, first_buf.at[i % 2], sems.at[0, i % 2]),
            pltpu.make_async_copy(second, second_buf.at[i % 2], sems.at[1, i % 2]),
        )

    @pl.when(step == 0)
    def _():
        for copy in fetch(0):
            copy.start()
        for w in range(sources):
            part = slice(w * slot_cap, (w + 1) * slot_cap)
            gate = jnp.sum(jnp.where(diagonal(slot_cap), gate_ref[w, 0:1, :], 0.0), axis=1, keepdims=True)
            grad_sc[part, :] = (cot_ref[part, :].astype(F32) * gate).astype(LOW)
        rows_t[...] = rows_ref[...].T
        acc_result[...] = jnp.zeros_like(acc_result)
        acc_sent[...] = jnp.zeros_like(acc_sent)

    for i in range(steps):

        @pl.when(step == i)
        def _():
            for copy in fetch(i):
                copy.wait()
            if i + 1 < steps:
                for copy in fetch(i + 1):
                    copy.start()

    first, second = first_buf[slot], second_buf[slot]
    hidden, slope = gelu_and_slope(dot(rows_ref[...], first))
    hidden = hidden.astype(LOW)
    grad_rows = grad_sc[...]
    grad_pre = (dot(grad_rows, second, NT) * slope).astype(LOW)
    acc_result[...] += dot(hidden, second)
    acc_sent[...] += dot(grad_pre, first, NT)
    din = dot(rows_t[...], grad_pre)
    douter = dot(hidden, grad_rows, TN)
    if more:
        din += old_in[...]
        douter += old_outer[...]
    if not last:
        din_ref[...] = din
        douter_ref[...] = douter
    else:

        @pl.when(step < per)
        def _():
            din_ref[...] = din
            douter_ref[...] = douter

        @pl.when(step >= per)
        def _():
            far_din[...] = din.astype(LOW)
            far_douter[...] = douter.astype(LOW)

    @pl.when(step == steps - 1)
    def _():
        result = acc_result[...].astype(LOW)
        result_ref[...] = result
        sent_ref[...] = acc_sent[...].astype(LOW)
        for w in range(sources):
            part = slice(w * slot_cap, (w + 1) * slot_cap)
            products = cot_ref[part, :].astype(F32) * result[part, :].astype(F32)
            column = jnp.sum(products, axis=1, keepdims=True)
            row = jnp.sum(jnp.where(diagonal(slot_cap), column, 0.0), axis=0, keepdims=True)
            dots_ref[w] = jnp.broadcast_to(row, (8, 128))


def tile_of(units):
    return min(512, units)


def expert_stage(rows, cot, gates, weights, old, last, slot_cap, moves, pushes, cid):
    own_in, own_outer, far_in, far_outer = weights
    width, units = own_in.shape
    count = lax.axis_size("narrow")
    height = rows.shape[0]
    tile = tile_of(units)
    per = units // tile
    steps = count * per
    whole = lambda shape: pl.BlockSpec(shape, lambda i: (0,) * len(shape))
    anywhere = pl.BlockSpec(memory_space=pl.ANY)
    din_spec = pl.BlockSpec((None, width, tile), lambda i: (i, 0, 0))
    douter_spec = pl.BlockSpec((None, tile, width), lambda i: (i, 0, 0))
    out_specs = [whole((height, width)), whole((height, width)), whole(gates.shape)]
    out_shape = [
        jax.ShapeDtypeStruct((height, width), LOW),
        jax.ShapeDtypeStruct((height, width), LOW),
        jax.ShapeDtypeStruct(gates.shape, F32),
    ]
    if last:
        near = lambda i: jnp.minimum(i, per - 1)
        away = lambda i: jnp.maximum(i - per, 0)
        out_specs += [
            pl.BlockSpec((width, tile), lambda i: (0, near(i))),
            pl.BlockSpec((tile, width), lambda i: (near(i), 0)),
            pl.BlockSpec((None, width, tile), lambda i: (away(i), 0, 0)),
            pl.BlockSpec((None, tile, width), lambda i: (away(i), 0, 0)),
        ]
        out_shape += [
            jax.ShapeDtypeStruct((width, units), F32),
            jax.ShapeDtypeStruct((units, width), F32),
            jax.ShapeDtypeStruct((steps - per, width, tile), LOW),
            jax.ShapeDtypeStruct((steps - per, tile, width), LOW),
        ]
    else:
        out_specs += [din_spec, douter_spec]
        out_shape += [
            jax.ShapeDtypeStruct((steps, width, tile), F32),
            jax.ShapeDtypeStruct((steps, tile, width), F32),
        ]
    return call_with_moves(
        functools.partial(
            expert_kernel, more=bool(old), last=last, per=per, steps=steps, slot_cap=slot_cap
        ),
        moves,
        pushes,
        cid,
        grid=(steps,),
        in_specs=[whole((height, width)), whole((height, width)), whole(gates.shape)]
        + [anywhere] * (2 + 2 * per)
        + ([din_spec, douter_spec] if old else []),
        out_specs=out_specs,
        out_shape=out_shape,
        scratch_shapes=[
            pltpu.VMEM((height, width), LOW),
            pltpu.VMEM((width, height), LOW),
            pltpu.VMEM((height, width), F32),
            pltpu.VMEM((height, width), F32),
            pltpu.VMEM((2, width, tile), LOW),
            pltpu.VMEM((2, tile, width), LOW),
            pltpu.SemaphoreType.DMA((2, 2)),
        ],
        cost=pl.CostEstimate(
            flops=12 * height * width * units * count, bytes_accessed=34 * 2**20, transcendentals=0
        ),
        name="expert_stage",
        args=(rows, cot, gates, own_in, own_outer, *far_in, *far_outer, *old),
    )


def local(
    tokens,
    grad_out,
    route_ids,
    slot_ids,
    keep_ids,
    gain_one,
    w_query,
    w_key,
    w_value,
    w_out,
    gain_two,
    w_route,
    embed,
    w_in,
    w_outer,
):
    micro_count, tok_count, feat_width = tokens.shape
    expert_count = embed.shape[0]
    slot_cap = max(2, tok_count // expert_count)
    slots = expert_count * slot_cap
    own_in, own_outer = w_in[0], w_outer[0]
    units = own_in.shape[1]
    tile = tile_of(units)
    per = units // tile
    weight_pushes = [
        (own_in, lambda ref, j, t=t: ref.at[:, t * tile : (t + 1) * tile], (feat_width, tile)) for t in range(per)
    ] + [
        (own_outer, lambda ref, j, t=t: ref.at[t * tile : (t + 1) * tile, :], (tile, feat_width)) for t in range(per)
    ]
    early = len(weight_pushes) // 3
    slot_index = jnp.where(keep_ids > 0, route_ids * slot_cap + slot_ids, -1)[:, None, :]
    route_rows = route_ids[:, None, :]
    gains = (gain_one[None], gain_two[None])
    mixers = (w_query, w_key, w_value, w_out)
    router = (w_route, embed, slot_index, route_rows)

    def boxes(rows):
        return rows.reshape((expert_count, slot_cap) + rows.shape[1:])

    def flat(boxed):
        return boxed.reshape((expert_count * slot_cap,) + boxed.shape[2:])

    cot_boxes = [boxes(rows) for rows in dispatch(slot_index, grad_out, slots)]
    (*ahead_0, sent, gates, projected), (cot_0,), far_a = forward_stage(
        0, tokens, gains, mixers, *router, slot_cap, (cot_boxes[0],), weight_pushes[:early], 1
    )
    ahead_0.append(projected)
    (*ahead_1, next_sent, next_gates, projected), (sent_0, gates_0, cot_1), far_b = forward_stage(
        1, tokens, gains, mixers, *router, slot_cap, (boxes(sent), gates, cot_boxes[1]), weight_pushes[early:], 2
    )
    ahead_1.append(projected)

    far = [*far_a, *far_b]
    weights = (own_in, own_outer, far[:per], far[per:])
    (result_0, grad_0, dots_0, *old), (sent_1, gates_1), _ = expert_stage(
        flat(sent_0), flat(cot_0), gates_0, weights, (), False, slot_cap, (boxes(next_sent), next_gates), (), 3
    )
    (result_1, grad_1, dots_1, near_din, near_douter, far_din, far_douter), (home_grad_0, home_dots_0), _ = expert_stage(
        flat(sent_1), flat(cot_1), gates_1, weights, tuple(old), True, slot_cap, (boxes(grad_0), dots_0), (), 4
    )
    grad_pushes = [
        (far_din, lambda ref, j, t=t: ref.at[j * per + t], (feat_width, tile)) for t in range(per)
    ] + [
        (far_douter, lambda ref, j, t=t: ref.at[j * per + t], (tile, feat_width)) for t in range(per)
    ]
    later = len(grad_pushes) - early

    def kept(ahead):
        q, k, v, soft, inverses, mixed, first, projected = ahead
        return first, projected, q, k, v, mixed, soft, inverses

    (*big_0, gtok_0, small_0), (home_grad_1, home_dots_1), got_a = backward_stage(
        0, tokens, grad_out, gains, mixers, *router, kept(ahead_0), (flat(home_grad_0), home_dots_0), slot_cap,
        (boxes(grad_1), dots_1), grad_pushes[:later], 5
    )
    (*big_1, gtok_1, small_1), (home_result_0, home_result_1), got_b = backward_stage(
        1, tokens, grad_out, gains, mixers, *router, kept(ahead_1), (flat(home_grad_1), home_dots_1), slot_cap,
        (boxes(result_0), boxes(result_1)), grad_pushes[later:], 6
    )
    block_out, grad_tokens = finish(
        slot_index, route_rows, embed,
        (
            (ahead_0[6], ahead_0[7], flat(home_result_0), gtok_0),
            (ahead_1[6], ahead_1[7], flat(home_result_1), gtok_1),
        ),
        slots,
    )
    big, small = reduce_everywhere(list(zip(big_0, big_1)), (small_0, small_1), 7)
    big = [big[:, k * feat_width : (k + 1) * feat_width].astype(F32) for k in range(4)]
    router_dim = w_route.shape[1]
    got = [*got_a, *got_b]
    return (
        block_out,
        grad_tokens,
        small[router_dim, :feat_width],
        *big,
        small[router_dim + 1, :feat_width],
        small[:router_dim, :feat_width].T,
        small[:expert_count, feat_width : feat_width + router_dim],
        join(near_din, got[:per], 1),
        join(near_douter, got[per:], 0),
    )


def solution(mesh):
    tokens_spec = P(None, ("wide", "narrow"), None)
    ids_spec = P(None, ("wide", "narrow"))
    in_spec, outer_spec = P("wide", None, "narrow"), P("wide", "narrow", None)
    return jax.shard_map(
        local,
        mesh=mesh,
        in_specs=(tokens_spec,) * 2 + (ids_spec,) * 3 + (P(),) * 8 + (in_spec, outer_spec),
        out_specs=(tokens_spec,) * 2 + (P(),) * 8 + (in_spec, outer_spec),
        check_vma=False,
    )
```

```python
import functools

import jax
import jax.numpy as jnp
from jax import lax
from jax.experimental import pallas as pl
from jax.experimental.pallas import tpu as pltpu
from jax.sharding import PartitionSpec as P

D = 768
HEADS = 12
HEAD_DIM = 64
LENGTH = 1024
PAIR = 2 * HEAD_DIM
GROUP = 4
NN = (((1,), (0,)), ((), ()))
NT = (((1,), (1,)), ((), ()))
TN = (((0,), (0,)), ((), ()))
LOW = jnp.bfloat16
F32 = jnp.float32
VMEM_BYTES = 60 << 20


def dot(left, right, dims=NN, precise=None):
    return lax.dot_general(left, right, dims, precision=precise, preferred_element_type=F32)


def normalise(values):
    centred = values - jnp.mean(values, axis=-1, keepdims=True)
    inverse = lax.rsqrt(jnp.mean(centred * centred, axis=-1, keepdims=True) + 1e-05)
    return centred * inverse, inverse


def normalise_back(grad, normed, inverse):
    return inverse * (
        grad
        - jnp.mean(grad, axis=-1, keepdims=True)
        - normed * jnp.mean(grad * normed, axis=-1, keepdims=True)
    )


def by_rows(count, size, body, carry=None):
    return lax.fori_loop(
        0, count // size, lambda i, c: body(pl.ds(pl.multiple_of(i * size, size), size), c), carry, unroll=2
    )


def fold_rows(values):
    return jnp.sum(values.reshape(values.shape[0] // 8, 8, values.shape[1]), axis=0)


def three_parts(values):
    high = values.astype(LOW)
    rest = values - high.astype(F32)
    middle = rest.astype(LOW)
    return high, middle, (rest - middle.astype(F32)).astype(LOW)


def spread_parts(column):
    lane = lax.broadcasted_iota(jnp.int32, (1, 128), 1)
    high, middle, low = (part.astype(F32) for part in three_parts(column))
    return jnp.where(lane == 0, high, jnp.where(lane == 1, middle, jnp.where(lane == 2, low, 0.0))).astype(LOW)


def diagonal(rows):
    shape = (rows, 128)
    return lax.broadcasted_iota(jnp.int32, shape, 0) == lax.broadcasted_iota(jnp.int32, shape, 1)


def to_column(row):
    pieces = [
        jnp.sum(jnp.where(diagonal(128), row[:, first : first + 128], 0.0), axis=1, keepdims=True)
        for first in range(0, row.shape[1], 128)
    ]
    return jnp.concatenate(pieces, axis=0)


def unit_length(rows):
    inverse = lax.rsqrt(jnp.sum(rows * rows, axis=-1, keepdims=True) + 1.0)
    return rows * inverse, inverse


def route_probs(projected, embed_rows, route_column):
    unit, inverse = unit_length(projected)
    anchor, anchor_inverse = unit_length(embed_rows)
    logits = 3.0 * dot(unit, anchor, NT, lax.Precision.HIGHEST)
    weights = jnp.exp(logits - jnp.max(logits, axis=-1, keepdims=True))
    probs = weights / jnp.sum(weights, axis=-1, keepdims=True)
    lane = lax.broadcasted_iota(jnp.int32, (1, probs.shape[1]), 1)
    picked = route_column == lane
    gate = jnp.sum(jnp.where(picked, probs, 0.0), axis=-1, keepdims=True)
    return unit, inverse, anchor, anchor_inverse, probs, picked, gate


def slot_line(m, route_ref, slot_ref, keep_ref, slot_cap):
    line = slice(m, m + 1)
    return jnp.where(keep_ref[line, :] > 0, route_ref[line, :] * slot_cap + slot_ref[line, :], -1)


def slot_rows(slot_row, first, count):
    slot = lax.broadcasted_iota(jnp.int32, (count, slot_row.shape[1]), 0) + first
    return jnp.where(slot == slot_row, 1.0, 0.0).astype(LOW)


def token_rows(slot_column, slots):
    lane = lax.broadcasted_iota(jnp.int32, (slot_column.shape[0], slots), 1)
    return jnp.where(lane == slot_column, 1.0, 0.0).astype(LOW)


MESH = pl.DeviceIdType.MESH


def call_with_moves(
    body, moves, pushes, cid, *, grid, in_specs, out_specs, out_shape, scratch_shapes=(), cost, name, args
):
    members, spread = lax.axis_size("wide"), lax.axis_size("narrow")
    n_in, n_out, n_moves, n_scratch = len(in_specs), len(out_specs), len(moves), len(scratch_shapes)
    arrays = []
    for array, _, _ in pushes:
        if not any(array is known for known in arrays):
            arrays.append(array)
    which = [next(k for k, known in enumerate(arrays) if known is array) for array, _, _ in pushes]
    n_arrays, n_pushes = len(arrays), len(pushes)

    def kernel(*refs):
        ins, refs = refs[:n_in], refs[n_in:]
        sources, refs = refs[:n_moves], refs[n_moves:]
        pushed, refs = refs[:n_arrays], refs[n_arrays:]
        outs, refs = refs[:n_out], refs[n_out:]
        targets, refs = refs[:n_moves], refs[n_moves:]
        landings, refs = refs[:n_pushes], refs[n_pushes:]
        scratch, refs = refs[:n_scratch], refs[n_scratch:]
        stages, refs = refs[:n_moves], refs[n_moves:]
        send_sem, recv_sem, own_sem, push_send, push_recv = refs
        me, side = lax.axis_index("wide"), lax.axis_index("narrow")
        step = pl.program_id(0)

        def remote(i, d):
            peer = lax.rem(me + d, members)
            return pltpu.make_async_remote_copy(
                src_ref=sources[i].at[peer],
                dst_ref=targets[i].at[me],
                send_sem=send_sem.at[i, d],
                recv_sem=recv_sem.at[i, d],
                device_id={"wide": peer},
                device_id_type=MESH,
            )

        def push(k, j):
            return pltpu.make_async_remote_copy(
                src_ref=pushes[k][1](pushed[which[k]], j),
                dst_ref=landings[k].at[j],
                send_sem=push_send.at[k, j],
                recv_sem=push_recv.at[k, j],
                device_id={"narrow": lax.rem(side + j + 1, spread)},
                device_id_type=MESH,
            )

        @pl.when(step == 0)
        def _():
            barrier = pltpu.get_barrier_semaphore()
            count = 0
            if n_moves:
                for d in range(1, members):
                    pl.semaphore_signal(
                        barrier, inc=1, device_id={"wide": lax.rem(me + d, members)}, device_id_type=MESH
                    )
                count += members - 1
            if n_pushes:
                for j in range(spread - 1):
                    pl.semaphore_signal(
                        barrier, inc=1, device_id={"narrow": lax.rem(side + j + 1, spread)}, device_id_type=MESH
                    )
                count += spread - 1
            pl.semaphore_wait(barrier, count)
            for k in range(n_pushes):
                for j in range(spread - 1):
                    push(k, j).start()
            for i in range(n_moves):
                for d in range(1, members):
                    remote(i, d).start()
                pltpu.make_async_copy(sources[i].at[me], stages[i], own_sem.at[i]).start()

        body(*ins, *outs, *scratch)

        @pl.when(step == grid[0] - 1)
        def _():
            for i in range(n_moves):
                pltpu.make_async_copy(sources[i].at[me], stages[i], own_sem.at[i]).wait()
                pltpu.make_async_copy(stages[i], targets[i].at[me], own_sem.at[i]).start()
            for i in range(n_moves):
                pltpu.make_async_copy(stages[i], targets[i].at[me], own_sem.at[i]).wait()
                for d in range(1, members):
                    remote(i, d).wait()
            for k in range(n_pushes):
                for j in range(spread - 1):
                    push(k, j).wait()

    anywhere = pl.BlockSpec(memory_space=pl.ANY)
    results = pl.pallas_call(
        kernel,
        grid=grid,
        in_specs=list(in_specs) + [anywhere] * (n_moves + n_arrays),
        out_specs=list(out_specs) + [anywhere] * (n_moves + n_pushes),
        out_shape=list(out_shape)
        + [jax.ShapeDtypeStruct(a.shape, a.dtype) for a in moves]
        + [jax.ShapeDtypeStruct((spread - 1, *shape), a.dtype) for a, _, shape in pushes],
        scratch_shapes=list(scratch_shapes)
        + [pltpu.VMEM(a.shape[1:], a.dtype) for a in moves]
        + [
            pltpu.SemaphoreType.DMA((max(1, n_moves), members)),
            pltpu.SemaphoreType.DMA((max(1, n_moves), members)),
            pltpu.SemaphoreType.DMA((max(1, n_moves),)),
            pltpu.SemaphoreType.DMA((max(1, n_pushes), spread)),
            pltpu.SemaphoreType.DMA((max(1, n_pushes), spread)),
        ],
        compiler_params=pltpu.CompilerParams(
            vmem_limit_bytes=VMEM_BYTES, collective_id=cid, has_side_effects=True
        ),
        cost_estimate=cost,
        name=name,
    )(*args, *moves, *arrays)
    return results[:n_out], results[n_out : n_out + n_moves], results[n_out + n_moves :]


def reduce_orders(wide_count, narrow_count):
    bits = lambda axis, count: [(axis, 1 << k) for k in range(count.bit_length() - 1)]
    wide, narrow = bits("wide", wide_count), bits("narrow", narrow_count)
    core, x_bits, z_bits = wide[:1], wide[1:2], wide[2:]
    return (
        core + x_bits + narrow + z_bits,
        core + narrow + x_bits + z_bits,
        core + z_bits + x_bits + narrow,
    ) * 2


def halvings(order, rows, columns):
    plan = []
    for _ in order:
        if columns % 256 == 0:
            columns //= 2
            plan.append("columns")
        elif rows % 32 == 0:
            rows //= 2
            plan.append("rows")
        else:
            plan.append("whole")
    return plan


def reduce_kernel(*refs, orders, width, places, sets):
    ins = [refs[k * sets : (k + 1) * sets] for k in range(len(places))]
    refs = refs[len(places) * sets :]
    smalls, refs = refs[:sets], refs[sets:]
    out_ref, small_out, total, result, small_send, small_recv = refs[:6]
    refs = refs[6:]
    parts, stages = len(orders), len(orders[0])
    outgoing = [refs[p * stages : (p + 1) * stages] for p in range(parts)]
    incoming = [refs[(parts + p) * stages : (parts + p + 1) * stages] for p in range(parts)]
    send_sem, recv_sem, back_send, back_recv, small_sems, small_rsems = refs[2 * parts * stages :]
    index = {axis: lax.axis_index(axis) for axis in ("wide", "narrow")}
    rows = total.shape[0]

    def own_bit(axis, bit):
        return lax.rem(index[axis] // bit, 2)

    def partner(axis, bit):
        return {axis: index[axis] + bit - 2 * bit * own_bit(axis, bit)}

    barrier = pltpu.get_barrier_semaphore()
    for axis, bit in orders[0]:
        pl.semaphore_signal(barrier, inc=1, device_id=partner(axis, bit), device_id_type=MESH)
    pl.semaphore_wait(barrier, stages)

    for group, place in zip(ins, places):
        total[:, place : place + group[0].shape[1]] = sum(ref[...].astype(F32) for ref in group)
    small_send[0] = sum(ref[...] for ref in smalls)

    regions = [[(0, rows, p * width, width)] for p in range(parts)]

    def take(region):
        row, height, column, span = region
        if not isinstance(row, int):
            row = pl.multiple_of(row, 16)
        if not isinstance(column, int):
            column = pl.multiple_of(column, 128)
        return pl.ds(row, height), pl.ds(column, span)

    def half(region, how, pick):
        row, height, column, span = region
        if how == "columns":
            return row, height, column + pick * (span // 2), span // 2
        if how == "rows":
            return row + pick * (height // 2), height // 2, column, span
        return region

    plans = [halvings(order, rows, width) for order in orders]

    def there(p, s):
        axis, bit = orders[p][s]
        return pltpu.make_async_remote_copy(
            src_ref=outgoing[p][s],
            dst_ref=incoming[p][s],
            send_sem=send_sem.at[p, s],
            recv_sem=recv_sem.at[p, s],
            device_id=partner(axis, bit),
            device_id_type=MESH,
        )

    def small_there(s):
        axis, bit = orders[0][s]
        return pltpu.make_async_remote_copy(
            src_ref=small_send.at[s],
            dst_ref=small_recv.at[s],
            send_sem=small_sems.at[s],
            recv_sem=small_rsems.at[s],
            device_id=partner(axis, bit),
            device_id_type=MESH,
        )

    def launch(p, s):
        axis, bit = orders[p][s]
        mine = own_bit(axis, bit)
        region, how = regions[p][-1], plans[p][s]
        outgoing[p][s][...] = total[take(half(region, how, 1 - mine))].astype(LOW)
        there(p, s).start()
        regions[p].append(half(region, how, mine))

    for p in range(parts):
        launch(p, 0)
    small_there(0).start()
    for s in range(stages):
        for p in range(parts):
            there(p, s).wait()
            kept = take(regions[p][-1])
            base = outgoing[p][s][...].astype(F32) if plans[p][s] == "whole" else total[kept]
            value = base + incoming[p][s][...].astype(F32)
            if s + 1 < stages:
                total[kept] = value
                launch(p, s + 1)
            else:
                result[kept] = value.astype(LOW)
        small_there(s).wait()
        fresh = small_send[s] + small_recv[s]
        if s + 1 < stages:
            small_send[s + 1] = fresh
            small_there(s + 1).start()
        else:
            small_out[...] = fresh

    def back(p, s):
        axis, bit = orders[p][s]
        spot = take(regions[p][s + 1])
        return pltpu.make_async_remote_copy(
            src_ref=result.at[spot],
            dst_ref=result.at[spot],
            send_sem=back_send.at[p, s],
            recv_sem=back_recv.at[p, s],
            device_id=partner(axis, bit),
            device_id_type=MESH,
        )

    for s in reversed(range(stages)):
        for p in range(parts):
            if plans[p][s] != "whole":
                back(p, s).start()
        for p in range(parts):
            if plans[p][s] != "whole":
                back(p, s).wait()
    out_ref[...] = result[...]


def reduce_everywhere(big, small, cid):
    orders = reduce_orders(lax.axis_size("wide"), lax.axis_size("narrow"))
    places, columns = [], 0
    for group in big:
        places.append(columns)
        columns += group[0].shape[1]
    rows = big[0][0].shape[0]
    sets = len(small)
    width, parts, stages = columns // len(orders), len(orders), len(orders[0])
    buffers = []
    for order in orders:
        height, span = rows, width
        for how in halvings(order, rows, width):
            height, span = (height // 2 if how == "rows" else height), (span // 2 if how == "columns" else span)
            buffers.append(pltpu.VMEM((height, span), LOW))
    vmem = pl.BlockSpec(memory_space=pltpu.VMEM)
    return pl.pallas_call(
        functools.partial(reduce_kernel, orders=orders, width=width, places=places, sets=sets),
        in_specs=[vmem] * ((len(big) + 1) * sets),
        out_specs=[vmem, vmem],
        out_shape=[jax.ShapeDtypeStruct((rows, columns), LOW), jax.ShapeDtypeStruct(small[0].shape, F32)],
        scratch_shapes=[
            pltpu.VMEM((rows, columns), F32),
            pltpu.VMEM((rows, columns), LOW),
            pltpu.VMEM((stages, *small[0].shape), F32),
            pltpu.VMEM((stages, *small[0].shape), F32),
        ]
        + buffers
        + buffers
        + [pltpu.SemaphoreType.DMA((parts, stages))] * 4
        + [pltpu.SemaphoreType.DMA((stages,))] * 2,
        compiler_params=pltpu.CompilerParams(
            vmem_limit_bytes=VMEM_BYTES, collective_id=cid, has_side_effects=True
        ),
        cost_estimate=pl.CostEstimate(flops=10**9, bytes_accessed=20 * 2**20, transcendentals=0),
        name="reduce_everywhere",
    )(*(array for group in big for array in group), *small)


def attend_pair(query, keys, values, soft_ref, place, rows):
    lane = lax.broadcasted_iota(jnp.int32, (1, PAIR), 1)
    none = jnp.zeros_like(keys)
    mixed_blocks, inverse_blocks = [], []
    for block in range(LENGTH // rows):
        part = slice(block * rows, (block + 1) * rows)
        scaled = query[part, :] * LOW(HEAD_DIM**-0.5)
        mixed, inverses = None, []
        for head in range(2):
            mine = (lane < HEAD_DIM) if head == 0 else (lane >= HEAD_DIM)
            scores = dot(scaled, jnp.where(mine, keys, none), NT)
            top = jnp.max(scores, axis=1, keepdims=True)
            weights = jnp.exp(scores - top)
            inverse = 1.0 / jnp.sum(weights, axis=1, keepdims=True)
            weights = weights.astype(LOW)
            soft_ref[place + head, part, :] = weights
            inverses.append(jnp.broadcast_to(inverse, (rows, PAIR)))
            term = dot(weights, jnp.where(mine, values, none)) * inverse
            mixed = term if mixed is None else mixed + term
        mixed_blocks.append(mixed)
        inverse_blocks.append(jnp.where(lane < HEAD_DIM, inverses[0], inverses[1]))
    return jnp.concatenate(mixed_blocks, axis=0), jnp.concatenate(inverse_blocks, axis=0)


def forward_kernel(
    tokens_ref, gain_one_ref, wq_ref, wk_ref, wv_ref, wo_ref, gain_two_ref, route_ref, embed_ref, *refs,
    m, steps, slots, slot_cap,
):
    ids_ref, slot_ids_ref, keep_ref = refs[:3]
    q_ref, k_ref, v_ref, soft_ref, inv_ref, mixed_ref, first_ref, sent_ref, gates_ref, projected_ref, normed = refs[3:]
    step = pl.program_id(0)
    height = tokens_ref.shape[0]

    @pl.when(step == 0)
    def _():
        gain = gain_one_ref[...]

        def body(rows, _):
            values = tokens_ref[rows, :].astype(F32)
            normed[rows, :] = (normalise(values)[0] * gain).astype(LOW)
            first_ref[rows, :] = values

        by_rows(height, 32, body)

    rows = normed[...]
    q_ref[...] = dot(rows, wq_ref[...]).astype(LOW)
    k_ref[...] = dot(rows, wk_ref[...]).astype(LOW)
    v_ref[...] = dot(rows, wv_ref[...]).astype(LOW)
    for pair in range(GROUP // 2):
        lanes = slice(pair * PAIR, (pair + 1) * PAIR)
        mixed, inverse = attend_pair(q_ref[:, lanes], k_ref[:, lanes], v_ref[:, lanes], soft_ref, 2 * pair, 512)
        mixed_ref[:, lanes] = mixed.astype(LOW)
        inv_ref[:, lanes] = inverse
    first_ref[...] += dot(mixed_ref[...], wo_ref[...])

    @pl.when(step == steps - 1)
    def _():
        gain = gain_two_ref[...]

        def body(rows, _):
            normed[rows, :] = (normalise(first_ref[rows, :])[0] * gain).astype(LOW)

        by_rows(height, 32, body)
        second = normed[...]
        projected = dot(second, route_ref[...], NT)
        projected_ref[...] = projected
        route_column = to_column(ids_ref[m : m + 1, :].astype(F32)).astype(jnp.int32)
        gate = route_probs(projected, embed_ref[...], route_column)[-1]
        parts = spread_parts(gate)
        slot_row = slot_line(m, ids_ref, slot_ids_ref, keep_ref, slot_cap)
        block = 256
        for begin in range(0, slots, block):
            table = slot_rows(slot_row, begin, block)
            sent_ref[begin : begin + block, :] = dot(table, second).astype(LOW)
            gathered = jnp.sum(dot(table, parts), axis=1, keepdims=True)
            for w in range(begin // slot_cap, (begin + block) // slot_cap):
                column = gathered[w * slot_cap - begin : (w + 1) * slot_cap - begin, :]
                row = jnp.sum(jnp.where(diagonal(slot_cap), column, 0.0), axis=0, keepdims=True)
                gates_ref[w] = jnp.broadcast_to(row, (8, 128))


def forward_stage(m, tokens, gains, weights, w_route, embed, ids, slot_cap, moves, pushes, cid):
    tok_count, width = tokens.shape[1:]
    experts = embed.shape[0]
    slots = experts * slot_cap
    steps = HEADS // GROUP
    span = GROUP * HEAD_DIM
    one = pl.Buffered(1)
    fixed = lambda shape: pl.BlockSpec(shape, lambda i: (0,) * len(shape), pipeline_mode=one)
    of_m = lambda *shape: pl.BlockSpec((None, *shape), lambda i: (m, 0, 0), pipeline_mode=one)
    columns = lambda height: pl.BlockSpec((height, span), lambda i: (0, i))
    whole = lambda *shape: pl.BlockSpec(shape, lambda i: (0,) * len(shape))
    gain_one, gain_two = gains
    wq, wk, wv, wo = weights
    low = lambda *shape: jax.ShapeDtypeStruct(shape, LOW)
    full = lambda *shape: jax.ShapeDtypeStruct(shape, F32)
    return call_with_moves(
        functools.partial(forward_kernel, m=m, steps=steps, slots=slots, slot_cap=slot_cap),
        moves,
        pushes,
        cid,
        grid=(steps,),
        in_specs=[
            of_m(tok_count, width), fixed((1, width)), columns(width), columns(width), columns(width),
            pl.BlockSpec((span, width), lambda i: (i, 0)), fixed((1, width)), fixed(w_route.shape),
            fixed(embed.shape),
        ]
        + [fixed(ids[0].shape)] * 3,
        out_specs=[
            columns(tok_count), columns(tok_count), columns(tok_count),
            pl.BlockSpec((GROUP, LENGTH, LENGTH), lambda i: (i, 0, 0)),
            columns(tok_count), columns(tok_count), whole(tok_count, width), whole(slots, width),
            whole(experts, 8, 128), whole(tok_count, w_route.shape[0]),
        ],
        out_shape=[
            low(tok_count, width), low(tok_count, width), low(tok_count, width), low(HEADS, LENGTH, LENGTH),
            full(tok_count, width), low(tok_count, width), full(tok_count, width), low(slots, width),
            full(experts, 8, 128), full(tok_count, w_route.shape[0]),
        ],
        scratch_shapes=[pltpu.VMEM((tok_count, width), LOW)],
        cost=pl.CostEstimate(
            flops=30 * 10**9, bytes_accessed=50 * 2**20, transcendentals=HEADS * LENGTH * LENGTH
        ),
        name="forward_stage",
        args=(tokens, gain_one, wq, wk, wv, wo, gain_two, w_route, embed, *ids),
    )


def dispatch_kernel(ids_ref, slot_ids_ref, keep_ref, rows_ref, *out_refs, slots, slot_cap):
    for m, out_ref in enumerate(out_refs):

        @pl.when(pl.program_id(0) == m)
        def _():
            slot_row = slot_line(m, ids_ref, slot_ids_ref, keep_ref, slot_cap)
            for begin in range(0, slots, 256):
                table = slot_rows(slot_row, begin, 256)
                out_ref[begin : begin + 256, :] = dot(table, rows_ref[...]).astype(LOW)


def dispatch(ids, rows, slots, slot_cap):
    micro_count, tok_count, width = rows.shape
    return pl.pallas_call(
        functools.partial(dispatch_kernel, slots=slots, slot_cap=slot_cap),
        grid=(micro_count,),
        in_specs=[pl.BlockSpec(ids[0].shape, lambda m: (0, 0))] * 3
        + [pl.BlockSpec((None, tok_count, width), lambda m: (m, 0, 0))],
        out_specs=[pl.BlockSpec((slots, width), lambda m: (0, 0))] * micro_count,
        out_shape=[jax.ShapeDtypeStruct((slots, width), LOW)] * micro_count,
        compiler_params=pltpu.CompilerParams(vmem_limit_bytes=VMEM_BYTES),
        cost_estimate=pl.CostEstimate(flops=3 * 10**9, bytes_accessed=6 * 2**20, transcendentals=0),
        name="dispatch",
    )(*ids, rows)


def attend_pair_back(query, keys, values, grad, mixed, soft_ref, place, inverses, rows):
    lane = lax.broadcasted_iota(jnp.int32, (1, PAIR), 1)
    scale = LOW(HEAD_DIM**-0.5)
    none = jnp.zeros_like(keys)
    dk_parts, dv_parts, dq_blocks = [None, None], [None, None], []
    for block in range(LENGTH // rows):
        part = slice(block * rows, (block + 1) * rows)
        query_t = (query[part, :] * scale).T
        scaled = grad[part, :].astype(F32) * inverses[part, :]
        inner = scaled * mixed[part, :].astype(F32)
        scaled = scaled.astype(LOW)
        scaled_t = scaled.T
        grad_query = None
        for head in range(2):
            mine = (lane < HEAD_DIM) if head == 0 else (lane >= HEAD_DIM)
            own = slice(head * HEAD_DIM, (head + 1) * HEAD_DIM)
            weights = soft_ref[place + head, part, :]
            grad_soft = dot(scaled, jnp.where(mine, values, none), NT)
            centre = jnp.sum(jnp.where(mine, inner, 0.0), axis=1, keepdims=True)
            grad_scores = (weights.astype(F32) * (grad_soft - centre)).astype(LOW)
            term = dot(grad_scores, jnp.where(mine, keys, none))
            grad_query = term if grad_query is None else grad_query + term
            dk = dot(query_t[own, :], grad_scores)
            dv = dot(scaled_t[own, :], weights)
            dk_parts[head] = dk if dk_parts[head] is None else dk_parts[head] + dk
            dv_parts[head] = dv if dv_parts[head] is None else dv_parts[head] + dv
        dq_blocks.append(grad_query * HEAD_DIM**-0.5)
    return (
        jnp.concatenate(dq_blocks, axis=0),
        jnp.concatenate(dk_parts, axis=0).T,
        jnp.concatenate(dv_parts, axis=0).T,
    )


def backward_kernel(
    tokens_ref, cot_ref, gain_one_ref, wq_ref, wk_ref, wv_ref, wo_ref, gain_two_ref, route_ref, embed_ref,
    ids_ref, slot_ids_ref, keep_ref, first_ref, projected_ref, home_ref, dots_ref,
    q_ref, k_ref, v_ref, mixed_ref, soft_ref, inv_ref,
    dwq_ref, dwk_ref, dwv_ref, dwo_ref, gtok_ref, small_ref,
    grad_first, branch, normed_t, total, mixed_grad, dq_sc, dk_sc, dv_sc, soft_buf, soft_sem,
    *, m, steps, slots, slot_cap,
):
    step = pl.program_id(0)
    height, width = tokens_ref.shape
    experts, router_dim = embed_ref.shape
    pairs = GROUP // 2

    def soft_pair(pair):
        at = step * GROUP + 2 * pair
        return pltpu.make_async_copy(soft_ref.at[pl.ds(at, 2)], soft_buf.at[pair % 2], soft_sem.at[pair % 2])

    @pl.when(step == 0)
    def _():
        soft_pair(0).start()
        gain_one, gain_two = gain_one_ref[...], gain_two_ref[...]

        def ahead(rows, _):
            branch[rows, :] = (normalise(tokens_ref[rows, :].astype(F32))[0] * gain_one).astype(LOW)

        by_rows(height, 32, ahead)
        normed_t[...] = branch[...].T
        slot_row = slot_line(m, ids_ref, slot_ids_ref, keep_ref, slot_cap)
        slot_column = to_column(slot_row.astype(F32)).astype(jnp.int32)
        route_column = to_column(ids_ref[m : m + 1, :].astype(F32)).astype(jnp.int32)
        columns = [
            jnp.sum(jnp.where(diagonal(slot_cap), dots_ref[w, 0:1, :], 0.0), axis=1, keepdims=True)
            for w in range(experts)
        ]
        dots = spread_parts(jnp.concatenate(columns, axis=0))
        grads = []
        block = 256
        for begin in range(0, height, block):
            table = token_rows(slot_column[begin : begin + block, :], slots)
            grad_first[begin : begin + block, :] = dot(table, home_ref[...])
            grads.append(jnp.sum(dot(table, dots), axis=1, keepdims=True))
        grad_gate = jnp.concatenate(grads, axis=0)
        projected, embed_rows = projected_ref[...], embed_ref[...]
        unit, inverse, anchor, anchor_inverse, probs, picked, gate = route_probs(
            projected, embed_rows, route_column
        )
        grad_logits = grad_gate * gate * (jnp.where(picked, 1.0, 0.0) - probs)
        grad_unit = 3.0 * dot(grad_logits, anchor, NN, lax.Precision.HIGHEST)
        grad_anchor = 3.0 * dot(grad_logits, unit, TN, lax.Precision.HIGHEST)
        grad_projected = inverse * grad_unit - inverse**3 * projected * jnp.sum(
            projected * grad_unit, axis=-1, keepdims=True
        )
        term_embed = anchor_inverse * grad_anchor - anchor_inverse**3 * embed_rows * jnp.sum(
            embed_rows * grad_anchor, axis=-1, keepdims=True
        )
        parts = three_parts(grad_projected)
        for begin in range(0, height, block):
            some = slice(begin, begin + block)
            grad_first[some, :] += sum(dot(part[some, :], route_ref[...]) for part in parts)
        thirds = (dq_sc, dk_sc, dv_sc)
        third = width // 3

        def middle(rows, gathered):
            normed_two, inverse_two = normalise(first_ref[rows, :])
            second = (normed_two * gain_two).astype(LOW)
            for at, ref in enumerate(thirds):
                ref[rows, :] = second[:, at * third : (at + 1) * third]
            grad_second = grad_first[rows, :]
            value = cot_ref[rows, :].astype(F32) + normalise_back(grad_second * gain_two, normed_two, inverse_two)
            grad_first[rows, :] = value
            branch[rows, :] = value.astype(LOW)
            return gathered + fold_rows(grad_second * normed_two)

        gathered = by_rows(height, 32, middle, jnp.zeros((8, width), F32))
        small_ref[...] = jnp.zeros_like(small_ref)
        for at, ref in enumerate(thirds):
            small_ref[0:router_dim, at * third : (at + 1) * third] = sum(dot(part, ref[...], TN) for part in parts)
        small_ref[router_dim + 1 : router_dim + 2, 0:width] = jnp.sum(gathered, axis=0, keepdims=True)
        small_ref[0:experts, width : width + router_dim] = term_embed
        total[...] = jnp.zeros_like(total)

    rows = branch[...]
    dwo_ref[...] = dot(mixed_ref[...], rows, TN).astype(LOW)
    mixed_grad[...] = dot(rows, wo_ref[...], NT).astype(LOW)
    for pair in range(pairs):
        lanes = slice(pair * PAIR, (pair + 1) * PAIR)
        soft_pair(pair).wait()
        if pair + 1 < pairs:
            soft_pair(pair + 1).start()
        else:

            @pl.when(step + 1 < steps)
            def _():
                soft_pair(pairs).start()

        dq, dk, dv = attend_pair_back(
            q_ref[:, lanes], k_ref[:, lanes], v_ref[:, lanes], mixed_grad[:, lanes], mixed_ref[:, lanes],
            soft_buf.at[pair % 2], 0, inv_ref[:, lanes], 512,
        )
        dq_sc[:, lanes] = dq.astype(LOW)
        dk_sc[:, lanes] = dk.astype(LOW)
        dv_sc[:, lanes] = dv.astype(LOW)
    normed_rows = normed_t[...]
    for grad_ref, weight_ref, out_ref in (
        (dq_sc, wq_ref, dwq_ref), (dk_sc, wk_ref, dwk_ref), (dv_sc, wv_ref, dwv_ref)
    ):
        grad = grad_ref[...]
        out_ref[...] = dot(normed_rows, grad).astype(LOW)
        total[...] += dot(grad, weight_ref[...], NT)

    @pl.when(step == steps - 1)
    def _():
        gain_one = gain_one_ref[...]

        def behind(rows, gathered):
            normed_one, inverse_one = normalise(tokens_ref[rows, :].astype(F32))
            grad = total[rows, :]
            value = grad_first[rows, :] + normalise_back(grad * gain_one, normed_one, inverse_one)
            gtok_ref[rows, :] = value.astype(LOW)
            return gathered + fold_rows(grad * normed_one)

        gathered = by_rows(height, 32, behind, jnp.zeros((8, width), F32))
        small_ref[router_dim : router_dim + 1, 0:width] = jnp.sum(gathered, axis=0, keepdims=True)


def backward_stage(
    m, tokens, grad_out, gains, weights, w_route, embed, ids, kept, home, slot_cap, moves, pushes, cid
):
    tok_count, width = tokens.shape[1:]
    experts, router_dim = embed.shape
    slots = experts * slot_cap
    steps = HEADS // GROUP
    span = GROUP * HEAD_DIM
    one = pl.Buffered(1)
    fixed = lambda shape: pl.BlockSpec(shape, lambda i: (0,) * len(shape), pipeline_mode=one)
    of_m = lambda *shape: pl.BlockSpec((None, *shape), lambda i: (m, 0, 0), pipeline_mode=one)
    columns = lambda height: pl.BlockSpec((height, span), lambda i: (0, i))
    lines = pl.BlockSpec((span, width), lambda i: (i, 0))
    gain_one, gain_two = gains
    wq, wk, wv, wo = weights
    first, projected, q, k, v, mixed, soft, inverses = kept
    low = lambda *shape: jax.ShapeDtypeStruct(shape, LOW)
    small = (-(-max(experts, router_dim + 2) // 8) * 8, width + 128)
    return call_with_moves(
        functools.partial(backward_kernel, m=m, steps=steps, slots=slots, slot_cap=slot_cap),
        moves,
        pushes,
        cid,
        grid=(steps,),
        in_specs=[
            of_m(tok_count, width), of_m(tok_count, width), fixed((1, width)), columns(width), columns(width),
            columns(width), lines, fixed((1, width)), fixed(w_route.shape), fixed(embed.shape),
            *[fixed(ids[0].shape)] * 3, fixed(first.shape), fixed(projected.shape), fixed(home[0].shape), fixed(home[1].shape),
            columns(tok_count), columns(tok_count), columns(tok_count), columns(tok_count),
            pl.BlockSpec(memory_space=pl.ANY), columns(tok_count),
        ],
        out_specs=[
            columns(width), columns(width), columns(width), lines, fixed((tok_count, width)), fixed(small),
        ],
        out_shape=[
            low(width, width), low(width, width), low(width, width), low(width, width), low(tok_count, width),
            jax.ShapeDtypeStruct(small, F32),
        ],
        scratch_shapes=[
            pltpu.VMEM((tok_count, width), F32), pltpu.VMEM((tok_count, width), LOW),
            pltpu.VMEM((width, tok_count), LOW), pltpu.VMEM((tok_count, width), F32),
        ]
        + [pltpu.VMEM((tok_count, span), LOW)] * 4
        + [pltpu.VMEM((2, 2, LENGTH, LENGTH), LOW), pltpu.SemaphoreType.DMA((2,))],
        cost=pl.CostEstimate(flops=40 * 10**9, bytes_accessed=50 * 2**20, transcendentals=0),
        name="backward_stage",
        args=(
            tokens, grad_out, gain_one, wq, wk, wv, wo, gain_two, w_route, embed, *ids, first,
            projected, *home, q, k, v, mixed, soft, inverses,
        ),
    )


def finish_kernel(*refs, micro_count, blocks, slots, slot_cap, tiles, wide_steps, per_tile):
    ids_ref, slot_ids_ref, keep_ref, embed_ref = refs[:4]
    ins, refs = refs[4 : 4 + 4 * micro_count], refs[4 + 4 * micro_count :]
    near_in, near_outer = refs[:2]
    far_in, far_outer = refs[2 : 2 + tiles], refs[2 + tiles : 2 + 2 * tiles]
    big_ref = refs[2 + 2 * tiles]
    out_ref, grad_ref, din_ref, douter_ref, *big_outs = refs[3 + 2 * tiles :]
    step = pl.program_id(0)
    rows, width = out_ref.shape
    for m in range(micro_count):
        first_ref, projected_ref, home_ref, gtok_ref = ins[4 * m : 4 * m + 4]
        for block in range(blocks):

            @pl.when(step == m * blocks + block)
            def _():
                some = slice(block * rows, (block + 1) * rows)
                slot_row = slot_line(m, ids_ref, slot_ids_ref, keep_ref, slot_cap)
                slot_column = to_column(slot_row[:, some].astype(F32)).astype(jnp.int32)
                route_column = to_column(ids_ref[m : m + 1, some].astype(F32)).astype(jnp.int32)
                gate = route_probs(projected_ref[...], embed_ref[...], route_column)[-1]
                returned = dot(token_rows(slot_column, slots), home_ref[...])
                out_ref[...] = (first_ref[...] + gate * returned).astype(LOW)
                grad_ref[...] = gtok_ref[...]

    for t in range(tiles):

        @pl.when((step >= t * per_tile) & (step < (t + 1) * per_tile))
        def _():
            din_ref[0] = near_in[...] + sum(far_in[t][j].astype(F32) for j in range(far_in[t].shape[0]))
            douter_ref[0] = near_outer[...] + sum(far_outer[t][j].astype(F32) for j in range(far_outer[t].shape[0]))

    for k, big_out in enumerate(big_outs):
        big_out[...] = big_ref[:, k * width : (k + 1) * width].astype(F32)


def finish(ids, embed, parts, near, far, big, slots, slot_cap):
    micro_count, tok_count = ids[0].shape
    width = parts[0][0].shape[1]
    near_in, near_outer = near
    tiles = len(far) // 2
    spread, _, tile = far[0].shape
    units = near_in.shape[1]
    span = 256 if tile % 256 == 0 else 128
    wide_steps, per_tile = units // span, tile // span
    rows = 256
    blocks = tok_count // rows
    steps = micro_count * blocks
    lines = big.shape[0] // steps
    whole = lambda shape: pl.BlockSpec(shape, lambda i: (0, 0), pipeline_mode=pl.Buffered(1))
    in_specs, args = [whole(ids[0].shape)] * 3 + [whole(embed.shape)], [*ids, embed]
    for at, (first, projected, home, gtok) in enumerate(parts):
        place = lambda i, at=at: (jnp.clip(i - at * blocks, 0, blocks - 1), 0)
        in_specs += [
            pl.BlockSpec((rows, width), place), pl.BlockSpec((rows, projected.shape[1]), place), whole(home.shape),
            pl.BlockSpec((rows, width), place),
        ]
        args += [first, projected, home, gtok]
    near_at = lambda i: jnp.minimum(i, wide_steps - 1)
    far_at = lambda i, t: jnp.clip(i - t * per_tile, 0, per_tile - 1)
    in_specs += [
        pl.BlockSpec((width, span), lambda i: (0, near_at(i))), pl.BlockSpec((span, width), lambda i: (near_at(i), 0)),
    ]
    in_specs += [pl.BlockSpec((spread, width, span), lambda i, t=t: (0, 0, far_at(i, t))) for t in range(tiles)]
    in_specs += [pl.BlockSpec((spread, span, width), lambda i, t=t: (0, far_at(i, t), 0)) for t in range(tiles)]
    in_specs += [pl.BlockSpec((lines, big.shape[1]), lambda i: (i, 0))]
    row_out = pl.BlockSpec((None, rows, width), lambda i: (i // blocks, i % blocks, 0))
    line_out = pl.BlockSpec((lines, width), lambda i: (i, 0))
    kinds = big.shape[1] // width
    return pl.pallas_call(
        functools.partial(
            finish_kernel, micro_count=micro_count, blocks=blocks, slots=slots, slot_cap=slot_cap, tiles=tiles,
            wide_steps=wide_steps, per_tile=per_tile,
        ),
        grid=(steps,),
        in_specs=in_specs,
        out_specs=[
            row_out, row_out, pl.BlockSpec((1, width, span), lambda i: (0, 0, near_at(i))),
            pl.BlockSpec((1, span, width), lambda i: (0, near_at(i), 0)),
        ]
        + [line_out] * kinds,
        out_shape=[jax.ShapeDtypeStruct((micro_count, tok_count, width), LOW)] * 2
        + [jax.ShapeDtypeStruct((1, *near_in.shape), F32), jax.ShapeDtypeStruct((1, *near_outer.shape), F32)]
        + [jax.ShapeDtypeStruct((big.shape[0], width), F32)] * kinds,
        compiler_params=pltpu.CompilerParams(vmem_limit_bytes=VMEM_BYTES),
        cost_estimate=pl.CostEstimate(flops=3 * 10**9, bytes_accessed=56 * 2**20, transcendentals=0),
        name="finish",
    )(*args, near_in, near_outer, *far, big)


def gelu_and_slope(values):
    ratio = 1.0 / (1.0 + jnp.abs(values) * (0.3275911 * 0.7071067811865476))
    bell = jnp.exp(values * values * -0.5)
    series = 0.5 * 1.061405429
    for factor in (-1.453152027, 1.421413741, -0.284496736, 0.254829592):
        series = series * ratio + 0.5 * factor
    tail = series * ratio * bell
    below = jnp.where(values >= 0.0, 1.0 - tail, tail)
    return values * below, below + values * bell * 0.3989422804014327


def expert_kernel(*refs, more, last, per, steps, slot_cap):
    rows_ref, cot_ref, gate_ref, own_in, own_outer = refs[:5]
    far_in, far_outer = refs[5 : 5 + per], refs[5 + per : 5 + 2 * per]
    refs = refs[5 + 2 * per :]
    if more:
        old_in, old_outer = refs[:2]
        refs = refs[2:]
    result_ref, sent_ref, dots_ref, din_ref, douter_ref = refs[:5]
    refs = refs[5:]
    if last:
        far_din, far_douter = refs[:2]
        refs = refs[2:]
    grad_sc, rows_t, acc_result, acc_sent, first_buf, second_buf, sems = refs
    step = pl.program_id(0)
    slot = lax.rem(step, 2)
    sources = rows_ref.shape[0] // slot_cap
    tile = first_buf.shape[2]

    def fetch(i):
        if i < per:
            first = own_in.at[:, i * tile : (i + 1) * tile]
            second = own_outer.at[i * tile : (i + 1) * tile, :]
        else:
            first, second = far_in[i % per].at[i // per - 1], far_outer[i % per].at[i // per - 1]
        return (
            pltpu.make_async_copy(first, first_buf.at[i % 2], sems.at[0, i % 2]),
            pltpu.make_async_copy(second, second_buf.at[i % 2], sems.at[1, i % 2]),
        )

    @pl.when(step == 0)
    def _():
        for copy in fetch(0):
            copy.start()
        for w in range(sources):
            part = slice(w * slot_cap, (w + 1) * slot_cap)
            gate = jnp.sum(jnp.where(diagonal(slot_cap), gate_ref[w, 0:1, :], 0.0), axis=1, keepdims=True)
            grad_sc[part, :] = (cot_ref[part, :].astype(F32) * gate).astype(LOW)
        rows_t[...] = rows_ref[...].T
        acc_result[...] = jnp.zeros_like(acc_result)
        acc_sent[...] = jnp.zeros_like(acc_sent)

    for i in range(steps):

        @pl.when(step == i)
        def _():
            for copy in fetch(i):
                copy.wait()
            if i + 1 < steps:
                for copy in fetch(i + 1):
                    copy.start()

    first, second = first_buf[slot], second_buf[slot]
    hidden, slope = gelu_and_slope(dot(rows_ref[...], first))
    hidden = hidden.astype(LOW)
    grad_rows = grad_sc[...]
    grad_pre = (dot(grad_rows, second, NT) * slope).astype(LOW)
    acc_result[...] += dot(hidden, second)
    acc_sent[...] += dot(grad_pre, first, NT)
    din = dot(rows_t[...], grad_pre)
    douter = dot(hidden, grad_rows, TN)
    if more:
        din += old_in[...]
        douter += old_outer[...]
    if not last:
        din_ref[...] = din
        douter_ref[...] = douter
    else:

        @pl.when(step < per)
        def _():
            din_ref[...] = din
            douter_ref[...] = douter

        @pl.when(step >= per)
        def _():
            far_din[...] = din.astype(LOW)
            far_douter[...] = douter.astype(LOW)

    @pl.when(step == steps - 1)
    def _():
        result = acc_result[...].astype(LOW)
        result_ref[...] = result
        sent_ref[...] = acc_sent[...].astype(LOW)
        for w in range(sources):
            part = slice(w * slot_cap, (w + 1) * slot_cap)
            products = cot_ref[part, :].astype(F32) * result[part, :].astype(F32)
            column = jnp.sum(products, axis=1, keepdims=True)
            row = jnp.sum(jnp.where(diagonal(slot_cap), column, 0.0), axis=0, keepdims=True)
            dots_ref[w] = jnp.broadcast_to(row, (8, 128))


def tile_of(units):
    return min(512, units)


def expert_stage(rows, cot, gates, weights, old, last, slot_cap, moves, pushes, cid):
    own_in, own_outer, far_in, far_outer = weights
    width, units = own_in.shape
    count = lax.axis_size("narrow")
    height = rows.shape[0]
    tile = tile_of(units)
    per = units // tile
    steps = count * per
    whole = lambda shape: pl.BlockSpec(shape, lambda i: (0,) * len(shape))
    anywhere = pl.BlockSpec(memory_space=pl.ANY)
    din_spec = pl.BlockSpec((None, width, tile), lambda i: (i, 0, 0))
    douter_spec = pl.BlockSpec((None, tile, width), lambda i: (i, 0, 0))
    out_specs = [whole((height, width)), whole((height, width)), whole(gates.shape)]
    out_shape = [
        jax.ShapeDtypeStruct((height, width), LOW),
        jax.ShapeDtypeStruct((height, width), LOW),
        jax.ShapeDtypeStruct(gates.shape, F32),
    ]
    if last:
        near = lambda i: jnp.minimum(i, per - 1)
        away = lambda i: jnp.maximum(i - per, 0)
        out_specs += [
            pl.BlockSpec((width, tile), lambda i: (0, near(i))),
            pl.BlockSpec((tile, width), lambda i: (near(i), 0)),
            pl.BlockSpec((None, width, tile), lambda i: (away(i), 0, 0)),
            pl.BlockSpec((None, tile, width), lambda i: (away(i), 0, 0)),
        ]
        out_shape += [
            jax.ShapeDtypeStruct((width, units), F32),
            jax.ShapeDtypeStruct((units, width), F32),
            jax.ShapeDtypeStruct((steps - per, width, tile), LOW),
            jax.ShapeDtypeStruct((steps - per, tile, width), LOW),
        ]
    else:
        out_specs += [din_spec, douter_spec]
        out_shape += [
            jax.ShapeDtypeStruct((steps, width, tile), F32),
            jax.ShapeDtypeStruct((steps, tile, width), F32),
        ]
    return call_with_moves(
        functools.partial(
            expert_kernel, more=bool(old), last=last, per=per, steps=steps, slot_cap=slot_cap
        ),
        moves,
        pushes,
        cid,
        grid=(steps,),
        in_specs=[whole((height, width)), whole((height, width)), whole(gates.shape)]
        + [anywhere] * (2 + 2 * per)
        + ([din_spec, douter_spec] if old else []),
        out_specs=out_specs,
        out_shape=out_shape,
        scratch_shapes=[
            pltpu.VMEM((height, width), LOW),
            pltpu.VMEM((width, height), LOW),
            pltpu.VMEM((height, width), F32),
            pltpu.VMEM((height, width), F32),
            pltpu.VMEM((2, width, tile), LOW),
            pltpu.VMEM((2, tile, width), LOW),
            pltpu.SemaphoreType.DMA((2, 2)),
        ],
        cost=pl.CostEstimate(
            flops=12 * height * width * units * count, bytes_accessed=34 * 2**20, transcendentals=0
        ),
        name="expert_stage",
        args=(rows, cot, gates, own_in, own_outer, *far_in, *far_outer, *old),
    )


def local(
    tokens,
    grad_out,
    route_ids,
    slot_ids,
    keep_ids,
    gain_one,
    w_query,
    w_key,
    w_value,
    w_out,
    gain_two,
    w_route,
    embed,
    w_in,
    w_outer,
):
    micro_count, tok_count, feat_width = tokens.shape
    expert_count = embed.shape[0]
    slot_cap = max(2, tok_count // expert_count)
    slots = expert_count * slot_cap
    own_in, own_outer = w_in[0], w_outer[0]
    units = own_in.shape[1]
    tile = tile_of(units)
    per = units // tile
    weight_pushes = [
        (own_in, lambda ref, j, t=t: ref.at[:, t * tile : (t + 1) * tile], (feat_width, tile)) for t in range(per)
    ] + [
        (own_outer, lambda ref, j, t=t: ref.at[t * tile : (t + 1) * tile, :], (tile, feat_width)) for t in range(per)
    ]
    early = len(weight_pushes) // 3
    gains = (gain_one[None], gain_two[None])
    mixers = (w_query, w_key, w_value, w_out)
    ids = (route_ids, slot_ids, keep_ids)
    router = (w_route.T, embed, ids)

    def boxes(rows):
        return rows.reshape((expert_count, slot_cap) + rows.shape[1:])

    def flat(boxed):
        return boxed.reshape((expert_count * slot_cap,) + boxed.shape[2:])

    cot_boxes = [boxes(rows) for rows in dispatch(ids, grad_out, slots, slot_cap)]
    (*ahead_0, sent, gates, projected), (cot_0,), far_a = forward_stage(
        0, tokens, gains, mixers, *router, slot_cap, (cot_boxes[0],), weight_pushes[:early], 1
    )
    ahead_0.append(projected)
    (*ahead_1, next_sent, next_gates, projected), (sent_0, gates_0, cot_1), far_b = forward_stage(
        1, tokens, gains, mixers, *router, slot_cap, (boxes(sent), gates, cot_boxes[1]), weight_pushes[early:], 2
    )
    ahead_1.append(projected)

    far = [*far_a, *far_b]
    weights = (own_in, own_outer, far[:per], far[per:])
    (result_0, grad_0, dots_0, *old), (sent_1, gates_1), _ = expert_stage(
        flat(sent_0), flat(cot_0), gates_0, weights, (), False, slot_cap, (boxes(next_sent), next_gates), (), 3
    )
    (result_1, grad_1, dots_1, near_din, near_douter, far_din, far_douter), (home_grad_0, home_dots_0), _ = expert_stage(
        flat(sent_1), flat(cot_1), gates_1, weights, tuple(old), True, slot_cap, (boxes(grad_0), dots_0), (), 4
    )
    grad_pushes = [
        (far_din, lambda ref, j, t=t: ref.at[j * per + t], (feat_width, tile)) for t in range(per)
    ] + [
        (far_douter, lambda ref, j, t=t: ref.at[j * per + t], (tile, feat_width)) for t in range(per)
    ]
    later = len(grad_pushes) // 2

    def kept(ahead):
        q, k, v, soft, inverses, mixed, first, projected = ahead
        return first, projected, q, k, v, mixed, soft, inverses

    (*big_0, gtok_0, small_0), (home_grad_1, home_dots_1), got_a = backward_stage(
        0, tokens, grad_out, gains, mixers, *router, kept(ahead_0), (flat(home_grad_0), home_dots_0), slot_cap,
        (boxes(grad_1), dots_1), grad_pushes[:later], 5
    )
    (*big_1, gtok_1, small_1), (home_result_0, home_result_1), got_b = backward_stage(
        1, tokens, grad_out, gains, mixers, *router, kept(ahead_1), (flat(home_grad_1), home_dots_1), slot_cap,
        (boxes(result_0), boxes(result_1)), grad_pushes[later:], 6
    )
    big, small = reduce_everywhere(list(zip(big_0, big_1)), (small_0, small_1), 7)
    block_out, grad_tokens, grad_in, grad_outer, *big = finish(
        ids, embed,
        (
            (ahead_0[6], ahead_0[7], flat(home_result_0), gtok_0),
            (ahead_1[6], ahead_1[7], flat(home_result_1), gtok_1),
        ),
        (near_din, near_douter), [*got_a, *got_b], big, slots, slot_cap,
    )
    router_dim = w_route.shape[1]
    return (
        block_out,
        grad_tokens,
        small[router_dim, :feat_width],
        *big,
        small[router_dim + 1, :feat_width],
        small[:router_dim, :feat_width].T,
        small[:expert_count, feat_width : feat_width + router_dim],
        grad_in,
        grad_outer,
    )


def solution(mesh):
    tokens_spec = P(None, ("wide", "narrow"), None)
    ids_spec = P(None, ("wide", "narrow"))
    in_spec, outer_spec = P("wide", None, "narrow"), P("wide", "narrow", None)
    return jax.shard_map(
        local,
        mesh=mesh,
        in_specs=(tokens_spec,) * 2 + (ids_spec,) * 3 + (P(),) * 8 + (in_spec, outer_spec),
        out_specs=(tokens_spec,) * 2 + (P(),) * 8 + (in_spec, outer_spec),
        check_vma=False,
    )
```

```python
import functools

import jax
import jax.numpy as jnp
from jax import lax
from jax.experimental import pallas as pl
from jax.experimental.pallas import tpu as pltpu
from jax.sharding import PartitionSpec as P

D = 768
HEADS = 12
HEAD_DIM = 64
LENGTH = 1024
PAIR = 2 * HEAD_DIM
GROUP = 4
PIECES = 4
NN = (((1,), (0,)), ((), ()))
NT = (((1,), (1,)), ((), ()))
TN = (((0,), (0,)), ((), ()))
LOW = jnp.bfloat16
F32 = jnp.float32
VMEM_BYTES = 60 << 20


def dot(left, right, dims=NN, precise=None):
    return lax.dot_general(left, right, dims, precision=precise, preferred_element_type=F32)


def normalise(values):
    centred = values - jnp.mean(values, axis=-1, keepdims=True)
    inverse = lax.rsqrt(jnp.mean(centred * centred, axis=-1, keepdims=True) + 1e-05)
    return centred * inverse, inverse


def normalise_back(grad, normed, inverse):
    return inverse * (
        grad
        - jnp.mean(grad, axis=-1, keepdims=True)
        - normed * jnp.mean(grad * normed, axis=-1, keepdims=True)
    )


def by_rows(count, size, body, carry=None):
    return lax.fori_loop(
        0, count // size, lambda i, c: body(pl.ds(pl.multiple_of(i * size, size), size), c), carry
    )


def fold_rows(values):
    return jnp.sum(values.reshape(values.shape[0] // 8, 8, values.shape[1]), axis=0)


def three_parts(values):
    high = values.astype(LOW)
    rest = values - high.astype(F32)
    middle = rest.astype(LOW)
    return high, middle, (rest - middle.astype(F32)).astype(LOW)


def spread_parts(column):
    lane = lax.broadcasted_iota(jnp.int32, (1, 128), 1)
    high, middle, low = (part.astype(F32) for part in three_parts(column))
    return jnp.where(lane == 0, high, jnp.where(lane == 1, middle, jnp.where(lane == 2, low, 0.0))).astype(LOW)


def diagonal(rows):
    shape = (rows, 128)
    return lax.broadcasted_iota(jnp.int32, shape, 0) == lax.broadcasted_iota(jnp.int32, shape, 1)


def to_column(row):
    pieces = [
        jnp.sum(jnp.where(diagonal(128), row[:, first : first + 128], 0.0), axis=1, keepdims=True)
        for first in range(0, row.shape[1], 128)
    ]
    return jnp.concatenate(pieces, axis=0)


def unit_length(rows):
    inverse = lax.rsqrt(jnp.sum(rows * rows, axis=-1, keepdims=True) + 1.0)
    return rows * inverse, inverse


def route_probs(projected, embed_rows, route_column):
    unit, inverse = unit_length(projected)
    anchor, anchor_inverse = unit_length(embed_rows)
    logits = 3.0 * dot(unit, anchor, NT, lax.Precision.HIGHEST)
    weights = jnp.exp(logits - jnp.max(logits, axis=-1, keepdims=True))
    probs = weights / jnp.sum(weights, axis=-1, keepdims=True)
    lane = lax.broadcasted_iota(jnp.int32, (1, probs.shape[1]), 1)
    picked = route_column == lane
    gate = jnp.sum(jnp.where(picked, probs, 0.0), axis=-1, keepdims=True)
    return unit, inverse, anchor, anchor_inverse, probs, picked, gate


def slot_line(m, route_ref, slot_ref, keep_ref, slot_cap):
    line = slice(m, m + 1)
    return jnp.where(keep_ref[line, :] > 0, route_ref[line, :] * slot_cap + slot_ref[line, :], -1)


def piece_line(m, route_ref, slot_ref, keep_ref, low, high):
    line = slice(m, m + 1)
    slot = slot_ref[line, :]
    inside = (keep_ref[line, :] > 0) & (slot >= low) & (slot < high)
    return jnp.where(inside, route_ref[line, :] * (high - low) + slot - low, -1)


def slot_rows(slot_row, first, count):
    slot = lax.broadcasted_iota(jnp.int32, (count, slot_row.shape[1]), 0) + first
    return jnp.where(slot == slot_row, 1.0, 0.0).astype(LOW)


def token_rows(slot_column, slots):
    lane = lax.broadcasted_iota(jnp.int32, (slot_column.shape[0], slots), 1)
    return jnp.where(lane == slot_column, 1.0, 0.0).astype(LOW)


MESH = pl.DeviceIdType.MESH


def call_with_moves(
    body, moves, pushes, cid, *, grid, in_specs, out_specs, out_shape, scratch_shapes=(), cost, name, args, late=False
):
    members, spread = lax.axis_size("wide"), lax.axis_size("narrow")
    n_in, n_out, n_moves, n_scratch = len(in_specs), len(out_specs), len(moves), len(scratch_shapes)
    arrays = []
    for array, _, _ in pushes:
        if not any(array is known for known in arrays):
            arrays.append(array)
    which = [next(k for k, known in enumerate(arrays) if known is array) for array, _, _ in pushes]
    n_arrays, n_pushes = len(arrays), len(pushes)

    def kernel(*refs):
        ins, refs = refs[:n_in], refs[n_in:]
        sources, refs = refs[:n_moves], refs[n_moves:]
        pushed, refs = refs[:n_arrays], refs[n_arrays:]
        outs, refs = refs[:n_out], refs[n_out:]
        targets, refs = refs[:n_moves], refs[n_moves:]
        landings, refs = refs[:n_pushes], refs[n_pushes:]
        scratch, refs = refs[:n_scratch], refs[n_scratch:]
        stages, refs = refs[:n_moves], refs[n_moves:]
        send_sem, recv_sem, own_sem, push_send, push_recv = refs
        me, side = lax.axis_index("wide"), lax.axis_index("narrow")
        step = pl.program_id(0)

        def piece(i, w):
            return sources[i].at[w, moves[i][1] : moves[i][2]]

        def remote(i, d):
            peer = lax.rem(me + d, members)
            return pltpu.make_async_remote_copy(
                src_ref=piece(i, peer),
                dst_ref=targets[i].at[me],
                send_sem=send_sem.at[i, d],
                recv_sem=recv_sem.at[i, d],
                device_id={"wide": peer},
                device_id_type=MESH,
            )

        def push(k, j, part):
            size = pushes[k][2][0] // PIECES
            some = slice(part * size, (part + 1) * size)
            return pltpu.make_async_remote_copy(
                src_ref=pushes[k][1](pushed[which[k]], j).at[some],
                dst_ref=landings[k].at[j].at[some],
                send_sem=push_send.at[k, j * PIECES + part],
                recv_sem=push_recv.at[k, j * PIECES + part],
                device_id={"narrow": lax.rem(side + j + 1, spread)},
                device_id_type=MESH,
            )

        def settle(k):
            for j in range(spread - 1):
                for part in range(PIECES):
                    push(k, j, part).wait()

        @pl.when(step == 0)
        def _():
            barrier = pltpu.get_barrier_semaphore()
            count = 0
            if n_moves:
                for d in range(1, members):
                    pl.semaphore_signal(
                        barrier, inc=1, device_id={"wide": lax.rem(me + d, members)}, device_id_type=MESH
                    )
                count += members - 1
            if n_pushes:
                for j in range(spread - 1):
                    pl.semaphore_signal(
                        barrier, inc=1, device_id={"narrow": lax.rem(side + j + 1, spread)}, device_id_type=MESH
                    )
                count += spread - 1
            pl.semaphore_wait(barrier, count)
            for i in range(n_moves):
                for d in range(1, members):
                    remote(i, d).start()
                pltpu.make_async_copy(piece(i, me), stages[i], own_sem.at[i]).start()
            for k in range(n_pushes):
                for j in range(spread - 1):
                    for part in range(PIECES):
                        push(k, j, part).start()

        if late:
            body(*ins, *outs, *scratch, landings=landings, settle=settle)
        else:
            body(*ins, *outs, *scratch)

        @pl.when(step == grid[0] - 1)
        def _():
            for i in range(n_moves):
                pltpu.make_async_copy(piece(i, me), stages[i], own_sem.at[i]).wait()
                pltpu.make_async_copy(stages[i], targets[i].at[me], own_sem.at[i]).start()
            for i in range(n_moves):
                pltpu.make_async_copy(stages[i], targets[i].at[me], own_sem.at[i]).wait()
                for d in range(1, members):
                    remote(i, d).wait()
            if not late:
                for k in range(n_pushes):
                    settle(k)

    anywhere = pl.BlockSpec(memory_space=pl.ANY)
    results = pl.pallas_call(
        kernel,
        grid=grid,
        in_specs=list(in_specs) + [anywhere] * (n_moves + n_arrays),
        out_specs=list(out_specs) + [anywhere] * (n_moves + n_pushes),
        out_shape=list(out_shape)
        + [jax.ShapeDtypeStruct((a.shape[0], high - low, *a.shape[2:]), a.dtype) for a, low, high in moves]
        + [jax.ShapeDtypeStruct((spread - 1, *shape), a.dtype) for a, _, shape in pushes],
        scratch_shapes=list(scratch_shapes)
        + [pltpu.VMEM((high - low, *a.shape[2:]), a.dtype) for a, low, high in moves]
        + [
            pltpu.SemaphoreType.DMA((max(1, n_moves), members)),
            pltpu.SemaphoreType.DMA((max(1, n_moves), members)),
            pltpu.SemaphoreType.DMA((max(1, n_moves),)),
            pltpu.SemaphoreType.DMA((max(1, n_pushes), spread * PIECES)),
            pltpu.SemaphoreType.DMA((max(1, n_pushes), spread * PIECES)),
        ],
        compiler_params=pltpu.CompilerParams(
            vmem_limit_bytes=VMEM_BYTES, collective_id=cid, has_side_effects=True
        ),
        cost_estimate=cost,
        name=name,
    )(*args, *(move[0] for move in moves), *arrays)
    return results[:n_out], results[n_out : n_out + n_moves], results[n_out + n_moves :]


def reduce_orders(wide_count, narrow_count):
    bits = lambda axis, count: [(axis, 1 << k) for k in range(count.bit_length() - 1)]
    wide, narrow = bits("wide", wide_count), bits("narrow", narrow_count)
    core, x_bits, z_bits = wide[:1], wide[1:2], wide[2:]
    return (
        core + x_bits + narrow + z_bits,
        core + narrow + x_bits + z_bits,
        core + z_bits + x_bits + narrow,
    ) * 2


def halvings(order, rows, columns):
    plan = []
    for _ in order:
        if columns % 256 == 0:
            columns //= 2
            plan.append("columns")
        elif rows % 32 == 0:
            rows //= 2
            plan.append("rows")
        else:
            plan.append("whole")
    return plan


def reduce_kernel(*refs, orders, width, places, sets):
    ins = [refs[k * sets : (k + 1) * sets] for k in range(len(places))]
    refs = refs[len(places) * sets :]
    smalls, refs = refs[:sets], refs[sets:]
    out_ref, small_out, total, result, small_send, small_recv = refs[:6]
    refs = refs[6:]
    parts, stages = len(orders), len(orders[0])
    outgoing = [refs[p * stages : (p + 1) * stages] for p in range(parts)]
    incoming = [refs[(parts + p) * stages : (parts + p + 1) * stages] for p in range(parts)]
    send_sem, recv_sem, back_send, back_recv, small_sems, small_rsems = refs[2 * parts * stages :]
    index = {axis: lax.axis_index(axis) for axis in ("wide", "narrow")}
    rows = total.shape[0]

    def own_bit(axis, bit):
        return lax.rem(index[axis] // bit, 2)

    def partner(axis, bit):
        return {axis: index[axis] + bit - 2 * bit * own_bit(axis, bit)}

    barrier = pltpu.get_barrier_semaphore()
    for axis, bit in orders[0]:
        pl.semaphore_signal(barrier, inc=1, device_id=partner(axis, bit), device_id_type=MESH)
    pl.semaphore_wait(barrier, stages)

    for group, place in zip(ins, places):
        total[:, place : place + group[0].shape[1]] = sum(ref[...].astype(F32) for ref in group)
    small_send[0] = sum(ref[...] for ref in smalls)

    regions = [[(0, rows, p * width, width)] for p in range(parts)]

    def take(region):
        row, height, column, span = region
        if not isinstance(row, int):
            row = pl.multiple_of(row, 16)
        if not isinstance(column, int):
            column = pl.multiple_of(column, 128)
        return pl.ds(row, height), pl.ds(column, span)

    def half(region, how, pick):
        row, height, column, span = region
        if how == "columns":
            return row, height, column + pick * (span // 2), span // 2
        if how == "rows":
            return row + pick * (height // 2), height // 2, column, span
        return region

    plans = [halvings(order, rows, width) for order in orders]

    def there(p, s):
        axis, bit = orders[p][s]
        return pltpu.make_async_remote_copy(
            src_ref=outgoing[p][s],
            dst_ref=incoming[p][s],
            send_sem=send_sem.at[p, s],
            recv_sem=recv_sem.at[p, s],
            device_id=partner(axis, bit),
            device_id_type=MESH,
        )

    def small_there(s):
        axis, bit = orders[0][s]
        return pltpu.make_async_remote_copy(
            src_ref=small_send.at[s],
            dst_ref=small_recv.at[s],
            send_sem=small_sems.at[s],
            recv_sem=small_rsems.at[s],
            device_id=partner(axis, bit),
            device_id_type=MESH,
        )

    def launch(p, s):
        axis, bit = orders[p][s]
        mine = own_bit(axis, bit)
        region, how = regions[p][-1], plans[p][s]
        outgoing[p][s][...] = total[take(half(region, how, 1 - mine))].astype(LOW)
        there(p, s).start()
        regions[p].append(half(region, how, mine))

    for p in range(parts):
        launch(p, 0)
    small_there(0).start()
    for s in range(stages):
        for p in range(parts):
            there(p, s).wait()
            kept = take(regions[p][-1])
            base = outgoing[p][s][...].astype(F32) if plans[p][s] == "whole" else total[kept]
            value = base + incoming[p][s][...].astype(F32)
            if s + 1 < stages:
                total[kept] = value
                launch(p, s + 1)
            else:
                result[kept] = value.astype(LOW)
        small_there(s).wait()
        fresh = small_send[s] + small_recv[s]
        if s + 1 < stages:
            small_send[s + 1] = fresh
            small_there(s + 1).start()
        else:
            small_out[...] = fresh

    def back(p, s):
        axis, bit = orders[p][s]
        spot = take(regions[p][s + 1])
        return pltpu.make_async_remote_copy(
            src_ref=result.at[spot],
            dst_ref=result.at[spot],
            send_sem=back_send.at[p, s],
            recv_sem=back_recv.at[p, s],
            device_id=partner(axis, bit),
            device_id_type=MESH,
        )

    for s in reversed(range(stages)):
        for p in range(parts):
            if plans[p][s] != "whole":
                back(p, s).start()
        for p in range(parts):
            if plans[p][s] != "whole":
                back(p, s).wait()
    out_ref[...] = result[...]


def reduce_everywhere(big, small, cid):
    orders = reduce_orders(lax.axis_size("wide"), lax.axis_size("narrow"))
    places, columns = [], 0
    for group in big:
        places.append(columns)
        columns += group[0].shape[1]
    rows = big[0][0].shape[0]
    sets = len(small)
    width, parts, stages = columns // len(orders), len(orders), len(orders[0])
    buffers = []
    for order in orders:
        height, span = rows, width
        for how in halvings(order, rows, width):
            height, span = (height // 2 if how == "rows" else height), (span // 2 if how == "columns" else span)
            buffers.append(pltpu.VMEM((height, span), LOW))
    vmem = pl.BlockSpec(memory_space=pltpu.VMEM)
    return pl.pallas_call(
        functools.partial(reduce_kernel, orders=orders, width=width, places=places, sets=sets),
        in_specs=[vmem] * ((len(big) + 1) * sets),
        out_specs=[vmem, vmem],
        out_shape=[jax.ShapeDtypeStruct((rows, columns), LOW), jax.ShapeDtypeStruct(small[0].shape, F32)],
        scratch_shapes=[
            pltpu.VMEM((rows, columns), F32),
            pltpu.VMEM((rows, columns), LOW),
            pltpu.VMEM((stages, *small[0].shape), F32),
            pltpu.VMEM((stages, *small[0].shape), F32),
        ]
        + buffers
        + buffers
        + [pltpu.SemaphoreType.DMA((parts, stages))] * 4
        + [pltpu.SemaphoreType.DMA((stages,))] * 2,
        compiler_params=pltpu.CompilerParams(
            vmem_limit_bytes=VMEM_BYTES, collective_id=cid, has_side_effects=True
        ),
        cost_estimate=pl.CostEstimate(flops=10**9, bytes_accessed=20 * 2**20, transcendentals=0),
        name="reduce_everywhere",
    )(*(array for group in big for array in group), *small)


def attend_pair(query, keys, values, soft_ref, place, rows):
    lane = lax.broadcasted_iota(jnp.int32, (1, PAIR), 1)
    none = jnp.zeros_like(keys)
    mixed_blocks, inverse_blocks = [], []
    for block in range(LENGTH // rows):
        part = slice(block * rows, (block + 1) * rows)
        scaled = query[part, :] * LOW(HEAD_DIM**-0.5)
        mixed, inverses = None, []
        for head in range(2):
            mine = (lane < HEAD_DIM) if head == 0 else (lane >= HEAD_DIM)
            scores = dot(scaled, jnp.where(mine, keys, none), NT)
            top = jnp.max(scores, axis=1, keepdims=True)
            weights = jnp.exp(scores - top)
            inverse = 1.0 / jnp.sum(weights, axis=1, keepdims=True)
            weights = weights.astype(LOW)
            soft_ref[place + head, part, :] = weights
            inverses.append(jnp.broadcast_to(inverse, (rows, PAIR)))
            term = dot(weights, jnp.where(mine, values, none)) * inverse
            mixed = term if mixed is None else mixed + term
        mixed_blocks.append(mixed)
        inverse_blocks.append(jnp.where(lane < HEAD_DIM, inverses[0], inverses[1]))
    return jnp.concatenate(mixed_blocks, axis=0), jnp.concatenate(inverse_blocks, axis=0)


def forward_kernel(
    tokens_ref, gain_one_ref, wq_ref, wk_ref, wv_ref, wo_ref, gain_two_ref, route_ref, embed_ref, *refs,
    m, steps, slots, slot_cap,
):
    ids_ref, slot_ids_ref, keep_ref = refs[:3]
    q_ref, k_ref, v_ref, soft_ref, inv_ref, mixed_ref, first_ref, sent_ref, gates_ref, projected_ref, normed = refs[3:]
    step = pl.program_id(0)
    height = tokens_ref.shape[0]

    @pl.when(step == 0)
    def _():
        gain = gain_one_ref[...]

        def body(rows, _):
            values = tokens_ref[rows, :].astype(F32)
            normed[rows, :] = (normalise(values)[0] * gain).astype(LOW)
            first_ref[rows, :] = values

        by_rows(height, 256, body)

    rows = normed[...]
    q_ref[...] = dot(rows, wq_ref[...]).astype(LOW)
    k_ref[...] = dot(rows, wk_ref[...]).astype(LOW)
    v_ref[...] = dot(rows, wv_ref[...]).astype(LOW)
    for pair in range(GROUP // 2):
        lanes = slice(pair * PAIR, (pair + 1) * PAIR)
        mixed, inverse = attend_pair(q_ref[:, lanes], k_ref[:, lanes], v_ref[:, lanes], soft_ref, 2 * pair, 512)
        mixed_ref[:, lanes] = mixed.astype(LOW)
        inv_ref[:, lanes] = inverse
    first_ref[...] += dot(mixed_ref[...], wo_ref[...])

    @pl.when(step == steps - 1)
    def _():
        gain = gain_two_ref[...]

        def body(rows, _):
            normed[rows, :] = (normalise(first_ref[rows, :])[0] * gain).astype(LOW)

        by_rows(height, 256, body)
        second = normed[...]
        projected = dot(second, route_ref[...], NT)
        projected_ref[...] = projected
        route_column = to_column(ids_ref[m : m + 1, :].astype(F32)).astype(jnp.int32)
        gate = route_probs(projected, embed_ref[...], route_column)[-1]
        parts = spread_parts(gate)
        slot_row = slot_line(m, ids_ref, slot_ids_ref, keep_ref, slot_cap)
        block = 256
        for begin in range(0, slots, block):
            table = slot_rows(slot_row, begin, block)
            sent_ref[begin : begin + block, :] = dot(table, second).astype(LOW)
            gathered = jnp.sum(dot(table, parts), axis=1, keepdims=True)
            for w in range(begin // slot_cap, (begin + block) // slot_cap):
                column = gathered[w * slot_cap - begin : (w + 1) * slot_cap - begin, :]
                row = jnp.sum(jnp.where(diagonal(slot_cap), column, 0.0), axis=0, keepdims=True)
                gates_ref[w] = jnp.broadcast_to(row, (8, 128))


def forward_stage(m, tokens, gains, weights, w_route, embed, ids, slot_cap, moves, pushes, cid):
    tok_count, width = tokens.shape[1:]
    experts = embed.shape[0]
    slots = experts * slot_cap
    steps = HEADS // GROUP
    span = GROUP * HEAD_DIM
    one = pl.Buffered(1)
    fixed = lambda shape: pl.BlockSpec(shape, lambda i: (0,) * len(shape), pipeline_mode=one)
    of_m = lambda *shape: pl.BlockSpec((None, *shape), lambda i: (m, 0, 0), pipeline_mode=one)
    columns = lambda height: pl.BlockSpec((height, span), lambda i: (0, i))
    whole = lambda *shape: pl.BlockSpec(shape, lambda i: (0,) * len(shape))
    gain_one, gain_two = gains
    wq, wk, wv, wo = weights
    low = lambda *shape: jax.ShapeDtypeStruct(shape, LOW)
    full = lambda *shape: jax.ShapeDtypeStruct(shape, F32)
    return call_with_moves(
        functools.partial(forward_kernel, m=m, steps=steps, slots=slots, slot_cap=slot_cap),
        moves,
        pushes,
        cid,
        grid=(steps,),
        in_specs=[
            of_m(tok_count, width), fixed((1, width)), columns(width), columns(width), columns(width),
            pl.BlockSpec((span, width), lambda i: (i, 0)), fixed((1, width)), fixed(w_route.shape),
            fixed(embed.shape),
        ]
        + [fixed(ids[0].shape)] * 3,
        out_specs=[
            columns(tok_count), columns(tok_count), columns(tok_count),
            pl.BlockSpec((GROUP, LENGTH, LENGTH), lambda i: (i, 0, 0)),
            columns(tok_count), columns(tok_count), whole(tok_count, width), whole(slots, width),
            whole(experts, 8, 128), whole(tok_count, w_route.shape[0]),
        ],
        out_shape=[
            low(tok_count, width), low(tok_count, width), low(tok_count, width), low(HEADS, LENGTH, LENGTH),
            full(tok_count, width), low(tok_count, width), full(tok_count, width), low(slots, width),
            full(experts, 8, 128), full(tok_count, w_route.shape[0]),
        ],
        scratch_shapes=[pltpu.VMEM((tok_count, width), LOW)],
        cost=pl.CostEstimate(
            flops=30 * 10**9, bytes_accessed=50 * 2**20, transcendentals=HEADS * LENGTH * LENGTH
        ),
        name="forward_stage",
        args=(tokens, gain_one, wq, wk, wv, wo, gain_two, w_route, embed, *ids),
    )


def dispatch_kernel(ids_ref, slot_ids_ref, keep_ref, rows_ref, *out_refs, slots, slot_cap):
    for m, out_ref in enumerate(out_refs):

        @pl.when(pl.program_id(0) == m)
        def _():
            slot_row = slot_line(m, ids_ref, slot_ids_ref, keep_ref, slot_cap)
            for begin in range(0, slots, 256):
                table = slot_rows(slot_row, begin, 256)
                out_ref[begin : begin + 256, :] = dot(table, rows_ref[...]).astype(LOW)


def dispatch(ids, rows, slots, slot_cap):
    micro_count, tok_count, width = rows.shape
    return pl.pallas_call(
        functools.partial(dispatch_kernel, slots=slots, slot_cap=slot_cap),
        grid=(micro_count,),
        in_specs=[pl.BlockSpec(ids[0].shape, lambda m: (0, 0))] * 3
        + [pl.BlockSpec((None, tok_count, width), lambda m: (m, 0, 0))],
        out_specs=[pl.BlockSpec((slots, width), lambda m: (0, 0))] * micro_count,
        out_shape=[jax.ShapeDtypeStruct((slots, width), LOW)] * micro_count,
        compiler_params=pltpu.CompilerParams(vmem_limit_bytes=VMEM_BYTES),
        cost_estimate=pl.CostEstimate(flops=3 * 10**9, bytes_accessed=6 * 2**20, transcendentals=0),
        name="dispatch",
    )(*ids, rows)


def attend_pair_back(query, keys, values, grad, mixed, soft_ref, place, inverses, rows):
    lane = lax.broadcasted_iota(jnp.int32, (1, PAIR), 1)
    scale = LOW(HEAD_DIM**-0.5)
    none = jnp.zeros_like(keys)
    dk_parts, dv_parts, dq_blocks = [None, None], [None, None], []
    for block in range(LENGTH // rows):
        part = slice(block * rows, (block + 1) * rows)
        query_t = (query[part, :] * scale).T
        scaled = grad[part, :].astype(F32) * inverses[part, :]
        inner = scaled * mixed[part, :].astype(F32)
        scaled = scaled.astype(LOW)
        scaled_t = scaled.T
        grad_query = None
        for head in range(2):
            mine = (lane < HEAD_DIM) if head == 0 else (lane >= HEAD_DIM)
            own = slice(head * HEAD_DIM, (head + 1) * HEAD_DIM)
            weights = soft_ref[place + head, part, :]
            grad_soft = dot(scaled, jnp.where(mine, values, none), NT)
            centre = jnp.sum(jnp.where(mine, inner, 0.0), axis=1, keepdims=True)
            grad_scores = (weights.astype(F32) * (grad_soft - centre)).astype(LOW)
            term = dot(grad_scores, jnp.where(mine, keys, none))
            grad_query = term if grad_query is None else grad_query + term
            dk = dot(query_t[own, :], grad_scores)
            dv = dot(scaled_t[own, :], weights)
            dk_parts[head] = dk if dk_parts[head] is None else dk_parts[head] + dk
            dv_parts[head] = dv if dv_parts[head] is None else dv_parts[head] + dv
        dq_blocks.append(grad_query * HEAD_DIM**-0.5)
    return (
        jnp.concatenate(dq_blocks, axis=0),
        jnp.concatenate(dk_parts, axis=0).T,
        jnp.concatenate(dv_parts, axis=0).T,
    )


def backward_kernel(
    tokens_ref, cot_ref, gain_one_ref, wq_ref, wk_ref, wv_ref, wo_ref, gain_two_ref, route_ref, embed_ref,
    ids_ref, slot_ids_ref, keep_ref, first_ref, projected_ref, home_ref, dots_ref,
    q_ref, k_ref, v_ref, mixed_ref, soft_ref, inv_ref,
    dwq_ref, dwk_ref, dwv_ref, dwo_ref, gtok_ref, small_ref,
    grad_first, branch, normed_t, total, mixed_grad, dq_sc, dk_sc, dv_sc, soft_buf, soft_sem,
    *, m, steps, slots, slot_cap,
):
    step = pl.program_id(0)
    height, width = tokens_ref.shape
    experts, router_dim = embed_ref.shape
    pairs = GROUP // 2

    def soft_pair(pair):
        at = step * GROUP + 2 * pair
        return pltpu.make_async_copy(soft_ref.at[pl.ds(at, 2)], soft_buf.at[pair % 2], soft_sem.at[pair % 2])

    @pl.when(step == 0)
    def _():
        soft_pair(0).start()
        gain_one, gain_two = gain_one_ref[...], gain_two_ref[...]

        def ahead(rows, _):
            branch[rows, :] = (normalise(tokens_ref[rows, :].astype(F32))[0] * gain_one).astype(LOW)

        by_rows(height, 256, ahead)
        normed_t[...] = branch[...].T
        slot_row = slot_line(m, ids_ref, slot_ids_ref, keep_ref, slot_cap)
        slot_column = to_column(slot_row.astype(F32)).astype(jnp.int32)
        route_column = to_column(ids_ref[m : m + 1, :].astype(F32)).astype(jnp.int32)
        columns = [
            jnp.sum(jnp.where(diagonal(slot_cap), dots_ref[w, 0:1, :], 0.0), axis=1, keepdims=True)
            for w in range(experts)
        ]
        dots = spread_parts(jnp.concatenate(columns, axis=0))
        grads = []
        block = 256
        for begin in range(0, height, block):
            table = token_rows(slot_column[begin : begin + block, :], slots)
            grad_first[begin : begin + block, :] = dot(table, home_ref[...])
            grads.append(jnp.sum(dot(table, dots), axis=1, keepdims=True))
        grad_gate = jnp.concatenate(grads, axis=0)
        projected, embed_rows = projected_ref[...], embed_ref[...]
        unit, inverse, anchor, anchor_inverse, probs, picked, gate = route_probs(
            projected, embed_rows, route_column
        )
        grad_logits = grad_gate * gate * (jnp.where(picked, 1.0, 0.0) - probs)
        grad_unit = 3.0 * dot(grad_logits, anchor, NN, lax.Precision.HIGHEST)
        grad_anchor = 3.0 * dot(grad_logits, unit, TN, lax.Precision.HIGHEST)
        grad_projected = inverse * grad_unit - inverse**3 * projected * jnp.sum(
            projected * grad_unit, axis=-1, keepdims=True
        )
        term_embed = anchor_inverse * grad_anchor - anchor_inverse**3 * embed_rows * jnp.sum(
            embed_rows * grad_anchor, axis=-1, keepdims=True
        )
        parts = three_parts(grad_projected)
        for begin in range(0, height, block):
            some = slice(begin, begin + block)
            grad_first[some, :] += sum(dot(part[some, :], route_ref[...]) for part in parts)
        thirds = (dq_sc, dk_sc, dv_sc)
        third = width // 3

        def middle(rows, gathered):
            normed_two, inverse_two = normalise(first_ref[rows, :])
            second = (normed_two * gain_two).astype(LOW)
            for at, ref in enumerate(thirds):
                ref[rows, :] = second[:, at * third : (at + 1) * third]
            grad_second = grad_first[rows, :]
            value = cot_ref[rows, :].astype(F32) + normalise_back(grad_second * gain_two, normed_two, inverse_two)
            grad_first[rows, :] = value
            branch[rows, :] = value.astype(LOW)
            return gathered + fold_rows(grad_second * normed_two)

        gathered = by_rows(height, 256, middle, jnp.zeros((8, width), F32))
        small_ref[...] = jnp.zeros_like(small_ref)
        for at, ref in enumerate(thirds):
            small_ref[0:router_dim, at * third : (at + 1) * third] = sum(dot(part, ref[...], TN) for part in parts)
        small_ref[router_dim + 1 : router_dim + 2, 0:width] = jnp.sum(gathered, axis=0, keepdims=True)
        small_ref[0:experts, width : width + router_dim] = term_embed
        total[...] = jnp.zeros_like(total)

    rows = branch[...]
    dwo_ref[...] = dot(mixed_ref[...], rows, TN).astype(LOW)
    mixed_grad[...] = dot(rows, wo_ref[...], NT).astype(LOW)
    for pair in range(pairs):
        lanes = slice(pair * PAIR, (pair + 1) * PAIR)
        soft_pair(pair).wait()
        if pair + 1 < pairs:
            soft_pair(pair + 1).start()
        else:

            @pl.when(step + 1 < steps)
            def _():
                soft_pair(pairs).start()

        dq, dk, dv = attend_pair_back(
            q_ref[:, lanes], k_ref[:, lanes], v_ref[:, lanes], mixed_grad[:, lanes], mixed_ref[:, lanes],
            soft_buf.at[pair % 2], 0, inv_ref[:, lanes], 512,
        )
        dq_sc[:, lanes] = dq.astype(LOW)
        dk_sc[:, lanes] = dk.astype(LOW)
        dv_sc[:, lanes] = dv.astype(LOW)
    normed_rows = normed_t[...]
    for grad_ref, weight_ref, out_ref in (
        (dq_sc, wq_ref, dwq_ref), (dk_sc, wk_ref, dwk_ref), (dv_sc, wv_ref, dwv_ref)
    ):
        grad = grad_ref[...]
        out_ref[...] = dot(normed_rows, grad).astype(LOW)
        total[...] += dot(grad, weight_ref[...], NT)

    @pl.when(step == steps - 1)
    def _():
        gain_one = gain_one_ref[...]

        def behind(rows, gathered):
            normed_one, inverse_one = normalise(tokens_ref[rows, :].astype(F32))
            grad = total[rows, :]
            value = grad_first[rows, :] + normalise_back(grad * gain_one, normed_one, inverse_one)
            gtok_ref[rows, :] = value.astype(LOW)
            return gathered + fold_rows(grad * normed_one)

        gathered = by_rows(height, 256, behind, jnp.zeros((8, width), F32))
        small_ref[router_dim : router_dim + 1, 0:width] = jnp.sum(gathered, axis=0, keepdims=True)


def backward_stage(
    m, tokens, grad_out, gains, weights, w_route, embed, ids, kept, home, slot_cap, moves, pushes, cid
):
    tok_count, width = tokens.shape[1:]
    experts, router_dim = embed.shape
    slots = experts * slot_cap
    steps = HEADS // GROUP
    span = GROUP * HEAD_DIM
    one = pl.Buffered(1)
    fixed = lambda shape: pl.BlockSpec(shape, lambda i: (0,) * len(shape), pipeline_mode=one)
    of_m = lambda *shape: pl.BlockSpec((None, *shape), lambda i: (m, 0, 0), pipeline_mode=one)
    columns = lambda height: pl.BlockSpec((height, span), lambda i: (0, i))
    lines = pl.BlockSpec((span, width), lambda i: (i, 0))
    gain_one, gain_two = gains
    wq, wk, wv, wo = weights
    first, projected, q, k, v, mixed, soft, inverses = kept
    low = lambda *shape: jax.ShapeDtypeStruct(shape, LOW)
    small = (-(-max(experts, router_dim + 2) // 8) * 8, width + 128)
    return call_with_moves(
        functools.partial(backward_kernel, m=m, steps=steps, slots=slots, slot_cap=slot_cap),
        moves,
        pushes,
        cid,
        grid=(steps,),
        in_specs=[
            of_m(tok_count, width), of_m(tok_count, width), fixed((1, width)), columns(width), columns(width),
            columns(width), lines, fixed((1, width)), fixed(w_route.shape), fixed(embed.shape),
            *[fixed(ids[0].shape)] * 3, fixed(first.shape), fixed(projected.shape), fixed(home[0].shape), fixed(home[1].shape),
            columns(tok_count), columns(tok_count), columns(tok_count), columns(tok_count),
            pl.BlockSpec(memory_space=pl.ANY), columns(tok_count),
        ],
        out_specs=[
            columns(width), columns(width), columns(width), lines, fixed((tok_count, width)), fixed(small),
        ],
        out_shape=[
            low(width, width), low(width, width), low(width, width), low(width, width), low(tok_count, width),
            jax.ShapeDtypeStruct(small, F32),
        ],
        scratch_shapes=[
            pltpu.VMEM((tok_count, width), F32), pltpu.VMEM((tok_count, width), LOW),
            pltpu.VMEM((width, tok_count), LOW), pltpu.VMEM((tok_count, width), F32),
        ]
        + [pltpu.VMEM((tok_count, span), LOW)] * 4
        + [pltpu.VMEM((2, 2, LENGTH, LENGTH), LOW), pltpu.SemaphoreType.DMA((2,))],
        cost=pl.CostEstimate(flops=40 * 10**9, bytes_accessed=50 * 2**20, transcendentals=0),
        name="backward_stage",
        args=(
            tokens, grad_out, gain_one, wq, wk, wv, wo, gain_two, w_route, embed, *ids, first,
            projected, *home, q, k, v, mixed, soft, inverses,
        ),
    )


def finish_kernel(*refs, cuts, blocks, tiles, per_tile):
    ids_ref, slot_ids_ref, keep_ref, embed_ref = refs[:4]
    ins, refs = [], refs[4:]
    for pieces in cuts:
        ins.append(refs[: 3 + len(pieces)])
        refs = refs[3 + len(pieces) :]
    near_in, near_outer = refs[:2]
    far_in, far_outer = refs[2 : 2 + tiles], refs[2 + tiles : 2 + 2 * tiles]
    big_ref = refs[2 + 2 * tiles]
    out_ref, grad_ref, din_ref, douter_ref, *big_outs = refs[3 + 2 * tiles :]
    step = pl.program_id(0)
    rows, width = out_ref.shape
    for m, pieces in enumerate(cuts):
        first_ref, projected_ref, gtok_ref, *home_refs = ins[m]
        for block in range(blocks):

            @pl.when(step == m * blocks + block)
            def _():
                some = slice(block * rows, (block + 1) * rows)
                returned = None
                for (low, high), home_ref in zip(pieces, home_refs):
                    line = piece_line(m, ids_ref, slot_ids_ref, keep_ref, low, high)[:, some]
                    column = to_column(line.astype(F32)).astype(jnp.int32)
                    term = dot(token_rows(column, home_ref.shape[0]), home_ref[...])
                    returned = term if returned is None else returned + term
                route_column = to_column(ids_ref[m : m + 1, some].astype(F32)).astype(jnp.int32)
                gate = route_probs(projected_ref[...], embed_ref[...], route_column)[-1]
                out_ref[...] = (first_ref[...] + gate * returned).astype(LOW)
                grad_ref[...] = gtok_ref[...]

    for t in range(tiles):

        @pl.when((step >= t * per_tile) & (step < (t + 1) * per_tile))
        def _():
            din_ref[0] = near_in[...] + sum(far_in[t][j].astype(F32) for j in range(far_in[t].shape[0]))
            douter_ref[0] = near_outer[...] + sum(far_outer[t][j].astype(F32) for j in range(far_outer[t].shape[0]))

    for k, big_out in enumerate(big_outs):
        big_out[...] = big_ref[:, k * width : (k + 1) * width].astype(F32)


def finish(ids, embed, parts, near, far, big):
    micro_count, tok_count = ids[0].shape
    width = parts[0][0].shape[1]
    near_in, near_outer = near
    tiles = len(far) // 2
    spread, _, tile = far[0].shape
    units = near_in.shape[1]
    span = 256 if tile % 256 == 0 else 128
    wide_steps, per_tile = units // span, tile // span
    rows = 256
    blocks = tok_count // rows
    steps = micro_count * blocks
    lines = big.shape[0] // steps
    whole = lambda shape: pl.BlockSpec(shape, lambda i: (0, 0), pipeline_mode=pl.Buffered(1))
    in_specs, args = [whole(ids[0].shape)] * 3 + [whole(embed.shape)], [*ids, embed]
    for at, (first, projected, gtok, homes) in enumerate(parts):
        place = lambda i, at=at: (jnp.clip(i - at * blocks, 0, blocks - 1), 0)
        in_specs += [
            pl.BlockSpec((rows, width), place), pl.BlockSpec((rows, projected.shape[1]), place),
            pl.BlockSpec((rows, width), place), *(whole(home.shape) for _, home in homes),
        ]
        args += [first, projected, gtok, *(home for _, home in homes)]
    near_at = lambda i: jnp.minimum(i, wide_steps - 1)
    far_at = lambda i, t: jnp.clip(i - t * per_tile, 0, per_tile - 1)
    in_specs += [
        pl.BlockSpec((width, span), lambda i: (0, near_at(i))), pl.BlockSpec((span, width), lambda i: (near_at(i), 0)),
    ]
    in_specs += [pl.BlockSpec((spread, width, span), lambda i, t=t: (0, 0, far_at(i, t))) for t in range(tiles)]
    in_specs += [pl.BlockSpec((spread, span, width), lambda i, t=t: (0, far_at(i, t), 0)) for t in range(tiles)]
    in_specs += [pl.BlockSpec((lines, big.shape[1]), lambda i: (i, 0))]
    row_out = pl.BlockSpec((None, rows, width), lambda i: (i // blocks, i % blocks, 0))
    line_out = pl.BlockSpec((lines, width), lambda i: (i, 0))
    kinds = big.shape[1] // width
    return pl.pallas_call(
        functools.partial(
            finish_kernel, cuts=[[cut for cut, _ in part[3]] for part in parts], blocks=blocks, tiles=tiles,
            per_tile=per_tile,
        ),
        grid=(steps,),
        in_specs=in_specs,
        out_specs=[
            row_out, row_out, pl.BlockSpec((1, width, span), lambda i: (0, 0, near_at(i))),
            pl.BlockSpec((1, span, width), lambda i: (0, near_at(i), 0)),
        ]
        + [line_out] * kinds,
        out_shape=[jax.ShapeDtypeStruct((micro_count, tok_count, width), LOW)] * 2
        + [jax.ShapeDtypeStruct((1, *near_in.shape), F32), jax.ShapeDtypeStruct((1, *near_outer.shape), F32)]
        + [jax.ShapeDtypeStruct((big.shape[0], width), F32)] * kinds,
        compiler_params=pltpu.CompilerParams(vmem_limit_bytes=VMEM_BYTES),
        cost_estimate=pl.CostEstimate(flops=3 * 10**9, bytes_accessed=56 * 2**20, transcendentals=0),
        name="finish",
    )(*args, near_in, near_outer, *far, big)


def gelu_and_slope(values):
    ratio = 1.0 / (1.0 + jnp.abs(values) * (0.3275911 * 0.7071067811865476))
    bell = jnp.exp(values * values * -0.5)
    series = 0.5 * 1.061405429
    for factor in (-1.453152027, 1.421413741, -0.284496736, 0.254829592):
        series = series * ratio + 0.5 * factor
    tail = series * ratio * bell
    below = jnp.where(values >= 0.0, 1.0 - tail, tail)
    return values * below, below + values * bell * 0.3989422804014327


def expert_kernel(*refs, cuts, more, last, per, steps, slot_cap, landings=(), settle=None):
    rows_ref, gate_ref, own_in, own_outer = refs[:4]
    cot_refs, refs = refs[4 : 4 + len(cuts)], refs[4 + len(cuts) :]
    far_in, refs = refs[:per], refs[per:]
    given = per - len(landings)
    far_outer, refs = [*refs[:given], *landings], refs[given:]
    if more:
        old_in, old_outer = refs[:2]
        refs = refs[2:]
    result_ref, sent_ref, dots_ref, din_ref, douter_ref = refs[:5]
    refs = refs[5:]
    if last:
        far_din, far_douter = refs[:2]
        refs = refs[2:]
    grad_sc, rows_t, acc_result, acc_sent, first_buf, second_buf, sems = refs
    step = pl.program_id(0)
    slot = lax.rem(step, 2)
    sources = rows_ref.shape[0] // slot_cap
    tile = first_buf.shape[2]

    def fetch(i):
        if i < per:
            first = own_in.at[:, i * tile : (i + 1) * tile]
            second = own_outer.at[i * tile : (i + 1) * tile, :]
        else:
            first, second = far_in[i % per].at[i // per - 1], far_outer[i % per].at[i // per - 1]
        return (
            pltpu.make_async_copy(first, first_buf.at[i % 2], sems.at[0, i % 2]),
            pltpu.make_async_copy(second, second_buf.at[i % 2], sems.at[1, i % 2]),
        )

    @pl.when(step == 0)
    def _():
        for copy in fetch(0):
            copy.start()
        for w in range(sources):
            part = slice(w * slot_cap, (w + 1) * slot_cap)
            gate = jnp.sum(jnp.where(diagonal(slot_cap), gate_ref[w, 0:1, :], 0.0), axis=1, keepdims=True)
            cot = jnp.concatenate([ref[w] for ref in cot_refs], axis=0)
            grad_sc[part, :] = (cot.astype(F32) * gate).astype(LOW)
        rows_t[...] = rows_ref[...].T
        acc_result[...] = jnp.zeros_like(acc_result)
        acc_sent[...] = jnp.zeros_like(acc_sent)

    for i in range(steps):

        @pl.when(step == i)
        def _():
            for copy in fetch(i):
                copy.wait()
            if landings and i + 1 == 2 * per - 1:
                settle(0)
            if i + 1 < steps:
                for copy in fetch(i + 1):
                    copy.start()

    first, second = first_buf[slot], second_buf[slot]
    hidden, slope = gelu_and_slope(dot(rows_ref[...], first))
    hidden = hidden.astype(LOW)
    grad_rows = grad_sc[...]
    grad_pre = (dot(grad_rows, second, NT) * slope).astype(LOW)
    acc_result[...] += dot(hidden, second)
    acc_sent[...] += dot(grad_pre, first, NT)
    din = dot(rows_t[...], grad_pre)
    douter = dot(hidden, grad_rows, TN)
    if more:
        din += old_in[...]
        douter += old_outer[...]
    if not last:
        din_ref[...] = din
        douter_ref[...] = douter
    else:

        @pl.when(step < per)
        def _():
            din_ref[...] = din
            douter_ref[...] = douter

        @pl.when(step >= per)
        def _():
            far_din[...] = din.astype(LOW)
            far_douter[...] = douter.astype(LOW)

    @pl.when(step == steps - 1)
    def _():
        result = acc_result[...].astype(LOW)
        result_ref[...] = result
        sent_ref[...] = acc_sent[...].astype(LOW)
        for w in range(sources):
            part = slice(w * slot_cap, (w + 1) * slot_cap)
            cot = jnp.concatenate([ref[w] for ref in cot_refs], axis=0)
            products = cot.astype(F32) * result[part, :].astype(F32)
            column = jnp.sum(products, axis=1, keepdims=True)
            row = jnp.sum(jnp.where(diagonal(slot_cap), column, 0.0), axis=0, keepdims=True)
            dots_ref[w] = jnp.broadcast_to(row, (8, 128))


def tile_of(units):
    return min(512, units)


def expert_stage(rows, cots, gates, weights, old, last, slot_cap, moves, pushes, cid):
    own_in, own_outer, far_in, far_outer = weights
    width, units = own_in.shape
    count = lax.axis_size("narrow")
    height = rows.shape[0]
    tile = tile_of(units)
    per = units // tile
    steps = count * per
    whole = lambda shape: pl.BlockSpec(shape, lambda i: (0,) * len(shape))
    anywhere = pl.BlockSpec(memory_space=pl.ANY)
    din_spec = pl.BlockSpec((None, width, tile), lambda i: (i, 0, 0))
    douter_spec = pl.BlockSpec((None, tile, width), lambda i: (i, 0, 0))
    out_specs = [whole((height, width)), whole((height, width)), whole(gates.shape)]
    out_shape = [
        jax.ShapeDtypeStruct((height, width), LOW),
        jax.ShapeDtypeStruct((height, width), LOW),
        jax.ShapeDtypeStruct(gates.shape, F32),
    ]
    if last:
        near = lambda i: jnp.minimum(i, per - 1)
        away = lambda i: jnp.maximum(i - per, 0)
        out_specs += [
            pl.BlockSpec((width, tile), lambda i: (0, near(i))),
            pl.BlockSpec((tile, width), lambda i: (near(i), 0)),
            pl.BlockSpec((None, width, tile), lambda i: (away(i), 0, 0)),
            pl.BlockSpec((None, tile, width), lambda i: (away(i), 0, 0)),
        ]
        out_shape += [
            jax.ShapeDtypeStruct((width, units), F32),
            jax.ShapeDtypeStruct((units, width), F32),
            jax.ShapeDtypeStruct((steps - per, width, tile), LOW),
            jax.ShapeDtypeStruct((steps - per, tile, width), LOW),
        ]
    else:
        out_specs += [din_spec, douter_spec]
        out_shape += [
            jax.ShapeDtypeStruct((steps, width, tile), F32),
            jax.ShapeDtypeStruct((steps, tile, width), F32),
        ]
    return call_with_moves(
        functools.partial(
            expert_kernel, cuts=[cot.shape[1] for cot in cots], more=bool(old), last=last, per=per, steps=steps,
            slot_cap=slot_cap,
        ),
        moves,
        pushes,
        cid,
        grid=(steps,),
        in_specs=[whole((height, width)), whole(gates.shape), anywhere, anywhere]
        + [whole(cot.shape) for cot in cots]
        + [anywhere] * (len(far_in) + len(far_outer))
        + ([din_spec, douter_spec] if old else []),
        out_specs=out_specs,
        out_shape=out_shape,
        scratch_shapes=[
            pltpu.VMEM((height, width), LOW),
            pltpu.VMEM((width, height), LOW),
            pltpu.VMEM((height, width), F32),
            pltpu.VMEM((height, width), F32),
            pltpu.VMEM((2, width, tile), LOW),
            pltpu.VMEM((2, tile, width), LOW),
            pltpu.SemaphoreType.DMA((2, 2)),
        ],
        cost=pl.CostEstimate(
            flops=12 * height * width * units * count, bytes_accessed=34 * 2**20, transcendentals=0
        ),
        name="expert_stage",
        args=(rows, gates, own_in, own_outer, *cots, *far_in, *far_outer, *old),
        late=len(far_outer) < per,
    )


def local(
    tokens,
    grad_out,
    route_ids,
    slot_ids,
    keep_ids,
    gain_one,
    w_query,
    w_key,
    w_value,
    w_out,
    gain_two,
    w_route,
    embed,
    w_in,
    w_outer,
):
    micro_count, tok_count, feat_width = tokens.shape
    expert_count = embed.shape[0]
    slot_cap = max(2, tok_count // expert_count)
    slots = expert_count * slot_cap
    own_in, own_outer = w_in[0], w_outer[0]
    units = own_in.shape[1]
    tile = tile_of(units)
    per = units // tile
    weight_pushes = []
    for t in range(per):
        some = slice(t * tile, (t + 1) * tile)
        weight_pushes.append((own_in, lambda ref, j, some=some: ref.at[:, some], (feat_width, tile)))
        weight_pushes.append((own_outer, lambda ref, j, some=some: ref.at[some, :], (tile, feat_width)))
    early = 2 if per > 1 else 1
    half = slot_cap // 2
    gains = (gain_one[None], gain_two[None])
    mixers = (w_query, w_key, w_value, w_out)
    ids = (route_ids, slot_ids, keep_ids)
    router = (w_route.T, embed, ids)

    def boxes(rows):
        return rows.reshape((expert_count, slot_cap) + rows.shape[1:])

    def flat(boxed):
        return boxed.reshape((boxed.shape[0] * boxed.shape[1],) + boxed.shape[2:])

    def entire(array):
        return array, 0, array.shape[1]

    cot_boxes = [boxes(rows) for rows in dispatch(ids, grad_out, slots, slot_cap)]
    (*ahead_0, sent, gates, projected), (cot_0,), far_a = forward_stage(
        0, tokens, gains, mixers, *router, slot_cap, (entire(cot_boxes[0]),), weight_pushes[:early], 1
    )
    ahead_0.append(projected)
    (*ahead_1, next_sent, next_gates, projected), (sent_0, gates_0, cot_1), far_b = forward_stage(
        1, tokens, gains, mixers, *router, slot_cap,
        (entire(boxes(sent)), entire(gates), entire(cot_boxes[1])), weight_pushes[early:-1], 2
    )
    ahead_1.append(projected)

    far = [*far_a, *far_b]
    (result_0, grad_0, dots_0, *old), (sent_1, gates_1), far_c = expert_stage(
        flat(sent_0), (cot_0,), gates_0, (own_in, own_outer, far[0::2], far[1::2]), (), False, slot_cap,
        (entire(boxes(next_sent)), entire(next_gates)), weight_pushes[-1:], 3
    )
    far = [*far, *far_c]
    result_0 = boxes(result_0)
    (result_1, grad_1, dots_1, near_din, near_douter, far_din, far_douter), (home_grad_0, home_dots_0), _ = (
        expert_stage(
            flat(sent_1), (cot_1,), gates_1, (own_in, own_outer, far[0::2], far[1::2]), tuple(old), True,
            slot_cap, (entire(boxes(grad_0)), entire(dots_0)), (), 4
        )
    )
    grad_pushes = [
        (far_din, lambda ref, j, t=t: ref.at[j * per + t], (feat_width, tile)) for t in range(per)
    ] + [
        (far_douter, lambda ref, j, t=t: ref.at[j * per + t], (tile, feat_width)) for t in range(per)
    ]
    later = len(grad_pushes) // 2

    def kept(ahead):
        q, k, v, soft, inverses, mixed, first, projected = ahead
        return first, projected, q, k, v, mixed, soft, inverses

    (*big_0, gtok_0, small_0), (home_grad_1, home_dots_1, home_b), got_a = backward_stage(
        0, tokens, grad_out, gains, mixers, *router, kept(ahead_0), (flat(home_grad_0), home_dots_0), slot_cap,
        (entire(boxes(grad_1)), entire(dots_1), (result_0, half, slot_cap)), grad_pushes[:later], 5
    )
    (*big_1, gtok_1, small_1), (home_1, home_c), got_b = backward_stage(
        1, tokens, grad_out, gains, mixers, *router, kept(ahead_1), (flat(home_grad_1), home_dots_1), slot_cap,
        (entire(boxes(result_1)), (result_0, 0, half)), grad_pushes[later:], 6
    )
    homes_0 = [((half, slot_cap), flat(home_b)), ((0, half), flat(home_c))]
    big, small = reduce_everywhere(list(zip(big_0, big_1)), (small_0, small_1), 7)
    block_out, grad_tokens, grad_in, grad_outer, *big = finish(
        ids, embed,
        (
            (ahead_0[6], ahead_0[7], gtok_0, homes_0),
            (ahead_1[6], ahead_1[7], gtok_1, [((0, slot_cap), flat(home_1))]),
        ),
        (near_din, near_douter), [*got_a, *got_b], big,
    )
    router_dim = w_route.shape[1]
    return (
        block_out,
        grad_tokens,
        small[router_dim, :feat_width],
        *big,
        small[router_dim + 1, :feat_width],
        small[:router_dim, :feat_width].T,
        small[:expert_count, feat_width : feat_width + router_dim],
        grad_in,
        grad_outer,
    )


def solution(mesh):
    tokens_spec = P(None, ("wide", "narrow"), None)
    ids_spec = P(None, ("wide", "narrow"))
    in_spec, outer_spec = P("wide", None, "narrow"), P("wide", "narrow", None)
    return jax.shard_map(
        local,
        mesh=mesh,
        in_specs=(tokens_spec,) * 2 + (ids_spec,) * 3 + (P(),) * 8 + (in_spec, outer_spec),
        out_specs=(tokens_spec,) * 2 + (P(),) * 8 + (in_spec, outer_spec),
        check_vma=False,
    )
```

```python
import functools

import jax
import jax.numpy as jnp
from jax import lax
from jax.experimental import pallas as pl
from jax.experimental.pallas import tpu as pltpu
from jax.sharding import PartitionSpec as P

D = 768
HEADS = 12
HEAD_DIM = 64
LENGTH = 1024
PAIR = 2 * HEAD_DIM
GROUP = 4
PIECES = 4
NN = (((1,), (0,)), ((), ()))
NT = (((1,), (1,)), ((), ()))
TN = (((0,), (0,)), ((), ()))
LOW = jnp.bfloat16
F32 = jnp.float32
VMEM_BYTES = 60 << 20


def dot(left, right, dims=NN, precise=None):
    return lax.dot_general(left, right, dims, precision=precise, preferred_element_type=F32)


def normalise(values):
    centred = values - jnp.mean(values, axis=-1, keepdims=True)
    inverse = lax.rsqrt(jnp.mean(centred * centred, axis=-1, keepdims=True) + 1e-05)
    return centred * inverse, inverse


def normalise_back(grad, normed, inverse):
    return inverse * (
        grad
        - jnp.mean(grad, axis=-1, keepdims=True)
        - normed * jnp.mean(grad * normed, axis=-1, keepdims=True)
    )


def by_rows(count, size, body, carry=None):
    return lax.fori_loop(
        0, count // size, lambda i, c: body(pl.ds(pl.multiple_of(i * size, size), size), c), carry
    )


def fold_rows(values):
    return jnp.sum(values.reshape(values.shape[0] // 8, 8, values.shape[1]), axis=0)


def three_parts(values):
    high = values.astype(LOW)
    rest = values - high.astype(F32)
    middle = rest.astype(LOW)
    return high, middle, (rest - middle.astype(F32)).astype(LOW)


def spread_parts(column):
    lane = lax.broadcasted_iota(jnp.int32, (1, 128), 1)
    high, middle, low = (part.astype(F32) for part in three_parts(column))
    return jnp.where(lane == 0, high, jnp.where(lane == 1, middle, jnp.where(lane == 2, low, 0.0))).astype(LOW)


def diagonal(rows):
    shape = (rows, 128)
    return lax.broadcasted_iota(jnp.int32, shape, 0) == lax.broadcasted_iota(jnp.int32, shape, 1)


def to_column(row):
    pieces = [
        jnp.sum(jnp.where(diagonal(128), row[:, first : first + 128], 0.0), axis=1, keepdims=True)
        for first in range(0, row.shape[1], 128)
    ]
    return jnp.concatenate(pieces, axis=0)


def unit_length(rows):
    inverse = lax.rsqrt(jnp.sum(rows * rows, axis=-1, keepdims=True) + 1.0)
    return rows * inverse, inverse


def route_probs(projected, embed_rows, route_column):
    unit, inverse = unit_length(projected)
    anchor, anchor_inverse = unit_length(embed_rows)
    logits = 3.0 * dot(unit, anchor, NT, lax.Precision.HIGHEST)
    weights = jnp.exp(logits - jnp.max(logits, axis=-1, keepdims=True))
    probs = weights / jnp.sum(weights, axis=-1, keepdims=True)
    lane = lax.broadcasted_iota(jnp.int32, (1, probs.shape[1]), 1)
    picked = route_column == lane
    gate = jnp.sum(jnp.where(picked, probs, 0.0), axis=-1, keepdims=True)
    return unit, inverse, anchor, anchor_inverse, probs, picked, gate


def slot_line(m, route_ref, slot_ref, keep_ref, slot_cap):
    line = slice(m, m + 1)
    return jnp.where(keep_ref[line, :] > 0, route_ref[line, :] * slot_cap + slot_ref[line, :], -1)


def piece_line(m, route_ref, slot_ref, keep_ref, low, high):
    line = slice(m, m + 1)
    slot = slot_ref[line, :]
    inside = (keep_ref[line, :] > 0) & (slot >= low) & (slot < high)
    return jnp.where(inside, route_ref[line, :] * (high - low) + slot - low, -1)


def slot_rows(slot_row, first, count):
    slot = lax.broadcasted_iota(jnp.int32, (count, slot_row.shape[1]), 0) + first
    return jnp.where(slot == slot_row, 1.0, 0.0).astype(LOW)


def token_rows(slot_column, slots):
    lane = lax.broadcasted_iota(jnp.int32, (slot_column.shape[0], slots), 1)
    return jnp.where(lane == slot_column, 1.0, 0.0).astype(LOW)


MESH = pl.DeviceIdType.MESH


def call_with_moves(
    body, moves, pushes, cid, *, grid, in_specs, out_specs, out_shape, scratch_shapes=(), cost, name, args, late=False
):
    members, spread = lax.axis_size("wide"), lax.axis_size("narrow")
    n_in, n_out, n_moves, n_scratch = len(in_specs), len(out_specs), len(moves), len(scratch_shapes)
    arrays = []
    for array, _, _ in pushes:
        if not any(array is known for known in arrays):
            arrays.append(array)
    which = [next(k for k, known in enumerate(arrays) if known is array) for array, _, _ in pushes]
    n_arrays, n_pushes = len(arrays), len(pushes)

    def kernel(*refs):
        ins, refs = refs[:n_in], refs[n_in:]
        sources, refs = refs[:n_moves], refs[n_moves:]
        pushed, refs = refs[:n_arrays], refs[n_arrays:]
        outs, refs = refs[:n_out], refs[n_out:]
        targets, refs = refs[:n_moves], refs[n_moves:]
        landings, refs = refs[:n_pushes], refs[n_pushes:]
        scratch, refs = refs[:n_scratch], refs[n_scratch:]
        stages, refs = refs[:n_moves], refs[n_moves:]
        send_sem, recv_sem, own_sem, push_send, push_recv = refs
        me, side = lax.axis_index("wide"), lax.axis_index("narrow")
        step = pl.program_id(0)

        def piece(i, w):
            return sources[i].at[w, moves[i][1] : moves[i][2]]

        def remote(i, d):
            peer = lax.rem(me + d, members)
            return pltpu.make_async_remote_copy(
                src_ref=piece(i, peer),
                dst_ref=targets[i].at[me],
                send_sem=send_sem.at[i, d],
                recv_sem=recv_sem.at[i, d],
                device_id={"wide": peer},
                device_id_type=MESH,
            )

        def push(k, j, part):
            size = pushes[k][2][0] // PIECES
            some = slice(part * size, (part + 1) * size)
            return pltpu.make_async_remote_copy(
                src_ref=pushes[k][1](pushed[which[k]], j).at[some],
                dst_ref=landings[k].at[j].at[some],
                send_sem=push_send.at[k, j * PIECES + part],
                recv_sem=push_recv.at[k, j * PIECES + part],
                device_id={"narrow": lax.rem(side + j + 1, spread)},
                device_id_type=MESH,
            )

        def settle(k):
            for j in range(spread - 1):
                for part in range(PIECES):
                    push(k, j, part).wait()

        @pl.when(step == 0)
        def _():
            barrier = pltpu.get_barrier_semaphore()
            count = 0
            if n_moves:
                for d in range(1, members):
                    pl.semaphore_signal(
                        barrier, inc=1, device_id={"wide": lax.rem(me + d, members)}, device_id_type=MESH
                    )
                count += members - 1
            if n_pushes:
                for j in range(spread - 1):
                    pl.semaphore_signal(
                        barrier, inc=1, device_id={"narrow": lax.rem(side + j + 1, spread)}, device_id_type=MESH
                    )
                count += spread - 1
            pl.semaphore_wait(barrier, count)
            for i in range(n_moves):
                for d in range(1, members):
                    remote(i, d).start()
                pltpu.make_async_copy(piece(i, me), stages[i], own_sem.at[i]).start()
            for k in range(n_pushes):
                for j in range(spread - 1):
                    for part in range(PIECES):
                        push(k, j, part).start()

        if late:
            body(*ins, *outs, *scratch, landings=landings, settle=settle)
        else:
            body(*ins, *outs, *scratch)

        @pl.when(step == grid[0] - 1)
        def _():
            for i in range(n_moves):
                pltpu.make_async_copy(piece(i, me), stages[i], own_sem.at[i]).wait()
                pltpu.make_async_copy(stages[i], targets[i].at[me], own_sem.at[i]).start()
            for i in range(n_moves):
                pltpu.make_async_copy(stages[i], targets[i].at[me], own_sem.at[i]).wait()
                for d in range(1, members):
                    remote(i, d).wait()
            if not late:
                for k in range(n_pushes):
                    settle(k)

    anywhere = pl.BlockSpec(memory_space=pl.ANY)
    results = pl.pallas_call(
        kernel,
        grid=grid,
        in_specs=list(in_specs) + [anywhere] * (n_moves + n_arrays),
        out_specs=list(out_specs) + [anywhere] * (n_moves + n_pushes),
        out_shape=list(out_shape)
        + [jax.ShapeDtypeStruct((a.shape[0], high - low, *a.shape[2:]), a.dtype) for a, low, high in moves]
        + [jax.ShapeDtypeStruct((spread - 1, *shape), a.dtype) for a, _, shape in pushes],
        scratch_shapes=list(scratch_shapes)
        + [pltpu.VMEM((high - low, *a.shape[2:]), a.dtype) for a, low, high in moves]
        + [
            pltpu.SemaphoreType.DMA((max(1, n_moves), members)),
            pltpu.SemaphoreType.DMA((max(1, n_moves), members)),
            pltpu.SemaphoreType.DMA((max(1, n_moves),)),
            pltpu.SemaphoreType.DMA((max(1, n_pushes), spread * PIECES)),
            pltpu.SemaphoreType.DMA((max(1, n_pushes), spread * PIECES)),
        ],
        compiler_params=pltpu.CompilerParams(
            vmem_limit_bytes=VMEM_BYTES, collective_id=cid, has_side_effects=True
        ),
        cost_estimate=cost,
        name=name,
    )(*args, *(move[0] for move in moves), *arrays)
    return results[:n_out], results[n_out : n_out + n_moves], results[n_out + n_moves :]


def reduce_orders(wide_count, narrow_count):
    bits = lambda axis, count: [(axis, 1 << k) for k in range(count.bit_length() - 1)]
    wide, narrow = bits("wide", wide_count), bits("narrow", narrow_count)
    core, x_bits, z_bits = wide[:1], wide[1:2], wide[2:]
    return (
        core + x_bits + narrow + z_bits,
        core + narrow + x_bits + z_bits,
        core + z_bits + x_bits + narrow,
    ) * 2


def halvings(order, rows, columns):
    plan = []
    for _ in order:
        if columns % 256 == 0:
            columns //= 2
            plan.append("columns")
        elif rows % 32 == 0:
            rows //= 2
            plan.append("rows")
        else:
            plan.append("whole")
    return plan


def reduce_kernel(*refs, orders, width, places, sets):
    ins = [refs[k * sets : (k + 1) * sets] for k in range(len(places))]
    refs = refs[len(places) * sets :]
    smalls, refs = refs[:sets], refs[sets:]
    out_ref, small_out, total, result, small_send, small_recv = refs[:6]
    refs = refs[6:]
    parts, stages = len(orders), len(orders[0])
    outgoing = [refs[p * stages : (p + 1) * stages] for p in range(parts)]
    incoming = [refs[(parts + p) * stages : (parts + p + 1) * stages] for p in range(parts)]
    send_sem, recv_sem, back_send, back_recv, small_sems, small_rsems = refs[2 * parts * stages :]
    index = {axis: lax.axis_index(axis) for axis in ("wide", "narrow")}
    rows = total.shape[0]

    def own_bit(axis, bit):
        return lax.rem(index[axis] // bit, 2)

    def partner(axis, bit):
        return {axis: index[axis] + bit - 2 * bit * own_bit(axis, bit)}

    barrier = pltpu.get_barrier_semaphore()
    for axis, bit in orders[0]:
        pl.semaphore_signal(barrier, inc=1, device_id=partner(axis, bit), device_id_type=MESH)
    pl.semaphore_wait(barrier, stages)

    for group, place in zip(ins, places):
        total[:, place : place + group[0].shape[1]] = sum(ref[...].astype(F32) for ref in group)
    small_send[0] = sum(ref[...] for ref in smalls)

    regions = [[(0, rows, p * width, width)] for p in range(parts)]

    def take(region):
        row, height, column, span = region
        if not isinstance(row, int):
            row = pl.multiple_of(row, 16)
        if not isinstance(column, int):
            column = pl.multiple_of(column, 128)
        return pl.ds(row, height), pl.ds(column, span)

    def half(region, how, pick):
        row, height, column, span = region
        if how == "columns":
            return row, height, column + pick * (span // 2), span // 2
        if how == "rows":
            return row + pick * (height // 2), height // 2, column, span
        return region

    plans = [halvings(order, rows, width) for order in orders]

    def there(p, s):
        axis, bit = orders[p][s]
        return pltpu.make_async_remote_copy(
            src_ref=outgoing[p][s],
            dst_ref=incoming[p][s],
            send_sem=send_sem.at[p, s],
            recv_sem=recv_sem.at[p, s],
            device_id=partner(axis, bit),
            device_id_type=MESH,
        )

    def small_there(s):
        axis, bit = orders[0][s]
        return pltpu.make_async_remote_copy(
            src_ref=small_send.at[s],
            dst_ref=small_recv.at[s],
            send_sem=small_sems.at[s],
            recv_sem=small_rsems.at[s],
            device_id=partner(axis, bit),
            device_id_type=MESH,
        )

    def launch(p, s):
        axis, bit = orders[p][s]
        mine = own_bit(axis, bit)
        region, how = regions[p][-1], plans[p][s]
        outgoing[p][s][...] = total[take(half(region, how, 1 - mine))].astype(LOW)
        there(p, s).start()
        regions[p].append(half(region, how, mine))

    for p in range(parts):
        launch(p, 0)
    small_there(0).start()
    for s in range(stages):
        for p in range(parts):
            there(p, s).wait()
            kept = take(regions[p][-1])
            base = outgoing[p][s][...].astype(F32) if plans[p][s] == "whole" else total[kept]
            value = base + incoming[p][s][...].astype(F32)
            if s + 1 < stages:
                total[kept] = value
                launch(p, s + 1)
            else:
                result[kept] = value.astype(LOW)
        small_there(s).wait()
        fresh = small_send[s] + small_recv[s]
        if s + 1 < stages:
            small_send[s + 1] = fresh
            small_there(s + 1).start()
        else:
            small_out[...] = fresh

    def back(p, s):
        axis, bit = orders[p][s]
        spot = take(regions[p][s + 1])
        return pltpu.make_async_remote_copy(
            src_ref=result.at[spot],
            dst_ref=result.at[spot],
            send_sem=back_send.at[p, s],
            recv_sem=back_recv.at[p, s],
            device_id=partner(axis, bit),
            device_id_type=MESH,
        )

    for s in reversed(range(stages)):
        for p in range(parts):
            if plans[p][s] != "whole":
                back(p, s).start()
        for p in range(parts):
            if plans[p][s] != "whole":
                back(p, s).wait()
    out_ref[...] = result[...]


def reduce_everywhere(big, small, cid):
    orders = reduce_orders(lax.axis_size("wide"), lax.axis_size("narrow"))
    places, columns = [], 0
    for group in big:
        places.append(columns)
        columns += group[0].shape[1]
    rows = big[0][0].shape[0]
    sets = len(small)
    width, parts, stages = columns // len(orders), len(orders), len(orders[0])
    buffers = []
    for order in orders:
        height, span = rows, width
        for how in halvings(order, rows, width):
            height, span = (height // 2 if how == "rows" else height), (span // 2 if how == "columns" else span)
            buffers.append(pltpu.VMEM((height, span), LOW))
    vmem = pl.BlockSpec(memory_space=pltpu.VMEM)
    return pl.pallas_call(
        functools.partial(reduce_kernel, orders=orders, width=width, places=places, sets=sets),
        in_specs=[vmem] * ((len(big) + 1) * sets),
        out_specs=[vmem, vmem],
        out_shape=[jax.ShapeDtypeStruct((rows, columns), LOW), jax.ShapeDtypeStruct(small[0].shape, F32)],
        scratch_shapes=[
            pltpu.VMEM((rows, columns), F32),
            pltpu.VMEM((rows, columns), LOW),
            pltpu.VMEM((stages, *small[0].shape), F32),
            pltpu.VMEM((stages, *small[0].shape), F32),
        ]
        + buffers
        + buffers
        + [pltpu.SemaphoreType.DMA((parts, stages))] * 4
        + [pltpu.SemaphoreType.DMA((stages,))] * 2,
        compiler_params=pltpu.CompilerParams(
            vmem_limit_bytes=VMEM_BYTES, collective_id=cid, has_side_effects=True
        ),
        cost_estimate=pl.CostEstimate(flops=10**9, bytes_accessed=20 * 2**20, transcendentals=0),
        name="reduce_everywhere",
    )(*(array for group in big for array in group), *small)


def attend_pair(query, keys, values, soft_ref, place, rows):
    lane = lax.broadcasted_iota(jnp.int32, (1, PAIR), 1)
    none = jnp.zeros_like(keys)
    mixed_blocks, inverse_blocks = [], []
    for block in range(LENGTH // rows):
        part = slice(block * rows, (block + 1) * rows)
        scaled = query[part, :] * LOW(HEAD_DIM**-0.5)
        mixed, inverses = None, []
        for head in range(2):
            mine = (lane < HEAD_DIM) if head == 0 else (lane >= HEAD_DIM)
            scores = dot(scaled, jnp.where(mine, keys, none), NT)
            top = jnp.max(scores, axis=1, keepdims=True)
            weights = jnp.exp(scores - top)
            inverse = 1.0 / jnp.sum(weights, axis=1, keepdims=True)
            weights = weights.astype(LOW)
            soft_ref[place + head, part, :] = weights
            inverses.append(jnp.broadcast_to(inverse, (rows, PAIR)))
            term = dot(weights, jnp.where(mine, values, none)) * inverse
            mixed = term if mixed is None else mixed + term
        mixed_blocks.append(mixed)
        inverse_blocks.append(jnp.where(lane < HEAD_DIM, inverses[0], inverses[1]))
    return jnp.concatenate(mixed_blocks, axis=0), jnp.concatenate(inverse_blocks, axis=0)


def forward_kernel(
    tokens_ref, gain_one_ref, wq_ref, wk_ref, wv_ref, wo_ref, gain_two_ref, route_ref, embed_ref, *refs,
    m, steps, slots, slot_cap,
):
    ids_ref, slot_ids_ref, keep_ref = refs[:3]
    q_ref, k_ref, v_ref, soft_ref, inv_ref, mixed_ref, first_ref, sent_ref, gates_ref, projected_ref, normed = refs[3:]
    step = pl.program_id(0)
    height = tokens_ref.shape[0]

    @pl.when(step == 0)
    def _():
        gain = gain_one_ref[...][None, :]

        def body(rows, _):
            values = tokens_ref[rows, :].astype(F32)
            normed[rows, :] = (normalise(values)[0] * gain).astype(LOW)
            first_ref[rows, :] = values

        by_rows(height, 256, body)

    rows = normed[...]
    q_ref[...] = dot(rows, wq_ref[...]).astype(LOW)
    k_ref[...] = dot(rows, wk_ref[...]).astype(LOW)
    v_ref[...] = dot(rows, wv_ref[...]).astype(LOW)
    for pair in range(GROUP // 2):
        lanes = slice(pair * PAIR, (pair + 1) * PAIR)
        mixed, inverse = attend_pair(q_ref[:, lanes], k_ref[:, lanes], v_ref[:, lanes], soft_ref, 2 * pair, 512)
        mixed_ref[:, lanes] = mixed.astype(LOW)
        inv_ref[:, lanes] = inverse
    first_ref[...] += dot(mixed_ref[...], wo_ref[...])

    @pl.when(step == steps - 1)
    def _():
        gain = gain_two_ref[...][None, :]

        def body(rows, _):
            normed[rows, :] = (normalise(first_ref[rows, :])[0] * gain).astype(LOW)

        by_rows(height, 256, body)
        second = normed[...]
        projected = dot(second, route_ref[...], NT)
        projected_ref[...] = projected
        route_column = to_column(ids_ref[m : m + 1, :].astype(F32)).astype(jnp.int32)
        gate = route_probs(projected, embed_ref[...], route_column)[-1]
        parts = spread_parts(gate)
        slot_row = slot_line(m, ids_ref, slot_ids_ref, keep_ref, slot_cap)
        block = 256
        for begin in range(0, slots, block):
            table = slot_rows(slot_row, begin, block)
            sent_ref[begin : begin + block, :] = dot(table, second).astype(LOW)
            gathered = jnp.sum(dot(table, parts), axis=1, keepdims=True)
            for w in range(begin // slot_cap, (begin + block) // slot_cap):
                column = gathered[w * slot_cap - begin : (w + 1) * slot_cap - begin, :]
                row = jnp.sum(jnp.where(diagonal(slot_cap), column, 0.0), axis=0, keepdims=True)
                gates_ref[w] = jnp.broadcast_to(row, (8, 128))


def forward_stage(m, tokens, gains, weights, w_route, embed, ids, slot_cap, moves, pushes, cid):
    tok_count, width = tokens.shape[1:]
    experts = embed.shape[0]
    slots = experts * slot_cap
    steps = HEADS // GROUP
    span = GROUP * HEAD_DIM
    one = pl.Buffered(1)
    fixed = lambda shape: pl.BlockSpec(shape, lambda i: (0,) * len(shape), pipeline_mode=one)
    of_m = lambda *shape: pl.BlockSpec((None, *shape), lambda i: (m, 0, 0), pipeline_mode=one)
    columns = lambda height: pl.BlockSpec((height, span), lambda i: (0, i))
    whole = lambda *shape: pl.BlockSpec(shape, lambda i: (0,) * len(shape))
    gain_one, gain_two = gains
    wq, wk, wv, wo = weights
    low = lambda *shape: jax.ShapeDtypeStruct(shape, LOW)
    full = lambda *shape: jax.ShapeDtypeStruct(shape, F32)
    return call_with_moves(
        functools.partial(forward_kernel, m=m, steps=steps, slots=slots, slot_cap=slot_cap),
        moves,
        pushes,
        cid,
        grid=(steps,),
        in_specs=[
            of_m(tok_count, width), fixed((width,)), columns(width), columns(width), columns(width),
            pl.BlockSpec((span, width), lambda i: (i, 0)), fixed((width,)), fixed(w_route.shape),
            fixed(embed.shape),
        ]
        + [fixed(ids[0].shape)] * 3,
        out_specs=[
            columns(tok_count), columns(tok_count), columns(tok_count),
            pl.BlockSpec((GROUP, LENGTH, LENGTH), lambda i: (i, 0, 0)),
            columns(tok_count), columns(tok_count), whole(tok_count, width), whole(slots, width),
            whole(experts, 8, 128), whole(tok_count, w_route.shape[0]),
        ],
        out_shape=[
            low(tok_count, width), low(tok_count, width), low(tok_count, width), low(HEADS, LENGTH, LENGTH),
            full(tok_count, width), low(tok_count, width), full(tok_count, width), low(slots, width),
            full(experts, 8, 128), full(tok_count, w_route.shape[0]),
        ],
        scratch_shapes=[pltpu.VMEM((tok_count, width), LOW)],
        cost=pl.CostEstimate(
            flops=30 * 10**9, bytes_accessed=50 * 2**20, transcendentals=HEADS * LENGTH * LENGTH
        ),
        name="forward_stage",
        args=(tokens, gain_one, wq, wk, wv, wo, gain_two, w_route, embed, *ids),
    )


def dispatch_kernel(ids_ref, slot_ids_ref, keep_ref, rows_ref, *out_refs, slots, slot_cap):
    for m, out_ref in enumerate(out_refs):

        @pl.when(pl.program_id(0) == m)
        def _():
            slot_row = slot_line(m, ids_ref, slot_ids_ref, keep_ref, slot_cap)
            for begin in range(0, slots, 256):
                table = slot_rows(slot_row, begin, 256)
                out_ref[begin : begin + 256, :] = dot(table, rows_ref[...]).astype(LOW)


def dispatch(ids, rows, slots, slot_cap):
    micro_count, tok_count, width = rows.shape
    return pl.pallas_call(
        functools.partial(dispatch_kernel, slots=slots, slot_cap=slot_cap),
        grid=(micro_count,),
        in_specs=[pl.BlockSpec(ids[0].shape, lambda m: (0, 0))] * 3
        + [pl.BlockSpec((None, tok_count, width), lambda m: (m, 0, 0))],
        out_specs=[pl.BlockSpec((slots, width), lambda m: (0, 0))] * micro_count,
        out_shape=[jax.ShapeDtypeStruct((slots, width), LOW)] * micro_count,
        compiler_params=pltpu.CompilerParams(vmem_limit_bytes=VMEM_BYTES),
        cost_estimate=pl.CostEstimate(flops=3 * 10**9, bytes_accessed=6 * 2**20, transcendentals=0),
        name="dispatch",
    )(*ids, rows)


def attend_pair_back(query, keys, values, grad, mixed, soft_ref, place, inverses, rows):
    lane = lax.broadcasted_iota(jnp.int32, (1, PAIR), 1)
    scale = LOW(HEAD_DIM**-0.5)
    none = jnp.zeros_like(keys)
    dk_parts, dv_parts, dq_blocks = [None, None], [None, None], []
    for block in range(LENGTH // rows):
        part = slice(block * rows, (block + 1) * rows)
        query_t = (query[part, :] * scale).T
        scaled = grad[part, :].astype(F32) * inverses[part, :]
        inner = scaled * mixed[part, :].astype(F32)
        scaled = scaled.astype(LOW)
        scaled_t = scaled.T
        grad_query = None
        for head in range(2):
            mine = (lane < HEAD_DIM) if head == 0 else (lane >= HEAD_DIM)
            own = slice(head * HEAD_DIM, (head + 1) * HEAD_DIM)
            weights = soft_ref[place + head, part, :]
            grad_soft = dot(scaled, jnp.where(mine, values, none), NT)
            centre = jnp.sum(jnp.where(mine, inner, 0.0), axis=1, keepdims=True)
            grad_scores = (weights.astype(F32) * (grad_soft - centre)).astype(LOW)
            term = dot(grad_scores, jnp.where(mine, keys, none))
            grad_query = term if grad_query is None else grad_query + term
            dk = dot(query_t[own, :], grad_scores)
            dv = dot(scaled_t[own, :], weights)
            dk_parts[head] = dk if dk_parts[head] is None else dk_parts[head] + dk
            dv_parts[head] = dv if dv_parts[head] is None else dv_parts[head] + dv
        dq_blocks.append(grad_query * HEAD_DIM**-0.5)
    return (
        jnp.concatenate(dq_blocks, axis=0),
        jnp.concatenate(dk_parts, axis=0).T,
        jnp.concatenate(dv_parts, axis=0).T,
    )


def backward_kernel(
    tokens_ref, cot_ref, gain_one_ref, wq_ref, wk_ref, wv_ref, wo_ref, gain_two_ref, route_ref, embed_ref,
    ids_ref, slot_ids_ref, keep_ref, first_ref, projected_ref, home_ref, dots_ref,
    q_ref, k_ref, v_ref, mixed_ref, soft_ref, inv_ref,
    dwq_ref, dwk_ref, dwv_ref, dwo_ref, gtok_ref, small_ref,
    grad_first, branch, normed_t, total, mixed_grad, dq_sc, dk_sc, dv_sc, soft_buf, soft_sem,
    *, m, steps, slots, slot_cap,
):
    step = pl.program_id(0)
    height, width = tokens_ref.shape
    experts, router_dim = embed_ref.shape
    pairs = GROUP // 2

    def soft_pair(pair):
        at = step * GROUP + 2 * pair
        return pltpu.make_async_copy(soft_ref.at[pl.ds(at, 2)], soft_buf.at[pair % 2], soft_sem.at[pair % 2])

    @pl.when(step == 0)
    def _():
        soft_pair(0).start()
        gain_one, gain_two = gain_one_ref[...][None, :], gain_two_ref[...][None, :]

        def ahead(rows, _):
            branch[rows, :] = (normalise(tokens_ref[rows, :].astype(F32))[0] * gain_one).astype(LOW)

        by_rows(height, 256, ahead)
        normed_t[...] = branch[...].T
        slot_row = slot_line(m, ids_ref, slot_ids_ref, keep_ref, slot_cap)
        slot_column = to_column(slot_row.astype(F32)).astype(jnp.int32)
        route_column = to_column(ids_ref[m : m + 1, :].astype(F32)).astype(jnp.int32)
        columns = [
            jnp.sum(jnp.where(diagonal(slot_cap), dots_ref[w, 0:1, :], 0.0), axis=1, keepdims=True)
            for w in range(experts)
        ]
        dots = spread_parts(jnp.concatenate(columns, axis=0))
        grads = []
        block = 256
        for begin in range(0, height, block):
            table = token_rows(slot_column[begin : begin + block, :], slots)
            grad_first[begin : begin + block, :] = dot(table, home_ref[...])
            grads.append(jnp.sum(dot(table, dots), axis=1, keepdims=True))
        grad_gate = jnp.concatenate(grads, axis=0)
        projected, embed_rows = projected_ref[...], embed_ref[...]
        unit, inverse, anchor, anchor_inverse, probs, picked, gate = route_probs(
            projected, embed_rows, route_column
        )
        grad_logits = grad_gate * gate * (jnp.where(picked, 1.0, 0.0) - probs)
        grad_unit = 3.0 * dot(grad_logits, anchor, NN, lax.Precision.HIGHEST)
        grad_anchor = 3.0 * dot(grad_logits, unit, TN, lax.Precision.HIGHEST)
        grad_projected = inverse * grad_unit - inverse**3 * projected * jnp.sum(
            projected * grad_unit, axis=-1, keepdims=True
        )
        term_embed = anchor_inverse * grad_anchor - anchor_inverse**3 * embed_rows * jnp.sum(
            embed_rows * grad_anchor, axis=-1, keepdims=True
        )
        parts = three_parts(grad_projected)
        for begin in range(0, height, block):
            some = slice(begin, begin + block)
            grad_first[some, :] += sum(dot(part[some, :], route_ref[...]) for part in parts)
        thirds = (dq_sc, dk_sc, dv_sc)
        third = width // 3

        def middle(rows, gathered):
            normed_two, inverse_two = normalise(first_ref[rows, :])
            second = (normed_two * gain_two).astype(LOW)
            for at, ref in enumerate(thirds):
                ref[rows, :] = second[:, at * third : (at + 1) * third]
            grad_second = grad_first[rows, :]
            value = cot_ref[rows, :].astype(F32) + normalise_back(grad_second * gain_two, normed_two, inverse_two)
            grad_first[rows, :] = value
            branch[rows, :] = value.astype(LOW)
            return gathered + fold_rows(grad_second * normed_two)

        gathered = by_rows(height, 256, middle, jnp.zeros((8, width), F32))
        small_ref[...] = jnp.zeros_like(small_ref)
        for at, ref in enumerate(thirds):
            small_ref[0:router_dim, at * third : (at + 1) * third] = sum(dot(part, ref[...], TN) for part in parts)
        small_ref[router_dim + 1 : router_dim + 2, 0:width] = jnp.sum(gathered, axis=0, keepdims=True)
        small_ref[0:experts, width : width + router_dim] = term_embed
        total[...] = jnp.zeros_like(total)

    rows = branch[...]
    dwo_ref[...] = dot(mixed_ref[...], rows, TN).astype(LOW)
    mixed_grad[...] = dot(rows, wo_ref[...], NT).astype(LOW)
    for pair in range(pairs):
        lanes = slice(pair * PAIR, (pair + 1) * PAIR)
        soft_pair(pair).wait()
        if pair + 1 < pairs:
            soft_pair(pair + 1).start()
        else:

            @pl.when(step + 1 < steps)
            def _():
                soft_pair(pairs).start()

        dq, dk, dv = attend_pair_back(
            q_ref[:, lanes], k_ref[:, lanes], v_ref[:, lanes], mixed_grad[:, lanes], mixed_ref[:, lanes],
            soft_buf.at[pair % 2], 0, inv_ref[:, lanes], 512,
        )
        dq_sc[:, lanes] = dq.astype(LOW)
        dk_sc[:, lanes] = dk.astype(LOW)
        dv_sc[:, lanes] = dv.astype(LOW)
    normed_rows = normed_t[...]
    for grad_ref, weight_ref, out_ref in (
        (dq_sc, wq_ref, dwq_ref), (dk_sc, wk_ref, dwk_ref), (dv_sc, wv_ref, dwv_ref)
    ):
        grad = grad_ref[...]
        out_ref[...] = dot(normed_rows, grad).astype(LOW)
        total[...] += dot(grad, weight_ref[...], NT)

    @pl.when(step == steps - 1)
    def _():
        gain_one = gain_one_ref[...][None, :]

        def behind(rows, gathered):
            normed_one, inverse_one = normalise(tokens_ref[rows, :].astype(F32))
            grad = total[rows, :]
            value = grad_first[rows, :] + normalise_back(grad * gain_one, normed_one, inverse_one)
            gtok_ref[rows, :] = value.astype(LOW)
            return gathered + fold_rows(grad * normed_one)

        gathered = by_rows(height, 256, behind, jnp.zeros((8, width), F32))
        small_ref[router_dim : router_dim + 1, 0:width] = jnp.sum(gathered, axis=0, keepdims=True)


def backward_stage(
    m, tokens, grad_out, gains, weights, w_route, embed, ids, kept, home, slot_cap, moves, pushes, cid
):
    tok_count, width = tokens.shape[1:]
    experts, router_dim = embed.shape
    slots = experts * slot_cap
    steps = HEADS // GROUP
    span = GROUP * HEAD_DIM
    one = pl.Buffered(1)
    fixed = lambda shape: pl.BlockSpec(shape, lambda i: (0,) * len(shape), pipeline_mode=one)
    of_m = lambda *shape: pl.BlockSpec((None, *shape), lambda i: (m, 0, 0), pipeline_mode=one)
    columns = lambda height: pl.BlockSpec((height, span), lambda i: (0, i))
    lines = pl.BlockSpec((span, width), lambda i: (i, 0))
    gain_one, gain_two = gains
    wq, wk, wv, wo = weights
    first, projected, q, k, v, mixed, soft, inverses = kept
    low = lambda *shape: jax.ShapeDtypeStruct(shape, LOW)
    small = (-(-max(experts, router_dim + 2) // 8) * 8, width + 128)
    return call_with_moves(
        functools.partial(backward_kernel, m=m, steps=steps, slots=slots, slot_cap=slot_cap),
        moves,
        pushes,
        cid,
        grid=(steps,),
        in_specs=[
            of_m(tok_count, width), of_m(tok_count, width), fixed((width,)), columns(width), columns(width),
            columns(width), lines, fixed((width,)), fixed(w_route.shape), fixed(embed.shape),
            *[fixed(ids[0].shape)] * 3, fixed(first.shape), fixed(projected.shape), fixed(home[0].shape), fixed(home[1].shape),
            columns(tok_count), columns(tok_count), columns(tok_count), columns(tok_count),
            pl.BlockSpec(memory_space=pl.ANY), columns(tok_count),
        ],
        out_specs=[
            columns(width), columns(width), columns(width), lines, fixed((tok_count, width)), fixed(small),
        ],
        out_shape=[
            low(width, width), low(width, width), low(width, width), low(width, width), low(tok_count, width),
            jax.ShapeDtypeStruct(small, F32),
        ],
        scratch_shapes=[
            pltpu.VMEM((tok_count, width), F32), pltpu.VMEM((tok_count, width), LOW),
            pltpu.VMEM((width, tok_count), LOW), pltpu.VMEM((tok_count, width), F32),
        ]
        + [pltpu.VMEM((tok_count, span), LOW)] * 4
        + [pltpu.VMEM((2, 2, LENGTH, LENGTH), LOW), pltpu.SemaphoreType.DMA((2,))],
        cost=pl.CostEstimate(flops=40 * 10**9, bytes_accessed=50 * 2**20, transcendentals=0),
        name="backward_stage",
        args=(
            tokens, grad_out, gain_one, wq, wk, wv, wo, gain_two, w_route, embed, *ids, first,
            projected, *home, q, k, v, mixed, soft, inverses,
        ),
    )


def finish_kernel(*refs, cuts, blocks, tiles, per_tile):
    ids_ref, slot_ids_ref, keep_ref, embed_ref = refs[:4]
    ins, refs = [], refs[4:]
    for pieces in cuts:
        ins.append(refs[: 3 + len(pieces)])
        refs = refs[3 + len(pieces) :]
    near_in, near_outer = refs[:2]
    far_in, far_outer = refs[2 : 2 + tiles], refs[2 + tiles : 2 + 2 * tiles]
    big_ref = refs[2 + 2 * tiles]
    out_ref, grad_ref, din_ref, douter_ref, *big_outs = refs[3 + 2 * tiles :]
    step = pl.program_id(0)
    rows, width = out_ref.shape
    for m, pieces in enumerate(cuts):
        first_ref, projected_ref, gtok_ref, *home_refs = ins[m]
        for block in range(blocks):

            @pl.when(step == m * blocks + block)
            def _():
                some = slice(block * rows, (block + 1) * rows)
                returned = None
                for (low, high), home_ref in zip(pieces, home_refs):
                    line = piece_line(m, ids_ref, slot_ids_ref, keep_ref, low, high)[:, some]
                    column = to_column(line.astype(F32)).astype(jnp.int32)
                    term = dot(token_rows(column, home_ref.shape[0]), home_ref[...])
                    returned = term if returned is None else returned + term
                route_column = to_column(ids_ref[m : m + 1, some].astype(F32)).astype(jnp.int32)
                gate = route_probs(projected_ref[...], embed_ref[...], route_column)[-1]
                out_ref[...] = (first_ref[...] + gate * returned).astype(LOW)
                grad_ref[...] = gtok_ref[...]

    for t in range(tiles):

        @pl.when((step >= t * per_tile) & (step < (t + 1) * per_tile))
        def _():
            din_ref[0] = near_in[...] + sum(far_in[t][j].astype(F32) for j in range(far_in[t].shape[0]))
            douter_ref[0] = near_outer[...] + sum(far_outer[t][j].astype(F32) for j in range(far_outer[t].shape[0]))

    for k, big_out in enumerate(big_outs):
        big_out[...] = big_ref[:, k * width : (k + 1) * width].astype(F32)


def finish(ids, embed, parts, near, far, big):
    micro_count, tok_count = ids[0].shape
    width = parts[0][0].shape[1]
    near_in, near_outer = near
    tiles = len(far) // 2
    spread, _, tile = far[0].shape
    units = near_in.shape[1]
    span = 256 if tile % 256 == 0 else 128
    wide_steps, per_tile = units // span, tile // span
    rows = 256
    blocks = tok_count // rows
    steps = micro_count * blocks
    lines = big.shape[0] // steps
    whole = lambda shape: pl.BlockSpec(shape, lambda i: (0, 0), pipeline_mode=pl.Buffered(1))
    in_specs, args = [whole(ids[0].shape)] * 3 + [whole(embed.shape)], [*ids, embed]
    for at, (first, projected, gtok, homes) in enumerate(parts):
        place = lambda i, at=at: (jnp.clip(i - at * blocks, 0, blocks - 1), 0)
        in_specs += [
            pl.BlockSpec((rows, width), place), pl.BlockSpec((rows, projected.shape[1]), place),
            pl.BlockSpec((rows, width), place), *(whole(home.shape) for _, home in homes),
        ]
        args += [first, projected, gtok, *(home for _, home in homes)]
    near_at = lambda i: jnp.minimum(i, wide_steps - 1)
    far_at = lambda i, t: jnp.clip(i - t * per_tile, 0, per_tile - 1)
    in_specs += [
        pl.BlockSpec((width, span), lambda i: (0, near_at(i))), pl.BlockSpec((span, width), lambda i: (near_at(i), 0)),
    ]
    in_specs += [pl.BlockSpec((spread, width, span), lambda i, t=t: (0, 0, far_at(i, t))) for t in range(tiles)]
    in_specs += [pl.BlockSpec((spread, span, width), lambda i, t=t: (0, far_at(i, t), 0)) for t in range(tiles)]
    in_specs += [pl.BlockSpec((lines, big.shape[1]), lambda i: (i, 0))]
    row_out = pl.BlockSpec((None, rows, width), lambda i: (i // blocks, i % blocks, 0))
    line_out = pl.BlockSpec((lines, width), lambda i: (i, 0))
    kinds = big.shape[1] // width
    return pl.pallas_call(
        functools.partial(
            finish_kernel, cuts=[[cut for cut, _ in part[3]] for part in parts], blocks=blocks, tiles=tiles,
            per_tile=per_tile,
        ),
        grid=(steps,),
        in_specs=in_specs,
        out_specs=[
            row_out, row_out, pl.BlockSpec((1, width, span), lambda i: (0, 0, near_at(i))),
            pl.BlockSpec((1, span, width), lambda i: (0, near_at(i), 0)),
        ]
        + [line_out] * kinds,
        out_shape=[jax.ShapeDtypeStruct((micro_count, tok_count, width), LOW)] * 2
        + [jax.ShapeDtypeStruct((1, *near_in.shape), F32), jax.ShapeDtypeStruct((1, *near_outer.shape), F32)]
        + [jax.ShapeDtypeStruct((big.shape[0], width), F32)] * kinds,
        compiler_params=pltpu.CompilerParams(vmem_limit_bytes=VMEM_BYTES),
        cost_estimate=pl.CostEstimate(flops=3 * 10**9, bytes_accessed=56 * 2**20, transcendentals=0),
        name="finish",
    )(*args, near_in, near_outer, *far, big)


def gelu_and_slope(values):
    ratio = 1.0 / (1.0 + jnp.abs(values) * (0.3275911 * 0.7071067811865476))
    bell = jnp.exp(values * values * -0.5)
    series = 0.5 * 1.061405429
    for factor in (-1.453152027, 1.421413741, -0.284496736, 0.254829592):
        series = series * ratio + 0.5 * factor
    tail = series * ratio * bell
    below = jnp.where(values >= 0.0, 1.0 - tail, tail)
    return values * below, below + values * bell * 0.3989422804014327


def expert_kernel(*refs, cuts, more, last, per, steps, slot_cap, landings=(), settle=None):
    rows_ref, gate_ref, own_in, own_outer = refs[:4]
    cot_refs, refs = refs[4 : 4 + len(cuts)], refs[4 + len(cuts) :]
    far_in, refs = refs[:per], refs[per:]
    given = per - len(landings)
    far_outer, refs = [*refs[:given], *landings], refs[given:]
    if more:
        old_in, old_outer = refs[:2]
        refs = refs[2:]
    result_ref, sent_ref, dots_ref, din_ref, douter_ref = refs[:5]
    refs = refs[5:]
    if last:
        far_din, far_douter = refs[:2]
        refs = refs[2:]
    grad_sc, rows_t, acc_result, acc_sent, first_buf, second_buf, sems = refs
    step = pl.program_id(0)
    slot = lax.rem(step, 2)
    sources = rows_ref.shape[0] // slot_cap
    tile = first_buf.shape[2]

    def fetch(i):
        if i < per:
            first = own_in.at[:, i * tile : (i + 1) * tile]
            second = own_outer.at[i * tile : (i + 1) * tile, :]
        else:
            first, second = far_in[i % per].at[i // per - 1], far_outer[i % per].at[i // per - 1]
        return (
            pltpu.make_async_copy(first, first_buf.at[i % 2], sems.at[0, i % 2]),
            pltpu.make_async_copy(second, second_buf.at[i % 2], sems.at[1, i % 2]),
        )

    @pl.when(step == 0)
    def _():
        for copy in fetch(0):
            copy.start()
        for w in range(sources):
            part = slice(w * slot_cap, (w + 1) * slot_cap)
            gate = jnp.sum(jnp.where(diagonal(slot_cap), gate_ref[w, 0:1, :], 0.0), axis=1, keepdims=True)
            cot = jnp.concatenate([ref[w] for ref in cot_refs], axis=0)
            grad_sc[part, :] = (cot.astype(F32) * gate).astype(LOW)
        rows_t[...] = rows_ref[...].T
        acc_result[...] = jnp.zeros_like(acc_result)
        acc_sent[...] = jnp.zeros_like(acc_sent)

    for i in range(steps):

        @pl.when(step == i)
        def _():
            for copy in fetch(i):
                copy.wait()
            if landings and i + 1 == 2 * per - 1:
                settle(0)
            if i + 1 < steps:
                for copy in fetch(i + 1):
                    copy.start()

    first, second = first_buf[slot], second_buf[slot]
    hidden, slope = gelu_and_slope(dot(rows_ref[...], first))
    hidden = hidden.astype(LOW)
    grad_rows = grad_sc[...]
    grad_pre = (dot(grad_rows, second, NT) * slope).astype(LOW)
    acc_result[...] += dot(hidden, second)
    acc_sent[...] += dot(grad_pre, first, NT)
    din = dot(rows_t[...], grad_pre)
    douter = dot(hidden, grad_rows, TN)
    if more:
        din += old_in[...]
        douter += old_outer[...]
    if not last:
        din_ref[...] = din
        douter_ref[...] = douter
    else:

        @pl.when(step < per)
        def _():
            din_ref[...] = din
            douter_ref[...] = douter

        @pl.when(step >= per)
        def _():
            far_din[...] = din.astype(LOW)
            far_douter[...] = douter.astype(LOW)

    @pl.when(step == steps - 1)
    def _():
        result = acc_result[...].astype(LOW)
        result_ref[...] = result
        sent_ref[...] = acc_sent[...].astype(LOW)
        for w in range(sources):
            part = slice(w * slot_cap, (w + 1) * slot_cap)
            cot = jnp.concatenate([ref[w] for ref in cot_refs], axis=0)
            products = cot.astype(F32) * result[part, :].astype(F32)
            column = jnp.sum(products, axis=1, keepdims=True)
            row = jnp.sum(jnp.where(diagonal(slot_cap), column, 0.0), axis=0, keepdims=True)
            dots_ref[w] = jnp.broadcast_to(row, (8, 128))


def tile_of(units):
    return min(512, units)


def expert_stage(rows, cots, gates, weights, old, last, slot_cap, moves, pushes, cid):
    own_in, own_outer, far_in, far_outer = weights
    width, units = own_in.shape
    count = lax.axis_size("narrow")
    height = rows.shape[0]
    tile = tile_of(units)
    per = units // tile
    steps = count * per
    whole = lambda shape: pl.BlockSpec(shape, lambda i: (0,) * len(shape))
    anywhere = pl.BlockSpec(memory_space=pl.ANY)
    din_spec = pl.BlockSpec((None, width, tile), lambda i: (i, 0, 0))
    douter_spec = pl.BlockSpec((None, tile, width), lambda i: (i, 0, 0))
    out_specs = [whole((height, width)), whole((height, width)), whole(gates.shape)]
    out_shape = [
        jax.ShapeDtypeStruct((height, width), LOW),
        jax.ShapeDtypeStruct((height, width), LOW),
        jax.ShapeDtypeStruct(gates.shape, F32),
    ]
    if last:
        near = lambda i: jnp.minimum(i, per - 1)
        away = lambda i: jnp.maximum(i - per, 0)
        out_specs += [
            pl.BlockSpec((width, tile), lambda i: (0, near(i))),
            pl.BlockSpec((tile, width), lambda i: (near(i), 0)),
            pl.BlockSpec((None, width, tile), lambda i: (away(i), 0, 0)),
            pl.BlockSpec((None, tile, width), lambda i: (away(i), 0, 0)),
        ]
        out_shape += [
            jax.ShapeDtypeStruct((width, units), F32),
            jax.ShapeDtypeStruct((units, width), F32),
            jax.ShapeDtypeStruct((steps - per, width, tile), LOW),
            jax.ShapeDtypeStruct((steps - per, tile, width), LOW),
        ]
    else:
        out_specs += [din_spec, douter_spec]
        out_shape += [
            jax.ShapeDtypeStruct((steps, width, tile), F32),
            jax.ShapeDtypeStruct((steps, tile, width), F32),
        ]
    return call_with_moves(
        functools.partial(
            expert_kernel, cuts=[cot.shape[1] for cot in cots], more=bool(old), last=last, per=per, steps=steps,
            slot_cap=slot_cap,
        ),
        moves,
        pushes,
        cid,
        grid=(steps,),
        in_specs=[whole((height, width)), whole(gates.shape), anywhere, anywhere]
        + [whole(cot.shape) for cot in cots]
        + [anywhere] * (len(far_in) + len(far_outer))
        + ([din_spec, douter_spec] if old else []),
        out_specs=out_specs,
        out_shape=out_shape,
        scratch_shapes=[
            pltpu.VMEM((height, width), LOW),
            pltpu.VMEM((width, height), LOW),
            pltpu.VMEM((height, width), F32),
            pltpu.VMEM((height, width), F32),
            pltpu.VMEM((2, width, tile), LOW),
            pltpu.VMEM((2, tile, width), LOW),
            pltpu.SemaphoreType.DMA((2, 2)),
        ],
        cost=pl.CostEstimate(
            flops=12 * height * width * units * count, bytes_accessed=34 * 2**20, transcendentals=0
        ),
        name="expert_stage",
        args=(rows, gates, own_in, own_outer, *cots, *far_in, *far_outer, *old),
        late=len(far_outer) < per,
    )


def local(
    tokens,
    grad_out,
    route_ids,
    slot_ids,
    keep_ids,
    gain_one,
    w_query,
    w_key,
    w_value,
    w_out,
    gain_two,
    w_route,
    embed,
    w_in,
    w_outer,
):
    micro_count, tok_count, feat_width = tokens.shape
    expert_count = embed.shape[0]
    slot_cap = max(2, tok_count // expert_count)
    slots = expert_count * slot_cap
    own_in, own_outer = w_in[0], w_outer[0]
    units = own_in.shape[1]
    tile = tile_of(units)
    per = units // tile
    weight_pushes = []
    for t in range(per):
        some = slice(t * tile, (t + 1) * tile)
        weight_pushes.append((own_in, lambda ref, j, some=some: ref.at[:, some], (feat_width, tile)))
        weight_pushes.append((own_outer, lambda ref, j, some=some: ref.at[some, :], (tile, feat_width)))
    early = 2 if per > 1 else 1
    half = slot_cap // 2
    gains = (gain_one, gain_two)
    mixers = (w_query, w_key, w_value, w_out)
    ids = (route_ids, slot_ids, keep_ids)
    router = (w_route.T, embed, ids)

    def boxes(rows):
        return rows.reshape((expert_count, slot_cap) + rows.shape[1:])

    def flat(boxed):
        return boxed.reshape((boxed.shape[0] * boxed.shape[1],) + boxed.shape[2:])

    def entire(array):
        return array, 0, array.shape[1]

    cot_boxes = [boxes(rows) for rows in dispatch(ids, grad_out, slots, slot_cap)]
    (*ahead_0, sent, gates, projected), (cot_0,), far_a = forward_stage(
        0, tokens, gains, mixers, *router, slot_cap, (entire(cot_boxes[0]),), weight_pushes[:early], 1
    )
    ahead_0.append(projected)
    (*ahead_1, next_sent, next_gates, projected), (sent_0, gates_0, cot_1), far_b = forward_stage(
        1, tokens, gains, mixers, *router, slot_cap,
        (entire(boxes(sent)), entire(gates), entire(cot_boxes[1])), weight_pushes[early:-1], 2
    )
    ahead_1.append(projected)

    far = [*far_a, *far_b]
    (result_0, grad_0, dots_0, *old), (sent_1, gates_1), far_c = expert_stage(
        flat(sent_0), (cot_0,), gates_0, (own_in, own_outer, far[0::2], far[1::2]), (), False, slot_cap,
        (entire(boxes(next_sent)), entire(next_gates)), weight_pushes[-1:], 3
    )
    far = [*far, *far_c]
    result_0 = boxes(result_0)
    (result_1, grad_1, dots_1, near_din, near_douter, far_din, far_douter), (home_grad_0, home_dots_0), _ = (
        expert_stage(
            flat(sent_1), (cot_1,), gates_1, (own_in, own_outer, far[0::2], far[1::2]), tuple(old), True,
            slot_cap, (entire(boxes(grad_0)), entire(dots_0)), (), 4
        )
    )
    grad_pushes = [
        (far_din, lambda ref, j, t=t: ref.at[j * per + t], (feat_width, tile)) for t in range(per)
    ] + [
        (far_douter, lambda ref, j, t=t: ref.at[j * per + t], (tile, feat_width)) for t in range(per)
    ]
    later = len(grad_pushes) // 2

    def kept(ahead):
        q, k, v, soft, inverses, mixed, first, projected = ahead
        return first, projected, q, k, v, mixed, soft, inverses

    (*big_0, gtok_0, small_0), (home_grad_1, home_dots_1, home_b), got_a = backward_stage(
        0, tokens, grad_out, gains, mixers, *router, kept(ahead_0), (flat(home_grad_0), home_dots_0), slot_cap,
        (entire(boxes(grad_1)), entire(dots_1), (result_0, half, slot_cap)), grad_pushes[:later], 5
    )
    (*big_1, gtok_1, small_1), (home_1, home_c), got_b = backward_stage(
        1, tokens, grad_out, gains, mixers, *router, kept(ahead_1), (flat(home_grad_1), home_dots_1), slot_cap,
        (entire(boxes(result_1)), (result_0, 0, half)), grad_pushes[later:], 6
    )
    homes_0 = [((half, slot_cap), flat(home_b)), ((0, half), flat(home_c))]
    big, small = reduce_everywhere(list(zip(big_0, big_1)), (small_0, small_1), 7)
    block_out, grad_tokens, grad_in, grad_outer, *big = finish(
        ids, embed,
        (
            (ahead_0[6], ahead_0[7], gtok_0, homes_0),
            (ahead_1[6], ahead_1[7], gtok_1, [((0, slot_cap), flat(home_1))]),
        ),
        (near_din, near_douter), [*got_a, *got_b], big,
    )
    router_dim = w_route.shape[1]
    return (
        block_out,
        grad_tokens,
        small[router_dim, :feat_width],
        *big,
        small[router_dim + 1, :feat_width],
        small[:router_dim, :feat_width].T,
        small[:expert_count, feat_width : feat_width + router_dim],
        grad_in,
        grad_outer,
    )


def solution(mesh):
    tokens_spec = P(None, ("wide", "narrow"), None)
    ids_spec = P(None, ("wide", "narrow"))
    in_spec, outer_spec = P("wide", None, "narrow"), P("wide", "narrow", None)
    return jax.shard_map(
        local,
        mesh=mesh,
        in_specs=(tokens_spec,) * 2 + (ids_spec,) * 3 + (P(),) * 8 + (in_spec, outer_spec),
        out_specs=(tokens_spec,) * 2 + (P(),) * 8 + (in_spec, outer_spec),
        check_vma=False,
    )
```
